8 devices in a mesh: dp: 1 (over z), sp: 2 (over y), tp: 4 (over x, core).
Axes of the slice: x: 2, y: 2, z: 1, core: 2. Of those that a mesh axis runs over, the one named last changes fastest.
Arguments:
- hidden: bfloat16 [256, 2048], P('dp')
- new_pos: int32 [256], P('dp')
- k_self: bfloat16 [256, 256, 8, 128], P('dp', 'sp', 'tp')
- v_self: bfloat16 [256, 256, 8, 128], P('dp', 'sp', 'tp')
- k_cross: bfloat16 [256, 512, 8, 128], P('dp', None, 'tp')
- v_cross: bfloat16 [256, 512, 8, 128], P('dp', None, 'tp')
- xvalid: int32 [256, 512], P('dp')
- rowmask: int32 [256], P('dp')
- self_attn_norm: bfloat16 [2048], replicated
- self_wq: bfloat16 [2048, 2048], P(None, 'tp')
- self_wk: bfloat16 [2048, 1024], P(None, 'tp')
- self_wv: bfloat16 [2048, 1024], P(None, 'tp')
- self_wo: bfloat16 [2048, 2048], P('tp')
- self_mlp_norm: bfloat16 [2048], replicated
- self_wgate: bfloat16 [2048, 6144], P(None, 'tp')
- self_wup: bfloat16 [2048, 6144], P(None, 'tp')
- self_wdown: bfloat16 [6144, 2048], P('tp')
- cross_attn_norm: bfloat16 [2048], replicated
- cross_wq: bfloat16 [2048, 2048], P(None, 'tp')
- cross_qnorm: bfloat16 [128], replicated
- cross_wo: bfloat16 [2048, 2048], P('tp')
- cross_gates: float32 [2], replicated
- cross_mlp_norm: bfloat16 [2048], replicated
- cross_wgate: bfloat16 [2048, 6144], P(None, 'tp')
- cross_wup: bfloat16 [2048, 6144], P(None, 'tp')
- cross_wdown: bfloat16 [6144, 2048], P('tp')
Outputs:
- output 1: bfloat16 [256, 2048], P('dp')
- output 2: bfloat16 [256, 256, 8, 128], P('dp', 'sp', 'tp')
- output 3: bfloat16 [256, 256, 8, 128], P('dp', 'sp', 'tp')
All inputs are finite; a program needn't handle non-finite values.
Results may differ from the reference program's by a relative error of at most 0.0146321.
Values sent between devices are 32-bit elements.
A program may use at most 1 GiB of HBM per device.

```python
import math
import jax
import jax.numpy as jnp
from jax import lax

BATCH = 256
SEQ_LEN = 256
VIS_TOKENS = 512
HIDDEN = 2048
HEADS = 16
KV_HEADS = 8
HEAD_DIM = 128
MLP_DIM = 6144

GROUP_SIZE = HEADS // KV_HEADS
Q_WIDTH = HEADS * HEAD_DIM
KV_WIDTH = KV_HEADS * HEAD_DIM
NORM_EPS = 1e-5
ROPE_THETA = 500000.0
ROPE_FACTOR = 8.0
LOW_FREQ = 1.0
HIGH_FREQ = 4.0
ORIG_CTX = 8192.0
NEG_BIG = -1e30
KEY_SCALE = 1.6


def rope_freqs():
    inv_freq = 1.0 / (ROPE_THETA ** (jnp.arange(0, HEAD_DIM, 2).astype(jnp.float32) / HEAD_DIM))
    wavelen = 2.0 * math.pi / inv_freq
    smooth = (ORIG_CTX / wavelen - LOW_FREQ) / (HIGH_FREQ - LOW_FREQ)
    mid_freq = (1.0 - smooth) * inv_freq / ROPE_FACTOR + smooth * inv_freq
    scaled = jnp.where(wavelen > ORIG_CTX / LOW_FREQ, inv_freq / ROPE_FACTOR, mid_freq)
    return jnp.where(wavelen < ORIG_CTX / HIGH_FREQ, inv_freq, scaled)


def apply_rope(vectors, positions):
    half_dim = HEAD_DIM // 2
    angles = positions.astype(jnp.float32)[:, None] * rope_freqs()[None, :]
    cos_t = jnp.cos(angles)[:, None, :]
    sin_t = jnp.sin(angles)[:, None, :]
    first_half = vectors[..., :half_dim]
    second_half = vectors[..., half_dim:]
    return jnp.concatenate([first_half * cos_t - second_half * sin_t, second_half * cos_t + first_half * sin_t], axis=-1)


def rms_norm(values, gain_vec):
    vals32 = values.astype(jnp.float32)
    inv_rms = lax.rsqrt(jnp.mean(vals32 * vals32, axis=-1, keepdims=True) + NORM_EPS)
    return (vals32 * inv_rms * gain_vec.astype(jnp.float32)).astype(jnp.bfloat16)


def gated_mlp(normed, w_gate, w_up, w_down):
    gate_val = jnp.dot(normed, w_gate, preferred_element_type=jnp.float32).astype(jnp.bfloat16)
    up_val = jnp.dot(normed, w_up, preferred_element_type=jnp.float32).astype(jnp.bfloat16)
    hidden_act = (jax.nn.silu(gate_val.astype(jnp.float32)) * up_val.astype(jnp.float32)).astype(jnp.bfloat16)
    return jnp.dot(hidden_act, w_down, preferred_element_type=jnp.float32)


def attend_row(queries, key_rows, val_rows, valid_mask):
    scores = jnp.einsum('kgd,tkd->kgt', queries.astype(jnp.float32), key_rows.astype(jnp.float32)) * (HEAD_DIM ** -0.5)
    scores = jnp.where(valid_mask[None, None, :], scores, NEG_BIG)
    weights = jax.nn.softmax(scores, axis=-1)
    return jnp.einsum('kgt,tkd->kgd', weights, val_rows.astype(jnp.float32))


def attend_item(item):
    return attend_row(item[0], item[1], item[2], item[3])


def dense_weight(rand_key, rows, cols):
    return (jax.random.normal(rand_key, (rows, cols), jnp.float32) * (rows ** -0.5)).astype(jnp.bfloat16)


def norm_gain(rand_key, width, center):
    return (center + 0.35 * jax.random.normal(rand_key, (width,), jnp.float32)).astype(jnp.bfloat16)


def drifting_values(rand_key, length):
    noise_key, walk_key, dir_key = jax.random.split(rand_key, 3)
    noise_part = 0.6 * jax.random.normal(noise_key, (BATCH, length, KV_HEADS, HEAD_DIM), jnp.float32)
    walk_path = jnp.cumsum(jax.random.normal(walk_key, (BATCH, KV_HEADS, length), jnp.float32), axis=-1) * (length ** -0.5)
    direction = jax.random.normal(dir_key, (BATCH, KV_HEADS, HEAD_DIM), jnp.float32)
    return (noise_part + jnp.transpose(walk_path, (0, 2, 1))[:, :, :, None] * direction[:, None, :, :]).astype(jnp.bfloat16)


def setup_inputs(seed: int = 0, part: int = 0) -> dict:
    data_keys = jax.random.split(jax.random.fold_in(jax.random.key(seed), part), 12)
    weight_keys = jax.random.split(jax.random.key(seed + 1), 20)
    row_ids = jnp.arange(BATCH)
    new_pos = jax.random.randint(data_keys[0], (BATCH,), SEQ_LEN // 4, SEQ_LEN)
    new_pos = jnp.where(row_ids == 0, SEQ_LEN - 1, new_pos).astype(jnp.int32)
    rowmask = (jax.random.randint(data_keys[1], (BATCH,), 0, 4) > 0).astype(jnp.int32)
    rowmask = jnp.where(row_ids == 0, 1, jnp.where(row_ids == 1, 0, rowmask)).astype(jnp.int32)
    valid_len = jax.random.randint(data_keys[2], (BATCH,), VIS_TOKENS // 4, VIS_TOKENS + 1)
    valid_len = jnp.where(row_ids == 0, VIS_TOKENS, valid_len)
    xvalid = (jnp.arange(VIS_TOKENS)[None, :] < valid_len[:, None]).astype(jnp.int32)
    hidden = jax.random.normal(data_keys[3], (BATCH, HIDDEN), jnp.float32).astype(jnp.bfloat16)
    k_self = (KEY_SCALE * jax.random.normal(data_keys[4], (BATCH, SEQ_LEN, KV_HEADS, HEAD_DIM), jnp.float32)).astype(jnp.bfloat16)
    v_self = drifting_values(data_keys[5], SEQ_LEN)
    k_cross = (KEY_SCALE * jax.random.normal(data_keys[6], (BATCH, VIS_TOKENS, KV_HEADS, HEAD_DIM), jnp.float32)).astype(jnp.bfloat16)
    v_cross = drifting_values(data_keys[7], VIS_TOKENS)
    return dict(
        hidden=hidden,
        new_pos=new_pos,
        k_self=k_self,
        v_self=v_self,
        k_cross=k_cross,
        v_cross=v_cross,
        xvalid=xvalid,
        rowmask=rowmask,
        self_attn_norm=norm_gain(weight_keys[0], HIDDEN, 1.0),
        self_wq=dense_weight(weight_keys[1], HIDDEN, Q_WIDTH),
        self_wk=dense_weight(weight_keys[2], HIDDEN, KV_WIDTH),
        self_wv=dense_weight(weight_keys[3], HIDDEN, KV_WIDTH),
        self_wo=dense_weight(weight_keys[4], Q_WIDTH, HIDDEN),
        self_mlp_norm=norm_gain(weight_keys[5], HIDDEN, 1.0),
        self_wgate=dense_weight(weight_keys[6], HIDDEN, MLP_DIM),
        self_wup=dense_weight(weight_keys[7], HIDDEN, MLP_DIM),
        self_wdown=dense_weight(weight_keys[8], MLP_DIM, HIDDEN),
        cross_attn_norm=norm_gain(weight_keys[9], HIDDEN, 1.0),
        cross_wq=dense_weight(weight_keys[10], HIDDEN, Q_WIDTH),
        cross_qnorm=norm_gain(weight_keys[11], HEAD_DIM, 1.5),
        cross_wo=dense_weight(weight_keys[12], Q_WIDTH, HIDDEN),
        cross_gates=jax.random.uniform(weight_keys[13], (2,), jnp.float32, 0.5, 1.5),
        cross_mlp_norm=norm_gain(weight_keys[14], HIDDEN, 1.0),
        cross_wgate=dense_weight(weight_keys[15], HIDDEN, MLP_DIM),
        cross_wup=dense_weight(weight_keys[16], HIDDEN, MLP_DIM),
        cross_wdown=dense_weight(weight_keys[17], MLP_DIM, HIDDEN),
    )


def reference(hidden, new_pos, k_self, v_self, k_cross, v_cross, xvalid, rowmask,
              self_attn_norm, self_wq, self_wk, self_wv, self_wo, self_mlp_norm,
              self_wgate, self_wup, self_wdown, cross_attn_norm, cross_wq, cross_qnorm,
              cross_wo, cross_gates, cross_mlp_norm, cross_wgate, cross_wup, cross_wdown):
    normed = rms_norm(hidden, self_attn_norm)
    queries = jnp.dot(normed, self_wq, preferred_element_type=jnp.float32).astype(jnp.bfloat16)
    key_new = jnp.dot(normed, self_wk, preferred_element_type=jnp.float32).astype(jnp.bfloat16)
    val_new = jnp.dot(normed, self_wv, preferred_element_type=jnp.float32).astype(jnp.bfloat16)
    queries = apply_rope(queries.reshape(BATCH, HEADS, HEAD_DIM).astype(jnp.float32), new_pos).astype(jnp.bfloat16)
    key_new = apply_rope(key_new.reshape(BATCH, KV_HEADS, HEAD_DIM).astype(jnp.float32), new_pos).astype(jnp.bfloat16)
    val_new = val_new.reshape(BATCH, KV_HEADS, HEAD_DIM)
    slot_ids = jnp.arange(SEQ_LEN)
    hit_mask = (slot_ids[None, :] == new_pos[:, None])[:, :, None, None]
    k_new_cache = jnp.where(hit_mask, key_new[:, None], k_self)
    v_new_cache = jnp.where(hit_mask, val_new[:, None], v_self)
    seen_mask = slot_ids[None, :] <= new_pos[:, None]
    self_out = lax.map(attend_item, (queries.reshape(BATCH, KV_HEADS, GROUP_SIZE, HEAD_DIM), k_new_cache, v_new_cache, seen_mask))
    self_flat = self_out.astype(jnp.bfloat16).reshape(BATCH, Q_WIDTH)
    after_attn = (hidden.astype(jnp.float32) + jnp.dot(self_flat, self_wo, preferred_element_type=jnp.float32)).astype(jnp.bfloat16)
    mlp_out = gated_mlp(rms_norm(after_attn, self_mlp_norm), self_wgate, self_wup, self_wdown)
    after_mlp = (after_attn.astype(jnp.float32) + mlp_out).astype(jnp.bfloat16)
    normed = rms_norm(after_mlp, cross_attn_norm)
    cross_q = jnp.dot(normed, cross_wq, preferred_element_type=jnp.float32).astype(jnp.bfloat16)
    cross_q = rms_norm(cross_q.reshape(BATCH, HEADS, HEAD_DIM), cross_qnorm)
    cross_out = lax.map(attend_item, (cross_q.reshape(BATCH, KV_HEADS, GROUP_SIZE, HEAD_DIM), k_cross, v_cross, xvalid > 0))
    cross_flat = cross_out.astype(jnp.bfloat16).reshape(BATCH, Q_WIDTH)
    gate_vals = jnp.tanh(cross_gates.astype(jnp.float32))
    row_scale = rowmask.astype(jnp.float32)[:, None]
    cross_proj = jnp.dot(cross_flat, cross_wo, preferred_element_type=jnp.float32)
    after_cross = (after_mlp.astype(jnp.float32) + gate_vals[0] * row_scale * cross_proj).astype(jnp.bfloat16)
    xmlp_out = gated_mlp(rms_norm(after_cross, cross_mlp_norm), cross_wgate, cross_wup, cross_wdown)
    after_xmlp = (after_cross.astype(jnp.float32) + gate_vals[1] * row_scale * xmlp_out).astype(jnp.bfloat16)
    return (after_xmlp, k_new_cache, v_new_cache)
```

```python
import functools
import math
import jax
import jax.numpy as jnp
from jax import lax
from jax.experimental import pallas as pl
from jax.experimental.pallas import tpu as pltpu
from jax.sharding import PartitionSpec as P

NORM_EPS = 1e-5
ROPE_THETA = 500000.0
ROPE_FACTOR = 8.0
LOW_FREQ = 1.0
HIGH_FREQ = 4.0
ORIG_CTX = 8192.0
NEG_BIG = -1e30

BF = jnp.bfloat16
F32 = jnp.float32
D = 128
HL = 4
KL = 2
NB = 256
NH = 128
NQ = 64
HID = 2048
NCH = 4
W = HID // NCH
VMEM_MAX = 66 * 1024 * 1024 - 2 * 1024 * 1024
MESH = pl.DeviceIdType.MESH
ANY = pl.BlockSpec(memory_space=pl.ANY)
VM = pl.BlockSpec(memory_space=pltpu.VMEM)


def rope_freqs(head_dim):
    inv_freq = 1.0 / (ROPE_THETA ** (jnp.arange(0, head_dim, 2).astype(jnp.float32) / head_dim))
    wavelen = 2.0 * math.pi / inv_freq
    smooth = (ORIG_CTX / wavelen - LOW_FREQ) / (HIGH_FREQ - LOW_FREQ)
    mid_freq = (1.0 - smooth) * inv_freq / ROPE_FACTOR + smooth * inv_freq
    scaled = jnp.where(wavelen > ORIG_CTX / LOW_FREQ, inv_freq / ROPE_FACTOR, mid_freq)
    return jnp.where(wavelen < ORIG_CTX / HIGH_FREQ, inv_freq, scaled)


def norm32(vals32, gain32):
    inv = lax.rsqrt(jnp.mean(vals32 * vals32, axis=-1, keepdims=True) + NORM_EPS)
    return (vals32 * inv * gain32).astype(BF)


def dot(a, b):
    return jnp.dot(a, b, preferred_element_type=F32)


def dot_nt(a, b):
    return lax.dot_general(a, b, (((1,), (1,)), ((), ())), preferred_element_type=F32)


def pair_attend(lhs, keys, vals, valid, scale):
    s = dot_nt(lhs, keys) * scale
    s = jnp.where(valid, s, NEG_BIG)
    m = jnp.max(s, axis=-1, keepdims=True)
    p = jnp.where(valid, jnp.exp(s - m), 0.0)
    l = jnp.sum(p, axis=-1, keepdims=True)
    o = dot(p.astype(BF), vals)
    first = lax.broadcasted_iota(jnp.int32, (8, D), 0) < HL
    return m, l, jnp.where(first, o[:, :D], o[:, D:])


def spread_heads(ref, heads, start, rows):
    odd = (lax.broadcasted_iota(jnp.int32, (rows, D), 0) % 2) == 1
    for h in range(HL):
        ref[pl.ds(start * 8 + h, rows, stride=8), :] = jnp.where(odd, 0.0, heads[h])
        ref[pl.ds(start * 8 + HL + h, rows, stride=8), :] = jnp.where(odd, heads[h], 0.0)


SR = 16


def self_kernel(pos_ref, hid_ref, g_ref, wq_ref, wk_ref, wv_ref, cos_ref, sin_ref, k_ref, v_ref,
                ko_ref, vo_ref, o_ref, st_ref, qs, kn, vn):
    step = pl.program_id(0)

    @pl.when(step == 0)
    def _():
        x = norm32(hid_ref[...].astype(F32), g_ref[...].astype(F32))
        cos, sin = cos_ref[...], sin_ref[...]

        def rope(part):
            part = part.astype(BF).astype(F32)
            return (part * cos + pltpu.roll(part, D // 2, 1) * sin).astype(BF).astype(F32)

        q = dot(x, wq_ref[...])
        spread_heads(qs, [rope(q[:, h * D:(h + 1) * D]) for h in range(HL)], 0, NB)
        k = dot(x, wk_ref[...])
        v = dot(x, wv_ref[...])
        for h in range(KL):
            kn[pl.ds(h, NB, stride=KL), :] = rope(k[:, h * D:(h + 1) * D])
            vn[pl.ds(h, NB, stride=KL), :] = v[:, h * D:(h + 1) * D].astype(BF).astype(F32)

    T2 = k_ref.shape[1]
    scale = D ** -0.5
    col = lax.broadcasted_iota(jnp.int32, (8, T2), 1)
    row = lax.broadcasted_iota(jnp.int32, (8, T2), 0)
    tok = col // KL
    head_ok = (col % KL) == ((row % HL) // (HL // KL))
    lane = lax.broadcasted_iota(jnp.int32, (8, D), 1)
    i16 = lax.broadcasted_iota(jnp.int32, (16, D), 0)

    def patch(new_ref, dst_ref, r, b, lp):
        base = pl.multiple_of((jnp.clip(lp, 0, T2 // KL - 1) // 8) * 16, 16)
        fresh = jnp.where(i16 % 2 == 0, new_ref[pl.ds(2 * b, 1), :], new_ref[pl.ds(2 * b + 1, 1), :])
        old = dst_ref[r, pl.ds(base, 16), :].astype(F32)
        dst_ref[r, pl.ds(base, 16), :] = jnp.where(base + i16 - i16 % 2 == 2 * lp, fresh, old).astype(BF)

    st = jnp.where(step % (NH // SR) == 0, jnp.zeros((8, D), F32), st_ref[...])
    for p in range(SR // 2):
        b0 = step * SR + 2 * p
        lp0, lp1 = pos_ref[b0], pos_ref[b0 + 1]
        for r, b, lp in ((2 * p, b0, lp0), (2 * p + 1, b0 + 1, lp1)):
            ko_ref[r] = k_ref[r]
            vo_ref[r] = v_ref[r]
            patch(kn, ko_ref, r, b, lp)
            patch(vn, vo_ref, r, b, lp)
        q16 = qs[pl.ds(pl.multiple_of(b0 * 8, 16), 16), :]
        lhs = jnp.concatenate([q16[:8], q16[8:]], axis=1).astype(BF)
        keys = jnp.concatenate([ko_ref[2 * p], ko_ref[2 * p + 1]], axis=1)
        vals = jnp.concatenate([vo_ref[2 * p], vo_ref[2 * p + 1]], axis=1)
        valid = head_ok & (tok <= jnp.where(row < HL, lp0, lp1))
        m, l, o = pair_attend(lhs, keys, vals, valid, scale)
        o_ref[pl.ds(8 * p, 8), :] = o
        pair = (step % (NH // SR)) * (SR // 2) + p
        st = jnp.where(lane == pair, m, jnp.where(lane == pair + NQ, l, st))
    st_ref[...] = st


def self_attention(hidden, local_pos, k_self, v_self, g1, wq, wk, wv, cos, sin):
    T2 = k_self.shape[1]
    const = lambda i, p: (0, 0)
    blk = pl.BlockSpec((SR, T2, D), lambda i, p: (i, 0, 0))
    full = lambda a: pl.BlockSpec(a.shape, const)
    small = [hidden, g1, wq, wk, wv, cos, sin]
    return pl.pallas_call(
        self_kernel,
        grid_spec=pltpu.PrefetchScalarGridSpec(
            num_scalar_prefetch=1,
            grid=(NB // SR,),
            in_specs=[full(a) for a in small] + [blk, blk],
            out_specs=[blk, blk, pl.BlockSpec((SR * HL, D), lambda i, p: (i, 0)),
                       pl.BlockSpec((8, D), lambda i, p: (i // (NH // SR), 0))],
            scratch_shapes=[pltpu.VMEM((NB * 8, D), F32), pltpu.VMEM((NB * KL, D), F32), pltpu.VMEM((NB * KL, D), F32)],
        ),
        out_shape=[jax.ShapeDtypeStruct(k_self.shape, BF), jax.ShapeDtypeStruct(v_self.shape, BF),
                   jax.ShapeDtypeStruct((NB * HL, D), F32), jax.ShapeDtypeStruct((16, D), F32)],
        compiler_params=pltpu.CompilerParams(vmem_limit_bytes=VMEM_MAX),
        name="self_attn",
    )(local_pos, *small, k_self, v_self)


def peers():
    sp, tp = lax.axis_index("sp"), lax.axis_index("tp")
    core = lax.rem(tp, 2)
    return dict(sp=sp, core=core, y={"sp": 1 - sp}, c={"tp": tp + 1 - 2 * core}, x={"tp": lax.rem(tp + 2, 4)})


def entry_barrier(pe):
    barrier = pltpu.get_barrier_semaphore()
    for name in ("y", "c", "x"):
        pl.semaphore_signal(barrier, inc=1, device_id=pe[name], device_id_type=MESH)
    pl.semaphore_wait(barrier, 3)


def rcopy(src, dst, ssem, rsem, dev):
    return pltpu.make_async_remote_copy(src_ref=src, dst_ref=dst, send_sem=ssem, recv_sem=rsem,
                                        device_id=dev, device_id_type=MESH)


def tp_sum(pe, compute, finish, snd, rcv, chip, xr, sems):
    to_core = [rcopy(snd.at[j], rcv.at[j], sems.at[0, j], sems.at[1, j], pe["c"]) for j in range(NCH)]
    to_chip = [rcopy(chip.at[j], xr.at[j], sems.at[2, j], sems.at[3, j], pe["x"]) for j in range(NCH)]
    for j in range(NCH + 1):
        if j < NCH:
            part = compute(j)
            snd[j] = part[NQ:]
            chip[j] = part[:NQ]
            to_core[j].start()
        if j >= 1:
            to_core[j - 1].wait_recv()
            chip[j - 1] = chip[j - 1] + rcv[j - 1]
            to_chip[j - 1].start()
    for j in range(NCH):
        to_chip[j].wait_recv()
        finish(j, chip[j] + xr[j])
    for j in range(NCH):
        to_core[j].wait_send()
        to_chip[j].wait_send()


def share_rows(pe, own, x_ref, snd, rcv, sem):
    snd[...] = own.astype(F32)
    cp = rcopy(snd, rcv, sem.at[0], sem.at[1], pe["c"])
    cp.start()
    x_ref[pl.ds(0, NQ), :] = own
    cp.wait()
    x_ref[pl.ds(NQ, NQ), :] = rcv[...].astype(BF)


def mlp_act(x_ref, wg, wu, act, n_cols):
    step = 512
    for c in range(n_cols // step):
        s = slice(c * step, (c + 1) * step)
        gate = dot(x_ref[...], wg[:, s]).astype(BF).astype(F32)
        up = dot(x_ref[...], wu[:, s]).astype(BF).astype(F32)
        act[:, s] = (gate * jax.nn.sigmoid(gate) * up).astype(BF)


def cols(j):
    return slice(j * W, (j + 1) * W)


def heads_to_lanes(ref, core):
    parts = []
    for start in (core * NQ, (1 - core) * NQ):
        parts.append(jnp.concatenate([ref[pl.ds(start * HL + h, NQ, stride=HL), :] for h in range(HL)], axis=1))
    return jnp.concatenate(parts, axis=0).astype(BF)


SUM_SCRATCH = [pltpu.VMEM((NCH, NQ, W), F32)] * 4 + [pltpu.SemaphoreType.DMA((4, NCH))]
SHARE_SCRATCH = [pltpu.VMEM((NQ, HID), F32)] * 2 + [pltpu.SemaphoreType.DMA((2,))]


def mid_kernel(o_hbm, st_ref, hid_hbm, g2_ref, g3_ref, qn_ref, wo_hbm, wg_hbm, wu_hbm, wd_hbm, wq_hbm,
               qx_ref, h2_ref,
               wo, wg, wu, wd, wq, wsem, osnd, orcv, sts, str_, ysem, hown, att, xbuf, act, hres,
               a0, a1, a2, a3, asem, b0, b1, b2, b3, bsem, s0, s1, ssem, t0, t1, tsem):
    pe = peers()
    sp, core = pe["sp"], pe["core"]
    half = NH * HL
    local = [pltpu.make_async_copy(o_hbm.at[pl.ds(pl.multiple_of(sp * half, half), half)], att, wsem.at[5]),
             pltpu.make_async_copy(o_hbm.at[pl.ds(pl.multiple_of((1 - sp) * half, half), half)], osnd, wsem.at[6]),
             pltpu.make_async_copy(hid_hbm.at[pl.ds(pl.multiple_of(sp * NH + core * NQ, NQ), NQ)], hown, wsem.at[7])]
    for cp in local:
        cp.start()
    loads = [pltpu.make_async_copy(a, b, wsem.at[n])
             for n, (a, b) in enumerate(((wo_hbm, wo), (wg_hbm, wg), (wu_hbm, wu), (wd_hbm, wd), (wq_hbm, wq)))]
    for cp in loads:
        cp.start()
    entry_barrier(pe)
    both = st_ref[...]
    mine = jnp.where(sp == 0, both[:8], both[8:])
    sts[...] = jnp.where(sp == 0, both[8:], both[:8])
    local[1].wait()
    cp_o = rcopy(osnd, orcv, ysem.at[0], ysem.at[1], pe["y"])
    cp_s = rcopy(sts, str_, ysem.at[2], ysem.at[3], pe["y"])
    cp_s.start()
    cp_o.start()
    local[0].wait()
    local[2].wait()
    cp_s.wait()
    theirs = str_[...]
    top = jnp.maximum(mine, theirs)
    f1, f2 = jnp.exp(mine - top), jnp.exp(theirs - top)
    den = pltpu.roll(mine, NQ, 1) * f1 + pltpu.roll(theirs, NQ, 1) * f2
    c1, c2 = f1 / den, f2 / den
    cp_o.wait()
    for p in range(NQ):
        s = pl.ds(8 * p, 8)
        att[s, :] = att[s, :] * c1[:, p:p + 1] + orcv[s, :] * c2[:, p:p + 1]
    lhs = heads_to_lanes(att, core)

    loads[0].wait()

    def done1(j, total):
        hres[:, cols(j)] = (hown[:, cols(j)].astype(F32) + total).astype(BF)

    tp_sum(pe, lambda j: dot(lhs, wo[:, cols(j)]), done1, a0, a1, a2, a3, asem)
    share_rows(pe, norm32(hres[...].astype(F32), g2_ref[...].astype(F32)), xbuf, s0, s1, ssem)
    loads[1].wait()
    loads[2].wait()
    mlp_act(xbuf, wg, wu, act, act.shape[1])
    loads[3].wait()

    def done2(j, total):
        h2_ref[:, cols(j)] = (hres[:, cols(j)].astype(F32) + total).astype(BF)

    tp_sum(pe, lambda j: dot(act[...], wd[:, cols(j)]), done2, b0, b1, b2, b3, bsem)
    share_rows(pe, norm32(h2_ref[...].astype(F32), g3_ref[...].astype(F32)), xbuf, t0, t1, tsem)
    loads[4].wait()
    q = dot(xbuf[...], wq[...])
    gain = qn_ref[...].astype(F32)
    heads = [norm32(q[:, h * D:(h + 1) * D].astype(BF).astype(F32), gain).astype(F32) for h in range(HL)]
    spread_heads(qx_ref, [h[:NQ] for h in heads], core * NQ, NQ)
    spread_heads(qx_ref, [h[NQ:] for h in heads], (1 - core) * NQ, NQ)


def mid_stage(o, st, hidden, g2, g3, qn, wo, wg, wu, wd, wq):
    F = wg.shape[1]
    return pl.pallas_call(
        mid_kernel,
        in_specs=[ANY, VM, ANY, VM, VM, VM] + [ANY] * 5,
        out_specs=[VM, VM],
        out_shape=[jax.ShapeDtypeStruct((NH * 8, D), F32), jax.ShapeDtypeStruct((NQ, HID), BF)],
        scratch_shapes=[pltpu.VMEM(wo.shape, BF), pltpu.VMEM(wg.shape, BF), pltpu.VMEM(wu.shape, BF),
                        pltpu.VMEM(wd.shape, BF), pltpu.VMEM(wq.shape, BF), pltpu.SemaphoreType.DMA((8,)),
                        pltpu.VMEM((NH * HL, D), F32), pltpu.VMEM((NH * HL, D), F32),
                        pltpu.VMEM((8, D), F32), pltpu.VMEM((8, D), F32), pltpu.SemaphoreType.DMA((4,)),
                        pltpu.VMEM((NQ, HID), BF), pltpu.VMEM((NH * HL, D), F32), pltpu.VMEM((NH, HID), BF),
                        pltpu.VMEM((NH, F), BF), pltpu.VMEM((NQ, HID), BF)]
        + SUM_SCRATCH + SUM_SCRATCH + SHARE_SCRATCH + SHARE_SCRATCH,
        compiler_params=pltpu.CompilerParams(collective_id=0, has_side_effects=True, vmem_limit_bytes=VMEM_MAX),
        name="mid_stage",
    )(o, st, hidden, g2, g3, qn, wo, wg, wu, wd, wq)


CR = 8


def cross_kernel(meta_ref, q_ref, k_ref, v_ref, o_ref):
    step = pl.program_id(0)
    T2 = k_ref.shape[1]
    scale = D ** -0.5
    col = lax.broadcasted_iota(jnp.int32, (8, T2), 1)
    row = lax.broadcasted_iota(jnp.int32, (8, T2), 0)
    tok = col // KL
    head_ok = (col % KL) == ((row % HL) // (HL // KL))
    for p in range(CR // 2):
        b0 = meta_ref[0] * NH + step * CR + 2 * p
        n0, n1 = meta_ref[1 + b0], meta_ref[2 + b0]
        q16 = q_ref[pl.ds(16 * p, 16), :]
        lhs = jnp.concatenate([q16[:8], q16[8:]], axis=1).astype(BF)
        keys = jnp.concatenate([k_ref[2 * p], k_ref[2 * p + 1]], axis=1)
        vals = jnp.concatenate([v_ref[2 * p], v_ref[2 * p + 1]], axis=1)
        valid = head_ok & (tok < jnp.where(row < HL, n0, n1))
        m, l, o = pair_attend(lhs, keys, vals, valid, scale)
        o_ref[pl.ds(8 * p, 8), :] = o / l


def cross_attention(q, meta, k_cross, v_cross):
    T2 = k_cross.shape[1]
    blk = pl.BlockSpec((CR, T2, D), lambda i, m: (m[0] * (NH // CR) + i, 0, 0))
    return pl.pallas_call(
        cross_kernel,
        grid_spec=pltpu.PrefetchScalarGridSpec(
            num_scalar_prefetch=1,
            grid=(NH // CR,),
            in_specs=[pl.BlockSpec((CR * 8, D), lambda i, m: (i, 0)), blk, blk],
            out_specs=pl.BlockSpec((CR * HL, D), lambda i, m: (i, 0)),
        ),
        out_shape=jax.ShapeDtypeStruct((NH * HL, D), F32),
        compiler_params=pltpu.CompilerParams(vmem_limit_bytes=VMEM_MAX),
        name="cross_attn",
    )(meta, q, k_cross, v_cross)


def last_kernel(att_ref, h2_ref, g4_ref, gates_ref, mask_ref, wo_hbm, wg_hbm, wu_hbm, wd_hbm,
                out_ref,
                wo, wg, wu, wd, wsem, xbuf, act, hres, fin, yr, cr, gsem,
                a0, a1, a2, a3, asem, b0, b1, b2, b3, bsem, s0, s1, ssem):
    pe = peers()
    sp, core = pe["sp"], pe["core"]
    loads = [pltpu.make_async_copy(a, b, wsem.at[n])
             for n, (a, b) in enumerate(((wo_hbm, wo), (wg_hbm, wg), (wu_hbm, wu), (wd_hbm, wd)))]
    for cp in loads:
        cp.start()
    entry_barrier(pe)
    lhs = heads_to_lanes(att_ref, core)

    def rows(half, of_core):
        return pl.ds(pl.multiple_of(half * NH + of_core * NQ, NQ), NQ)

    row_scale = mask_ref[rows(sp, core), :]
    gates = jnp.tanh(gates_ref[...])
    gate0, gate1 = gates[:, 0:1] * row_scale, gates[:, 1:2] * row_scale
    loads[0].wait()

    def done3(j, total):
        hres[:, cols(j)] = (h2_ref[:, cols(j)].astype(F32) + gate0 * total).astype(BF)

    tp_sum(pe, lambda j: dot(lhs, wo[:, cols(j)]), done3, a0, a1, a2, a3, asem)
    share_rows(pe, norm32(hres[...].astype(F32), g4_ref[...].astype(F32)), xbuf, s0, s1, ssem)
    loads[1].wait()
    loads[2].wait()
    mlp_act(xbuf, wg, wu, act, act.shape[1])
    loads[3].wait()

    to_y = [rcopy(fin.at[j], yr.at[j], gsem.at[0, j], gsem.at[1, j], pe["y"]) for j in range(NCH)]
    to_c = [rcopy(fin.at[j], cr.at[0, j], gsem.at[2, j], gsem.at[3, j], pe["c"]) for j in range(NCH)]
    pass_c = [rcopy(yr.at[j], cr.at[1, j], gsem.at[4, j], gsem.at[5, j], pe["c"]) for j in range(NCH)]

    def done4(j, total):
        res = (hres[:, cols(j)].astype(F32) + gate1 * total).astype(BF)
        out_ref[rows(sp, core), cols(j)] = res
        fin[j] = res.astype(F32)
        to_y[j].start()
        to_c[j].start()
        if j >= 1:
            to_y[j - 1].wait_recv()
            pass_c[j - 1].start()

    tp_sum(pe, lambda j: dot(act[...], wd[:, cols(j)]), done4, b0, b1, b2, b3, bsem)
    to_y[NCH - 1].wait_recv()
    pass_c[NCH - 1].start()
    for j in range(NCH):
        out_ref[rows(1 - sp, core), cols(j)] = yr[j].astype(BF)
        to_c[j].wait_recv()
        out_ref[rows(sp, 1 - core), cols(j)] = cr[0, j].astype(BF)
    for j in range(NCH):
        pass_c[j].wait_recv()
        out_ref[rows(1 - sp, 1 - core), cols(j)] = cr[1, j].astype(BF)
    for j in range(NCH):
        to_y[j].wait_send()
        to_c[j].wait_send()
        pass_c[j].wait_send()


def last_stage(att, h2, g4, gates, mask, wo, wg, wu, wd):
    F = wg.shape[1]
    return pl.pallas_call(
        last_kernel,
        in_specs=[VM] * 5 + [ANY] * 4,
        out_specs=VM,
        out_shape=jax.ShapeDtypeStruct((NB, HID), BF),
        scratch_shapes=[pltpu.VMEM(wo.shape, BF), pltpu.VMEM(wg.shape, BF), pltpu.VMEM(wu.shape, BF),
                        pltpu.VMEM(wd.shape, BF), pltpu.SemaphoreType.DMA((4,)),
                        pltpu.VMEM((NH, HID), BF), pltpu.VMEM((NH, F), BF), pltpu.VMEM((NQ, HID), BF),
                        pltpu.VMEM((NCH, NQ, W), F32), pltpu.VMEM((NCH, NQ, W), F32),
                        pltpu.VMEM((2, NCH, NQ, W), F32), pltpu.SemaphoreType.DMA((6, NCH))]
        + SUM_SCRATCH + SUM_SCRATCH + SHARE_SCRATCH,
        compiler_params=pltpu.CompilerParams(collective_id=1, has_side_effects=True, vmem_limit_bytes=VMEM_MAX),
        name="last_stage",
    )(att, h2, g4, gates, mask, wo, wg, wu, wd)


def solution(mesh):
    cache_spec = P('dp', 'sp', 'tp', None)
    cross_spec = P('dp', None, 'tp', None)
    row_spec = P('dp', None)
    vec_spec = P('dp')
    full_spec = P(None)
    col_spec = P(None, 'tp')
    split_rows = P('tp', None)
    in_specs = (row_spec, vec_spec, cache_spec, cache_spec, cross_spec, cross_spec, row_spec, vec_spec,
                full_spec, col_spec, col_spec, col_spec, split_rows, full_spec, col_spec, col_spec, split_rows,
                full_spec, col_spec, full_spec, split_rows, full_spec, full_spec, col_spec, col_spec, split_rows)
    out_specs = (row_spec, cache_spec, cache_spec)

    def local_step(hidden, new_pos, k_self, v_self, k_cross, v_cross, xvalid, rowmask,
                   self_attn_norm, self_wq, self_wk, self_wv, self_wo, self_mlp_norm,
                   self_wgate, self_wup, self_wdown, cross_attn_norm, cross_wq, cross_qnorm,
                   cross_wo, cross_gates, cross_mlp_norm, cross_wgate, cross_wup, cross_wdown):
        sp = lax.axis_index('sp')
        len_local = k_self.shape[1]
        angles = new_pos.astype(F32)[:, None] * rope_freqs(D)[None, :]
        cos_t, sin_t = jnp.cos(angles), jnp.sin(angles)
        cos = jnp.concatenate([cos_t, cos_t], axis=1)
        sin = jnp.concatenate([-sin_t, sin_t], axis=1)
        flat = lambda a: a.reshape(a.shape[0], a.shape[1] * a.shape[2], a.shape[3])
        row = lambda a: a.reshape(1, -1)
        k_out, v_out, o, st = self_attention(
            hidden, new_pos - sp * len_local, flat(k_self), flat(v_self), row(self_attn_norm),
            self_wq, self_wk, self_wv, cos, sin)
        qx, h2 = mid_stage(o, st, hidden, row(self_mlp_norm), row(cross_attn_norm), row(cross_qnorm),
                           self_wo, self_wgate, self_wup, self_wdown, cross_wq)
        counts = jnp.sum((xvalid > 0).astype(jnp.int32), axis=1)
        meta = jnp.concatenate([sp.astype(jnp.int32)[None], counts])
        att = cross_attention(qx, meta, flat(k_cross), flat(v_cross))
        h4 = last_stage(att, h2, row(cross_mlp_norm), row(cross_gates.astype(F32)),
                        rowmask.astype(F32)[:, None], cross_wo, cross_wgate, cross_wup, cross_wdown)
        return h4, k_out.reshape(k_self.shape), v_out.reshape(v_self.shape)

    return jax.shard_map(local_step, mesh=mesh, in_specs=in_specs, out_specs=out_specs, check_vma=False)
```

```python
import functools
import math
import numpy as np
import jax
import jax.numpy as jnp
from jax import lax
from jax.experimental import pallas as pl
from jax.experimental.pallas import tpu as pltpu
from jax.sharding import PartitionSpec as P

NORM_EPS = 1e-5
ROPE_THETA = 500000.0
ROPE_FACTOR = 8.0
LOW_FREQ = 1.0
HIGH_FREQ = 4.0
ORIG_CTX = 8192.0
NEG_BIG = -1e30

BF = jnp.bfloat16
F32 = jnp.float32
D = 128
HL = 4
KL = 2
NB = 256
NH = 128
NQ = 64
HID = 2048
NCH = 4
W = HID // NCH
VMEM_MAX = 66 * 1024 * 1024 - 2 * 1024 * 1024
MESH = pl.DeviceIdType.MESH
ANY = pl.BlockSpec(memory_space=pl.ANY)
VM = pl.BlockSpec(memory_space=pltpu.VMEM)


def rope_freqs(head_dim):
    inv_freq = 1.0 / (ROPE_THETA ** (np.arange(0, head_dim, 2) / head_dim))
    wavelen = 2.0 * math.pi / inv_freq
    smooth = (ORIG_CTX / wavelen - LOW_FREQ) / (HIGH_FREQ - LOW_FREQ)
    mid_freq = (1.0 - smooth) * inv_freq / ROPE_FACTOR + smooth * inv_freq
    scaled = np.where(wavelen > ORIG_CTX / LOW_FREQ, inv_freq / ROPE_FACTOR, mid_freq)
    scaled = np.where(wavelen < ORIG_CTX / HIGH_FREQ, inv_freq, scaled)
    return np.concatenate([scaled, scaled]).astype(np.float32)[None, :]


def norm32(vals32, gain32):
    inv = lax.rsqrt(jnp.mean(vals32 * vals32, axis=-1, keepdims=True) + NORM_EPS)
    return (vals32 * inv * gain32).astype(BF)


def dot(a, b):
    return jnp.dot(a, b, preferred_element_type=F32)


def dot_nt(a, b):
    return lax.dot_general(a, b, (((1,), (1,)), ((), ())), preferred_element_type=F32)


def attend(lhs, keys, vals, valid):
    first = lax.broadcasted_iota(jnp.int32, (8, D), 0) < HL
    s = [dot_nt(a, k) * (D ** -0.5) for a, k in zip(lhs, keys)]
    s = [jnp.where(ok, x, NEG_BIG) for ok, x in zip(valid, s)]
    m = [jnp.max(x, axis=-1, keepdims=True) for x in s]
    p = [jnp.where(ok, jnp.exp(x - t), 0.0) for ok, x, t in zip(valid, s, m)]
    l = [jnp.sum(x, axis=-1, keepdims=True) for x in p]
    o = [dot(x.astype(BF), v) for x, v in zip(p, vals)]
    return m, l, [jnp.where(first, x[:, :D], x[:, D:]) for x in o]


def pair_lhs(q_ref, b0):
    q16 = q_ref[pl.ds(pl.multiple_of(b0 * 8, 16), 16), :]
    return jnp.concatenate([q16[:8], q16[8:]], axis=1).astype(BF)


def column(vec, first, rows):
    n = vec.shape[1]
    at = lax.broadcasted_iota(jnp.int32, (rows, n), 1) == lax.broadcasted_iota(jnp.int32, (rows, n), 0) + first
    return jnp.sum(jnp.where(at, vec, 0.0), axis=1, keepdims=True)


def spread_heads(ref, heads, start, rows):
    odd = (lax.broadcasted_iota(jnp.int32, (rows, D), 0) % 2) == 1
    for h in range(HL):
        ref[pl.ds(start * 8 + h, rows, stride=8), :] = jnp.where(odd, 0.0, heads[h])
        ref[pl.ds(start * 8 + HL + h, rows, stride=8), :] = jnp.where(odd, heads[h], 0.0)


SR = 16
NS = 8
PRE = 5


def self_kernel(pos_ref, posv_ref, freq_ref, g_ref, hid_hbm, wq_hbm, wk_hbm, wv_hbm, k_hbm, v_hbm,
                ko_hbm, vo_hbm, o_ref, st_ref,
                hid, wq, wk, wv, wsem, kbuf, vbuf, isem, osem, qs, kn, vn):
    T2 = k_hbm.shape[1]
    steps = NB // SR
    first_pos = lax.axis_index("sp") * (T2 // KL)
    loads = [pltpu.make_async_copy(a, b, wsem.at[n])
             for n, (a, b) in enumerate(((hid_hbm, hid), (wq_hbm, wq), (wk_hbm, wk), (wv_hbm, wv)))]
    for cp in loads:
        cp.start()

    def into(i):
        rows, slot = pl.ds(pl.multiple_of(i * SR, SR), SR), i % NS
        return (pltpu.make_async_copy(k_hbm.at[rows], kbuf.at[slot], isem.at[0, slot]),
                pltpu.make_async_copy(v_hbm.at[rows], vbuf.at[slot], isem.at[1, slot]))

    def out_of(i):
        rows, slot = pl.ds(pl.multiple_of(i * SR, SR), SR), i % NS
        return (pltpu.make_async_copy(kbuf.at[slot], ko_hbm.at[rows], osem.at[0, slot]),
                pltpu.make_async_copy(vbuf.at[slot], vo_hbm.at[rows], osem.at[1, slot]))

    for i in range(PRE):
        for cp in into(i):
            cp.start()

    angle = column(posv_ref[...].astype(F32).reshape(1, NB), 0, NB) * freq_ref[...]
    cos, sin = jnp.cos(angle), jnp.sin(angle)
    sin = jnp.where(lax.broadcasted_iota(jnp.int32, (NB, D), 1) < D // 2, -sin, sin)

    def rope(part):
        part = part.astype(BF).astype(F32)
        return (part * cos + pltpu.roll(part, D // 2, 1) * sin).astype(BF).astype(F32)

    loads[0].wait()
    x = norm32(hid[...].astype(F32), g_ref[...].astype(F32).reshape(1, HID))
    loads[1].wait()
    q = dot(x, wq[...])
    spread_heads(qs, [rope(q[:, h * D:(h + 1) * D]) for h in range(HL)], 0, NB)
    loads[2].wait()
    k = dot(x, wk[...])
    loads[3].wait()
    v = dot(x, wv[...])
    for h in range(KL):
        kn[pl.ds(h, NB, stride=KL), :] = rope(k[:, h * D:(h + 1) * D])
        vn[pl.ds(h, NB, stride=KL), :] = v[:, h * D:(h + 1) * D].astype(BF).astype(F32)
    st_ref[...] = jnp.zeros_like(st_ref)

    col = lax.broadcasted_iota(jnp.int32, (8, T2), 1)
    row = lax.broadcasted_iota(jnp.int32, (8, T2), 0)
    tok = col // KL
    head_ok = (col % KL) == ((row % HL) // (HL // KL))
    lane = lax.broadcasted_iota(jnp.int32, (8, D), 1)
    i16 = lax.broadcasted_iota(jnp.int32, (16, D), 0)

    def patch(new_ref, dst_ref, slot, r, b, lp):
        base = pl.multiple_of((jnp.clip(lp, 0, T2 // KL - 1) // 8) * 16, 16)
        fresh = jnp.where(i16 % 2 == 0, new_ref[pl.ds(2 * b, 1), :], new_ref[pl.ds(2 * b + 1, 1), :])
        old = dst_ref[slot, r, pl.ds(base, 16), :].astype(F32)
        dst_ref[slot, r, pl.ds(base, 16), :] = jnp.where(base + i16 - i16 % 2 == 2 * lp, fresh, old).astype(BF)

    def body(i, _):
        slot = i % NS

        @pl.when(i >= NS - PRE)
        def _():
            for cp in out_of(i - (NS - PRE)):
                cp.wait()

        @pl.when(i + PRE < steps)
        def _():
            for cp in into(i + PRE):
                cp.start()

        for cp in into(i):
            cp.wait()
        lps = [pos_ref[i * SR + r] - first_pos for r in range(SR)]
        for r in range(SR):
            patch(kn, kbuf, slot, r, i * SR + r, lps[r])
            patch(vn, vbuf, slot, r, i * SR + r, lps[r])
        pairs = range(SR // 2)
        both = lambda buf, p: jnp.concatenate([buf[slot, 2 * p], buf[slot, 2 * p + 1]], axis=1)
        m, l, o = attend([pair_lhs(qs, i * SR + 2 * p) for p in pairs], [both(kbuf, p) for p in pairs],
                         [both(vbuf, p) for p in pairs],
                         [head_ok & (tok <= jnp.where(row < HL, lps[2 * p], lps[2 * p + 1])) for p in pairs])
        half = i // (NH // SR)
        srow = pl.ds(pl.multiple_of(half * 8, 8), 8)
        st = st_ref[srow, :]
        for p in pairs:
            o_ref[pl.ds(pl.multiple_of(i * SR * HL + 8 * p, 8), 8), :] = o[p]
            at = (i - half * (NH // SR)) * (SR // 2) + p
            st = jnp.where(lane == at, m[p], jnp.where(lane == at + NQ, l[p], st))
        st_ref[srow, :] = st
        for cp in out_of(i):
            cp.start()
        return 0

    lax.fori_loop(0, steps, body, 0)
    for i in range(steps - (NS - PRE), steps):
        for cp in out_of(i):
            cp.wait()


def self_attention(new_pos, g1, hidden, wq, wk, wv, k_self, v_self):
    T2 = k_self.shape[1]
    return pl.pallas_call(
        self_kernel,
        in_specs=[pl.BlockSpec(memory_space=pltpu.SMEM), VM, VM, VM] + [ANY] * 6,
        out_specs=[ANY, ANY, VM, VM],
        scratch_shapes=[pltpu.VMEM(hidden.shape, BF), pltpu.VMEM(wq.shape, BF), pltpu.VMEM(wk.shape, BF),
                        pltpu.VMEM(wv.shape, BF), pltpu.SemaphoreType.DMA((4,)),
                        pltpu.VMEM((NS, SR, T2, D), BF), pltpu.VMEM((NS, SR, T2, D), BF),
                        pltpu.SemaphoreType.DMA((2, NS)), pltpu.SemaphoreType.DMA((2, NS)),
                        pltpu.VMEM((NB * 8, D), F32), pltpu.VMEM((NB * KL, D), F32), pltpu.VMEM((NB * KL, D), F32)],
        out_shape=[jax.ShapeDtypeStruct(k_self.shape, BF), jax.ShapeDtypeStruct(v_self.shape, BF),
                   jax.ShapeDtypeStruct((NB * HL, D), F32), jax.ShapeDtypeStruct((16, D), F32)],
        compiler_params=pltpu.CompilerParams(vmem_limit_bytes=VMEM_MAX),
        name="self_attn",
    )(new_pos, new_pos, jnp.asarray(rope_freqs(D)), g1, hidden, wq, wk, wv, k_self, v_self)


def peers():
    sp, tp = lax.axis_index("sp"), lax.axis_index("tp")
    core = lax.rem(tp, 2)
    return dict(sp=sp, core=core, y={"sp": 1 - sp}, c={"tp": tp + 1 - 2 * core}, x={"tp": lax.rem(tp + 2, 4)})


def entry_barrier(pe):
    barrier = pltpu.get_barrier_semaphore()
    for name in ("y", "c", "x"):
        pl.semaphore_signal(barrier, inc=1, device_id=pe[name], device_id_type=MESH)
    pl.semaphore_wait(barrier, 3)


def rcopy(src, dst, ssem, rsem, dev):
    return pltpu.make_async_remote_copy(src_ref=src, dst_ref=dst, send_sem=ssem, recv_sem=rsem,
                                        device_id=dev, device_id_type=MESH)


def tp_sum(pe, compute, finish, snd, rcv, chip, xr, sems):
    to_core = [rcopy(snd.at[j], rcv.at[j], sems.at[0, j], sems.at[1, j], pe["c"]) for j in range(NCH)]
    to_chip = [rcopy(chip.at[j], xr.at[j], sems.at[2, j], sems.at[3, j], pe["x"]) for j in range(NCH)]
    for j in range(NCH + 1):
        if j < NCH:
            part = compute(j)
            snd[j] = part[NQ:]
            chip[j] = part[:NQ]
            to_core[j].start()
        if j >= 1:
            to_core[j - 1].wait_recv()
            chip[j - 1] = chip[j - 1] + rcv[j - 1]
            to_chip[j - 1].start()
    for j in range(NCH):
        to_chip[j].wait_recv()
        finish(j, chip[j] + xr[j])
    for j in range(NCH):
        to_core[j].wait_send()
        to_chip[j].wait_send()


def share_rows(pe, own, x_ref, snd, rcv, sem):
    snd[...] = own.astype(F32)
    cp = rcopy(snd, rcv, sem.at[0], sem.at[1], pe["c"])
    cp.start()
    x_ref[pl.ds(0, NQ), :] = own
    cp.wait()
    x_ref[pl.ds(NQ, NQ), :] = rcv[...].astype(BF)


def mlp_act(x_ref, wg, wu, act, n_cols):
    step = 512
    for c in range(n_cols // step):
        s = slice(c * step, (c + 1) * step)
        gate = dot(x_ref[...], wg[:, s]).astype(BF).astype(F32)
        up = dot(x_ref[...], wu[:, s]).astype(BF).astype(F32)
        act[:, s] = (gate * jax.nn.sigmoid(gate) * up).astype(BF)


def cols(j):
    return slice(j * W, (j + 1) * W)


def heads_to_lanes(ref, starts, rows):
    parts = [jnp.concatenate([ref[pl.ds(s * HL + h, rows, stride=HL), :] for h in range(HL)], axis=1) for s in starts]
    return jnp.concatenate(parts, axis=0).astype(BF)


CR = 8
NR = 5
RC = NQ // NCH
XB = 2 * RC // CR


def rest_kernel(o_hbm, st_ref, hid_hbm, g2_ref, g3_ref, qn_ref, g4_ref, gates_ref, mask_ref, valid_hbm,
                wo_hbm, wg_hbm, wu_hbm, wd_hbm, wq_hbm, wo2_hbm, wg2_hbm, wu2_hbm, wd2_hbm, k_hbm, v_hbm,
                out_ref,
                wo, wg, wu, wd, wq, wo2, wsem, kbuf, vbuf, ksem, osnd, orcv, sts, str_, ysem, hown, att, valid, cnt,
                qx, xbuf, act, hres, h2, fin, yr, cr, gsem,
                a0, a1, a2, a3, asem, b0, b1, b2, b3, bsem, c0, c1, c2, c3, csem, dsem,
                s0, s1, ssem, t0, t1, tsem, esem):
    pe = peers()
    sp, core = pe["sp"], pe["core"]
    T2 = k_hbm.shape[1]
    half = NH * HL
    blocks = NH // CR

    local = [pltpu.make_async_copy(o_hbm.at[pl.ds(pl.multiple_of((1 - sp) * half, half), half)], osnd, wsem.at[6]),
             pltpu.make_async_copy(o_hbm.at[pl.ds(pl.multiple_of(sp * half, half), half)], att, wsem.at[7]),
             pltpu.make_async_copy(hid_hbm.at[pl.ds(pl.multiple_of(sp * NH + core * NQ, NQ), NQ)], hown, wsem.at[8]),
             pltpu.make_async_copy(valid_hbm.at[pl.ds(pl.multiple_of(sp * NH, NH), NH)], valid, wsem.at[9])]
    pairs = ((wo_hbm, wo), (wg_hbm, wg), (wu_hbm, wu), (wd_hbm, wd), (wq_hbm, wq), (wo2_hbm, wo2))
    loads = [pltpu.make_async_copy(a, b, wsem.at[n]) for n, (a, b) in enumerate(pairs)]
    for cp in local + loads:
        cp.start()

    def block_row(t):
        chunk, of_core, sub = t // XB, (t % XB) // (XB // 2), t % (XB // 2)
        return of_core * NQ + chunk * RC + sub * CR

    def kv_loads(t):
        rows, slot = pl.ds(pl.multiple_of(sp * NH + block_row(t), CR), CR), t % NR
        return (pltpu.make_async_copy(k_hbm.at[rows], kbuf.at[slot], ksem.at[0, slot]),
                pltpu.make_async_copy(v_hbm.at[rows], vbuf.at[slot], ksem.at[1, slot]))

    for t in range(NR):
        for cp in kv_loads(t):
            cp.start()

    entry_barrier(pe)
    both = st_ref[...]
    mine = jnp.where(sp == 0, both[:8], both[8:])
    sts[...] = jnp.where(sp == 0, both[8:], both[:8])
    local[0].wait()
    cp_o = rcopy(osnd, orcv, ysem.at[0], ysem.at[1], pe["y"])
    cp_s = rcopy(sts, str_, ysem.at[2], ysem.at[3], pe["y"])
    cp_s.start()
    cp_o.start()
    for cp in local[1:]:
        cp.wait()
    some = jnp.sum((valid[...] > 0).astype(jnp.int32), axis=1, keepdims=True)
    cnt[...] = jnp.broadcast_to(some, cnt.shape)
    row_scale = column(mask_ref[...].astype(F32).reshape(1, NB), sp * NH + core * NQ, NQ)
    gate0 = jnp.tanh(jnp.full((8, D), gates_ref[0], F32))[0:1, 0:1] * row_scale
    gate1 = jnp.tanh(jnp.full((8, D), gates_ref[1], F32))[0:1, 0:1] * row_scale
    cp_s.wait()
    theirs = str_[...]
    top = jnp.maximum(mine, theirs)
    f1, f2 = jnp.exp(mine - top), jnp.exp(theirs - top)
    den = pltpu.roll(mine, NQ, 1) * f1 + pltpu.roll(theirs, NQ, 1) * f2
    w1, w2 = f1 / den, f2 / den
    cp_o.wait()
    for p in range(NQ):
        s = pl.ds(8 * p, 8)
        att[s, :] = att[s, :] * w1[:, p:p + 1] + orcv[s, :] * w2[:, p:p + 1]
    lhs = heads_to_lanes(att, (core * NQ, (1 - core) * NQ), NQ)
    gain = lambda ref: ref[...].astype(F32).reshape(1, HID)

    loads[0].wait()

    def done1(j, total):
        hres[:, cols(j)] = (hown[:, cols(j)].astype(F32) + total).astype(BF)

    tp_sum(pe, lambda j: dot(lhs, wo[:, cols(j)]), done1, a0, a1, a2, a3, asem)
    share_rows(pe, norm32(hres[...].astype(F32), gain(g2_ref)), xbuf, s0, s1, ssem)
    loads[1].wait()
    loads[2].wait()
    mlp_act(xbuf, wg, wu, act, act.shape[1])
    loads[3].wait()

    def done2(j, total):
        if j == 0:
            for cp in loads2:
                cp.start()
        h2[:, cols(j)] = (hres[:, cols(j)].astype(F32) + total).astype(BF)

    loads2 = [pltpu.make_async_copy(a, b, wsem.at[1 + n])
              for n, (a, b) in enumerate(((wg2_hbm, wg), (wu2_hbm, wu), (wd2_hbm, wd)))]
    tp_sum(pe, lambda j: dot(act[...], wd[:, cols(j)]), done2, b0, b1, b2, b3, bsem)
    share_rows(pe, norm32(h2[...].astype(F32), gain(g3_ref)), xbuf, t0, t1, tsem)
    loads[4].wait()
    q = dot(xbuf[...], wq[...])
    qgain = qn_ref[...].astype(F32).reshape(1, D)
    heads = [norm32(q[:, h * D:(h + 1) * D].astype(BF).astype(F32), qgain).astype(F32) for h in range(HL)]
    spread_heads(qx, [h[:NQ] for h in heads], core * NQ, NQ)
    spread_heads(qx, [h[NQ:] for h in heads], (1 - core) * NQ, NQ)
    loads[5].wait()

    col = lax.broadcasted_iota(jnp.int32, (8, T2), 1)
    row = lax.broadcasted_iota(jnp.int32, (8, T2), 0)
    tok = col // KL
    head_ok = (col % KL) == ((row % HL) // (HL // KL))
    first = lax.broadcasted_iota(jnp.int32, (8, D), 0) < HL

    def block(t, _):
        slot = t % NR
        r0 = pl.multiple_of(block_row(t), CR)
        for cp in kv_loads(t):
            cp.wait()
        ps = range(CR // 2)
        lane_pair = lambda buf, p: jnp.concatenate([buf[slot, 2 * p], buf[slot, 2 * p + 1]], axis=1)
        n8 = cnt[pl.ds(r0, CR), :]
        limit = [jnp.concatenate([jnp.where(first, n8[2 * p:2 * p + 1], n8[2 * p + 1:2 * p + 2])] * (T2 // D), axis=1)
                 for p in ps]
        m, l, o = attend([pair_lhs(qx, r0 + 2 * p) for p in ps], [lane_pair(kbuf, p) for p in ps],
                         [lane_pair(vbuf, p) for p in ps], [head_ok & (tok < n) for n in limit])
        for p in ps:
            att[pl.ds(pl.multiple_of(r0 * HL + 8 * p, 8), 8), :] = o[p] / l[p]

        @pl.when(t + NR < blocks)
        def _():
            for cp in kv_loads(t + NR):
                cp.start()
        return 0

    to_core = [rcopy(c0.at[j], c1.at[j], csem.at[0, j], csem.at[1, j], pe["c"]) for j in range(NCH)]
    to_chip = [rcopy(c2.at[j], c3.at[j], csem.at[2, j], csem.at[3, j], pe["x"]) for j in range(NCH)]
    share = [rcopy(s0.at[pl.ds(j * RC, RC)], s1.at[pl.ds(j * RC, RC)], dsem.at[0, j], dsem.at[1, j], pe["c"])
             for j in range(NCH)]

    def pass_chip(j):
        to_core[j].wait_recv()
        c2[j] = c2[j] + c1[j]
        to_chip[j].start()

    def close(j):
        mine = slice(j * RC, (j + 1) * RC)
        to_chip[j].wait_recv()
        hres[mine, :] = (h2[mine, :].astype(F32) + gate0[mine] * (c2[j] + c3[j])).astype(BF)
        own = norm32(hres[mine, :].astype(F32), gain(g4_ref))
        s0[mine, :] = own.astype(F32)
        share[j].start()
        xbuf[mine, :] = own

    for j in range(NCH):
        lax.fori_loop(j * XB, j * XB + 1, block, 0)
        if j >= 1:
            pass_chip(j - 1)
        lax.fori_loop(j * XB + 1, (j + 1) * XB, block, 0)
        lhs = heads_to_lanes(att, (core * NQ + j * RC, (1 - core) * NQ + j * RC), RC)
        for n in range(NCH):
            part = dot(lhs, wo2[:, cols(n)])
            c0[j, :, cols(n)] = part[RC:]
            c2[j, :, cols(n)] = part[:RC]
        to_core[j].start()
        if j >= 1:
            close(j - 1)
    pass_chip(NCH - 1)
    close(NCH - 1)
    for j in range(NCH):
        share[j].wait_recv()
        xbuf[pl.ds(NQ + j * RC, RC), :] = s1[pl.ds(j * RC, RC), :].astype(BF)
    for j in range(NCH):
        to_core[j].wait_send()
        to_chip[j].wait_send()
        share[j].wait_send()
    for cp in loads2[:2]:
        cp.wait()
    mlp_act(xbuf, wg, wu, act, act.shape[1])
    loads2[2].wait()

    to_y = [rcopy(fin.at[j], yr.at[j], gsem.at[0, j], gsem.at[1, j], pe["y"]) for j in range(NCH)]
    to_c = [rcopy(fin.at[j], cr.at[0, j], gsem.at[2, j], gsem.at[3, j], pe["c"]) for j in range(NCH)]
    pass_c = [rcopy(yr.at[j], cr.at[1, j], gsem.at[4, j], gsem.at[5, j], pe["c"]) for j in range(NCH)]

    def rows(of_half, of_core):
        return pl.ds(pl.multiple_of(of_half * NH + of_core * NQ, NQ), NQ)

    def done4(j, total):
        res = (hres[:, cols(j)].astype(F32) + gate1 * total).astype(BF)
        out_ref[rows(sp, core), cols(j)] = res
        fin[j] = res.astype(F32)
        to_y[j].start()
        to_c[j].start()
        if j >= 1:
            to_y[j - 1].wait_recv()
            pass_c[j - 1].start()

    tp_sum(pe, lambda j: dot(act[...], wd[:, cols(j)]), done4, a0, a1, a2, a3, esem)
    to_y[NCH - 1].wait_recv()
    pass_c[NCH - 1].start()
    for j in range(NCH):
        out_ref[rows(1 - sp, core), cols(j)] = yr[j].astype(BF)
        to_c[j].wait_recv()
        out_ref[rows(sp, 1 - core), cols(j)] = cr[0, j].astype(BF)
    for j in range(NCH):
        pass_c[j].wait_recv()
        out_ref[rows(1 - sp, 1 - core), cols(j)] = cr[1, j].astype(BF)
    for j in range(NCH):
        to_y[j].wait_send()
        to_c[j].wait_send()
        pass_c[j].wait_send()


def rest_of_step(o, st, hidden, g2, g3, qn, g4, gates, mask, xvalid, ws, k_cross, v_cross):
    wo, wg, wu, wd, wq, wo2 = ws[:6]
    F = wg.shape[1]
    T2 = k_cross.shape[1]
    dma = pltpu.SemaphoreType.DMA
    sum_bufs = [pltpu.VMEM((NCH, NQ, W), F32)] * 4 + [dma((4, NCH))]
    share_bufs = [pltpu.VMEM((NQ, HID), F32)] * 2 + [dma((2,))]
    return pl.pallas_call(
        rest_kernel,
        in_specs=[ANY, VM, ANY, VM, VM, VM, VM, pl.BlockSpec(memory_space=pltpu.SMEM), VM] + [ANY] * 12,
        out_specs=VM,
        out_shape=jax.ShapeDtypeStruct((NB, HID), BF),
        scratch_shapes=[pltpu.VMEM(w.shape, BF) for w in (wo, wg, wu, wd, wq, wo2)] + [
            dma((10,)), pltpu.VMEM((NR, CR, T2, D), BF), pltpu.VMEM((NR, CR, T2, D), BF), dma((2, NR)),
            pltpu.VMEM((NH * HL, D), F32), pltpu.VMEM((NH * HL, D), F32), pltpu.VMEM((8, D), F32),
            pltpu.VMEM((8, D), F32), dma((4,)), pltpu.VMEM((NQ, HID), BF), pltpu.VMEM((NH * HL, D), F32),
            pltpu.VMEM((NH, xvalid.shape[1]), jnp.int32), pltpu.VMEM((NH, D), jnp.int32),
            pltpu.VMEM((NH * 8, D), F32), pltpu.VMEM((NH, HID), BF), pltpu.VMEM((NH, F), BF),
            pltpu.VMEM((NQ, HID), BF), pltpu.VMEM((NQ, HID), BF), pltpu.VMEM((NCH, NQ, W), F32),
            pltpu.VMEM((NCH, NQ, W), F32), pltpu.VMEM((2, NCH, NQ, W), F32), dma((6, NCH))]
        + sum_bufs + sum_bufs + [pltpu.VMEM((NCH, RC, HID), F32)] * 4 + [dma((4, NCH)), dma((2, NCH))]
        + share_bufs + share_bufs + [dma((4, NCH))],
        compiler_params=pltpu.CompilerParams(collective_id=0, has_side_effects=True, vmem_limit_bytes=VMEM_MAX),
        name="rest_of_step",
    )(o, st, hidden, g2, g3, qn, g4, gates, mask, xvalid, *ws, k_cross, v_cross)


def solution(mesh):
    cache_spec = P('dp', 'sp', 'tp', None)
    cross_spec = P('dp', None, 'tp', None)
    row_spec = P('dp', None)
    vec_spec = P('dp')
    full_spec = P(None)
    col_spec = P(None, 'tp')
    split_rows = P('tp', None)
    in_specs = (row_spec, vec_spec, cache_spec, cache_spec, cross_spec, cross_spec, row_spec, vec_spec,
                full_spec, col_spec, col_spec, col_spec, split_rows, full_spec, col_spec, col_spec, split_rows,
                full_spec, col_spec, full_spec, split_rows, full_spec, full_spec, col_spec, col_spec, split_rows)
    out_specs = (row_spec, cache_spec, cache_spec)

    def local_step(hidden, new_pos, k_self, v_self, k_cross, v_cross, xvalid, rowmask,
                   self_attn_norm, self_wq, self_wk, self_wv, self_wo, self_mlp_norm,
                   self_wgate, self_wup, self_wdown, cross_attn_norm, cross_wq, cross_qnorm,
                   cross_wo, cross_gates, cross_mlp_norm, cross_wgate, cross_wup, cross_wdown):
        flat = lambda a: a.reshape(a.shape[0], a.shape[1] * a.shape[2], a.shape[3])
        k_out, v_out, o, st = self_attention(new_pos, self_attn_norm, hidden, self_wq, self_wk, self_wv,
                                             flat(k_self), flat(v_self))
        weights = (self_wo, self_wgate, self_wup, self_wdown, cross_wq, cross_wo, cross_wgate, cross_wup, cross_wdown)
        h4 = rest_of_step(o, st, hidden, self_mlp_norm, cross_attn_norm, cross_qnorm, cross_mlp_norm, cross_gates,
                          rowmask, xvalid, weights, flat(k_cross), flat(v_cross))
        return h4, k_out.reshape(k_self.shape), v_out.reshape(v_self.shape)

    return jax.shard_map(local_step, mesh=mesh, in_specs=in_specs, out_specs=out_specs, check_vma=False)
```

```python
import functools
import math
import numpy as np
import jax
import jax.numpy as jnp
from jax import lax
from jax.experimental import pallas as pl
from jax.experimental.pallas import tpu as pltpu
from jax.sharding import PartitionSpec as P

NORM_EPS = 1e-5
ROPE_THETA = 500000.0
ROPE_FACTOR = 8.0
LOW_FREQ = 1.0
HIGH_FREQ = 4.0
ORIG_CTX = 8192.0
NEG_BIG = -1e30

BF = jnp.bfloat16
F32 = jnp.float32
D = 128
HL = 4
KL = 2
NB = 256
NH = 128
NQ = 64
HID = 2048
HQ = NQ // 2
NCH = 4
W = HID // NCH
VMEM_MAX = 66 * 1024 * 1024 - 2 * 1024 * 1024
MESH = pl.DeviceIdType.MESH
ANY = pl.BlockSpec(memory_space=pl.ANY)
VM = pl.BlockSpec(memory_space=pltpu.VMEM)


def rope_freqs(head_dim):
    inv_freq = 1.0 / (ROPE_THETA ** (np.arange(0, head_dim, 2) / head_dim))
    wavelen = 2.0 * math.pi / inv_freq
    smooth = (ORIG_CTX / wavelen - LOW_FREQ) / (HIGH_FREQ - LOW_FREQ)
    mid_freq = (1.0 - smooth) * inv_freq / ROPE_FACTOR + smooth * inv_freq
    scaled = np.where(wavelen > ORIG_CTX / LOW_FREQ, inv_freq / ROPE_FACTOR, mid_freq)
    scaled = np.where(wavelen < ORIG_CTX / HIGH_FREQ, inv_freq, scaled)
    return np.concatenate([scaled, scaled]).astype(np.float32)[None, :]


def norm32(vals32, gain32):
    inv = lax.rsqrt(jnp.mean(vals32 * vals32, axis=-1, keepdims=True) + NORM_EPS)
    return (vals32 * inv * gain32).astype(BF)


def dot(a, b):
    return jnp.dot(a, b, preferred_element_type=F32)


def dot_nt(a, b):
    return lax.dot_general(a, b, (((1,), (1,)), ((), ())), preferred_element_type=F32)


def attend(lhs, keys, vals, valid):
    first = lax.broadcasted_iota(jnp.int32, (8, D), 0) < HL
    s = [dot_nt(a, k) * (D ** -0.5) for a, k in zip(lhs, keys)]
    s = [jnp.where(ok, x, NEG_BIG) for ok, x in zip(valid, s)]
    m = [jnp.max(x, axis=-1, keepdims=True) for x in s]
    p = [jnp.where(ok, jnp.exp(x - t), 0.0) for ok, x, t in zip(valid, s, m)]
    l = [jnp.sum(x, axis=-1, keepdims=True) for x in p]
    o = [dot(x.astype(BF), v) for x, v in zip(p, vals)]
    return m, l, [jnp.where(first, x[:, :D], x[:, D:]) for x in o]


def pair_lhs(q_ref, b0):
    q16 = q_ref[pl.ds(pl.multiple_of(b0 * 8, 16), 16), :]
    return jnp.concatenate([q16[:8], q16[8:]], axis=1).astype(BF)


def column(vec, first, rows):
    n = vec.shape[1]
    at = lax.broadcasted_iota(jnp.int32, (rows, n), 1) == lax.broadcasted_iota(jnp.int32, (rows, n), 0) + first
    return jnp.sum(jnp.where(at, vec, 0.0), axis=1, keepdims=True)


def spread_heads(ref, heads, start, rows):
    odd = (lax.broadcasted_iota(jnp.int32, (rows, D), 0) % 2) == 1
    for h in range(HL):
        ref[pl.ds(start * 8 + h, rows, stride=8), :] = jnp.where(odd, 0.0, heads[h])
        ref[pl.ds(start * 8 + HL + h, rows, stride=8), :] = jnp.where(odd, heads[h], 0.0)


SR = 16
NS = 8
PRE = 5


def self_kernel(pos_ref, posv_ref, freq_ref, g_ref, hid_hbm, wq_hbm, wk_hbm, wv_hbm, k_hbm, v_hbm,
                ko_hbm, vo_hbm, o_ref, st_ref,
                hid, wq, wk, wv, wsem, kbuf, vbuf, isem, osem, qs, kn, vn):
    T2 = k_hbm.shape[1]
    steps = NB // SR
    first_pos = lax.axis_index("sp") * (T2 // KL)
    loads = [pltpu.make_async_copy(a, b, wsem.at[n])
             for n, (a, b) in enumerate(((hid_hbm, hid), (wq_hbm, wq), (wk_hbm, wk), (wv_hbm, wv)))]
    for cp in loads:
        cp.start()

    def into(i):
        rows, slot = pl.ds(pl.multiple_of(i * SR, SR), SR), i % NS
        return (pltpu.make_async_copy(k_hbm.at[rows], kbuf.at[slot], isem.at[0, slot]),
                pltpu.make_async_copy(v_hbm.at[rows], vbuf.at[slot], isem.at[1, slot]))

    def out_of(i):
        rows, slot = pl.ds(pl.multiple_of(i * SR, SR), SR), i % NS
        return (pltpu.make_async_copy(kbuf.at[slot], ko_hbm.at[rows], osem.at[0, slot]),
                pltpu.make_async_copy(vbuf.at[slot], vo_hbm.at[rows], osem.at[1, slot]))

    for i in range(PRE):
        for cp in into(i):
            cp.start()

    angle = column(posv_ref[...].astype(F32).reshape(1, NB), 0, NB) * freq_ref[...]
    cos, sin = jnp.cos(angle), jnp.sin(angle)
    sin = jnp.where(lax.broadcasted_iota(jnp.int32, (NB, D), 1) < D // 2, -sin, sin)

    def rope(part):
        part = part.astype(BF).astype(F32)
        return (part * cos + pltpu.roll(part, D // 2, 1) * sin).astype(BF).astype(F32)

    loads[0].wait()
    x = norm32(hid[...].astype(F32), g_ref[...].astype(F32).reshape(1, HID))
    loads[1].wait()
    q = dot(x, wq[...])
    spread_heads(qs, [rope(q[:, h * D:(h + 1) * D]) for h in range(HL)], 0, NB)
    loads[2].wait()
    k = dot(x, wk[...])
    loads[3].wait()
    v = dot(x, wv[...])
    for h in range(KL):
        kn[pl.ds(h, NB, stride=KL), :] = rope(k[:, h * D:(h + 1) * D])
        vn[pl.ds(h, NB, stride=KL), :] = v[:, h * D:(h + 1) * D].astype(BF).astype(F32)
    st_ref[...] = jnp.zeros_like(st_ref)

    col = lax.broadcasted_iota(jnp.int32, (8, T2), 1)
    row = lax.broadcasted_iota(jnp.int32, (8, T2), 0)
    tok = col // KL
    head_ok = (col % KL) == ((row % HL) // (HL // KL))
    lane = lax.broadcasted_iota(jnp.int32, (8, D), 1)
    i16 = lax.broadcasted_iota(jnp.int32, (16, D), 0)

    def patch(new_ref, dst_ref, slot, r, b, lp):
        base = pl.multiple_of((jnp.clip(lp, 0, T2 // KL - 1) // 8) * 16, 16)
        fresh = jnp.where(i16 % 2 == 0, new_ref[pl.ds(2 * b, 1), :], new_ref[pl.ds(2 * b + 1, 1), :])
        old = dst_ref[slot, r, pl.ds(base, 16), :].astype(F32)
        dst_ref[slot, r, pl.ds(base, 16), :] = jnp.where(base + i16 - i16 % 2 == 2 * lp, fresh, old).astype(BF)

    def body(i, _):
        slot = i % NS

        @pl.when(i >= NS - PRE)
        def _():
            for cp in out_of(i - (NS - PRE)):
                cp.wait()

        @pl.when(i + PRE < steps)
        def _():
            for cp in into(i + PRE):
                cp.start()

        for cp in into(i):
            cp.wait()
        lps = [pos_ref[i * SR + r] - first_pos for r in range(SR)]
        for r in range(SR):
            patch(kn, kbuf, slot, r, i * SR + r, lps[r])
            patch(vn, vbuf, slot, r, i * SR + r, lps[r])
        pairs = range(SR // 2)
        both = lambda buf, p: jnp.concatenate([buf[slot, 2 * p], buf[slot, 2 * p + 1]], axis=1)
        m, l, o = attend([pair_lhs(qs, i * SR + 2 * p) for p in pairs], [both(kbuf, p) for p in pairs],
                         [both(vbuf, p) for p in pairs],
                         [head_ok & (tok <= jnp.where(row < HL, lps[2 * p], lps[2 * p + 1])) for p in pairs])
        half = i // (NH // SR)
        srow = pl.ds(pl.multiple_of(half * 8, 8), 8)
        st = st_ref[srow, :]
        for p in pairs:
            o_ref[pl.ds(pl.multiple_of(i * SR * HL + 8 * p, 8), 8), :] = o[p]
            at = (i - half * (NH // SR)) * (SR // 2) + p
            st = jnp.where(lane == at, m[p], jnp.where(lane == at + NQ, l[p], st))
        st_ref[srow, :] = st
        for cp in out_of(i):
            cp.start()
        return 0

    lax.fori_loop(0, steps, body, 0)
    for i in range(steps - (NS - PRE), steps):
        for cp in out_of(i):
            cp.wait()


def self_attention(new_pos, g1, hidden, wq, wk, wv, k_self, v_self):
    T2 = k_self.shape[1]
    return pl.pallas_call(
        self_kernel,
        in_specs=[pl.BlockSpec(memory_space=pltpu.SMEM), VM, VM, VM] + [ANY] * 6,
        out_specs=[ANY, ANY, VM, VM],
        scratch_shapes=[pltpu.VMEM(hidden.shape, BF), pltpu.VMEM(wq.shape, BF), pltpu.VMEM(wk.shape, BF),
                        pltpu.VMEM(wv.shape, BF), pltpu.SemaphoreType.DMA((4,)),
                        pltpu.VMEM((NS, SR, T2, D), BF), pltpu.VMEM((NS, SR, T2, D), BF),
                        pltpu.SemaphoreType.DMA((2, NS)), pltpu.SemaphoreType.DMA((2, NS)),
                        pltpu.VMEM((NB * 8, D), F32), pltpu.VMEM((NB * KL, D), F32), pltpu.VMEM((NB * KL, D), F32)],
        out_shape=[jax.ShapeDtypeStruct(k_self.shape, BF), jax.ShapeDtypeStruct(v_self.shape, BF),
                   jax.ShapeDtypeStruct((NB * HL, D), F32), jax.ShapeDtypeStruct((16, D), F32)],
        compiler_params=pltpu.CompilerParams(vmem_limit_bytes=VMEM_MAX),
        name="self_attn",
    )(new_pos, new_pos, jnp.asarray(rope_freqs(D)), g1, hidden, wq, wk, wv, k_self, v_self)


def peers():
    sp, tp = lax.axis_index("sp"), lax.axis_index("tp")
    core = lax.rem(tp, 2)
    return dict(sp=sp, core=core, y={"sp": 1 - sp}, c={"tp": tp + 1 - 2 * core}, x={"tp": lax.rem(tp + 2, 4)})


def entry_barrier(pe):
    barrier = pltpu.get_barrier_semaphore()
    for name in ("y", "c", "x"):
        pl.semaphore_signal(barrier, inc=1, device_id=pe[name], device_id_type=MESH)
    pl.semaphore_wait(barrier, 3)


def rcopy(src, dst, ssem, rsem, dev):
    return pltpu.make_async_remote_copy(src_ref=src, dst_ref=dst, send_sem=ssem, recv_sem=rsem,
                                        device_id=dev, device_id_type=MESH)


class TpSum:
    def __init__(self, pe, half, bufs):
        snd, rcv, chip, xr, sems = bufs
        self.snd, self.rcv, self.chip, self.xr = (b.at[half] for b in (snd, rcv, chip, xr))
        at = lambda n, j: sems.at[half, n, j]
        self.to_core = [rcopy(self.snd.at[j], self.rcv.at[j], at(0, j), at(1, j), pe["c"]) for j in range(NCH)]
        self.to_chip = [rcopy(self.chip.at[j], self.xr.at[j], at(2, j), at(3, j), pe["x"]) for j in range(NCH)]

    def start(self, compute):
        for j in range(NCH + 1):
            if j < NCH:
                part = compute(j)
                self.snd[j] = part[HQ:]
                self.chip[j] = part[:HQ]
                self.to_core[j].start()
            if j >= 1:
                self.to_core[j - 1].wait_recv()
                self.chip[j - 1] = self.chip[j - 1] + self.rcv[j - 1]
                self.to_chip[j - 1].start()

    def close(self, finish):
        for j in range(NCH):
            self.to_chip[j].wait_recv()
            finish(j, self.chip[j] + self.xr[j])
        for j in range(NCH):
            self.to_core[j].wait_send()
            self.to_chip[j].wait_send()


class Share:
    def __init__(self, pe, half, x_ref, snd, rcv, sems):
        rows = pl.ds(half * HQ, HQ)
        self.snd, self.rcv, self.x = snd.at[rows], rcv.at[rows], x_ref.at[half]
        self.copy = rcopy(self.snd, self.rcv, sems.at[0, half], sems.at[1, half], pe["c"])

    def start(self, own):
        self.snd[...] = own.astype(F32)
        self.copy.start()
        self.x[pl.ds(0, HQ), :] = own

    def finish(self):
        self.copy.wait()
        self.x[pl.ds(HQ, HQ), :] = self.rcv[...].astype(BF)


def mlp_act(x_ref, wg, wu, act, n_cols):
    step = 512
    for c in range(n_cols // step):
        s = slice(c * step, (c + 1) * step)
        gate = dot(x_ref[...], wg[:, s]).astype(BF).astype(F32)
        up = dot(x_ref[...], wu[:, s]).astype(BF).astype(F32)
        act[:, s] = (gate * jax.nn.sigmoid(gate) * up).astype(BF)


def cols(j):
    return slice(j * W, (j + 1) * W)


def heads_to_lanes(ref, starts, rows):
    parts = [jnp.concatenate([ref[pl.ds(s * HL + h, rows, stride=HL), :] for h in range(HL)], axis=1) for s in starts]
    return jnp.concatenate(parts, axis=0).astype(BF)


CR = 8
NR = 5
RC = NQ // NCH
XB = 2 * RC // CR


def rest_kernel(o_hbm, st_ref, hid_hbm, g2_ref, g3_ref, qn_ref, g4_ref, gates_ref, mask_ref, valid_hbm,
                wo_hbm, wg_hbm, wu_hbm, wd_hbm, wq_hbm, wo2_hbm, wg2_hbm, wu2_hbm, wd2_hbm, k_hbm, v_hbm,
                out_ref,
                wo, wg, wu, wd, wq, wo2, wsem, kbuf, vbuf, ksem, osnd, orcv, sts, str_, ysem, hown, att, valid, cnt,
                qx, xbuf, act, hres, h2, fin, yr, cr, gsem,
                a0, a1, a2, a3, asem, b0, b1, b2, b3, bsem, c0, c1, c2, c3, csem, dsem,
                s0, s1, ssem, t0, t1, tsem, esem):
    pe = peers()
    sp, core = pe["sp"], pe["core"]
    T2 = k_hbm.shape[1]
    half = NH * HL
    blocks = NH // CR

    local = [pltpu.make_async_copy(o_hbm.at[pl.ds(pl.multiple_of((1 - sp) * half, half), half)], osnd, wsem.at[6]),
             pltpu.make_async_copy(o_hbm.at[pl.ds(pl.multiple_of(sp * half, half), half)], att, wsem.at[7]),
             pltpu.make_async_copy(hid_hbm.at[pl.ds(pl.multiple_of(sp * NH + core * NQ, NQ), NQ)], hown, wsem.at[8]),
             pltpu.make_async_copy(valid_hbm.at[pl.ds(pl.multiple_of(sp * NH, NH), NH)], valid, wsem.at[9])]
    pairs = ((wo_hbm, wo), (wg_hbm, wg), (wu_hbm, wu), (wd_hbm, wd), (wq_hbm, wq), (wo2_hbm, wo2))
    loads = [pltpu.make_async_copy(a, b, wsem.at[n]) for n, (a, b) in enumerate(pairs)]
    for cp in local + loads:
        cp.start()

    def block_row(t):
        chunk, of_core, sub = t // XB, (t % XB) // (XB // 2), t % (XB // 2)
        return of_core * NQ + chunk * RC + sub * CR

    def kv_loads(t):
        rows, slot = pl.ds(pl.multiple_of(sp * NH + block_row(t), CR), CR), t % NR
        return (pltpu.make_async_copy(k_hbm.at[rows], kbuf.at[slot], ksem.at[0, slot]),
                pltpu.make_async_copy(v_hbm.at[rows], vbuf.at[slot], ksem.at[1, slot]))

    for t in range(NR):
        for cp in kv_loads(t):
            cp.start()

    entry_barrier(pe)
    both = st_ref[...]
    mine = jnp.where(sp == 0, both[:8], both[8:])
    sts[...] = jnp.where(sp == 0, both[8:], both[:8])
    local[0].wait()
    cp_s = rcopy(sts, str_, ysem.at[0, 4], ysem.at[1, 4], pe["y"])
    cp_s.start()

    def quarter(h, c):
        rows = pl.ds((c * NQ + h * HQ) * HL, HQ * HL)
        return rcopy(osnd.at[rows], orcv.at[rows], ysem.at[0, 2 * h + c], ysem.at[1, 2 * h + c], pe["y"])

    quarters = [quarter(h, c) for h in range(2) for c in range(2)]
    for cp in quarters:
        cp.start()
    for cp in local[1:]:
        cp.wait()
    some = jnp.sum((valid[...] > 0).astype(jnp.int32), axis=1, keepdims=True)
    cnt[...] = jnp.broadcast_to(some, cnt.shape)
    row_scale = column(mask_ref[...].astype(F32).reshape(1, NB), sp * NH + core * NQ, NQ)
    gate0 = jnp.tanh(jnp.full((8, D), gates_ref[0], F32))[0:1, 0:1] * row_scale
    gate1 = jnp.tanh(jnp.full((8, D), gates_ref[1], F32))[0:1, 0:1] * row_scale
    gain = lambda ref: ref[...].astype(F32).reshape(1, HID)
    owned = [slice(h * HQ, (h + 1) * HQ) for h in range(2)]
    sum1 = [TpSum(pe, h, (a0, a1, a2, a3, asem)) for h in range(2)]
    sum2 = [TpSum(pe, h, (b0, b1, b2, b3, bsem)) for h in range(2)]
    sum4 = [TpSum(pe, h, (a0, a1, a2, a3, esem)) for h in range(2)]
    share1 = [Share(pe, h, xbuf, s0, s1, ssem) for h in range(2)]
    share2 = [Share(pe, h, xbuf, t0, t1, tsem) for h in range(2)]

    cp_s.wait()
    theirs = str_[...]
    top = jnp.maximum(mine, theirs)
    f1, f2 = jnp.exp(mine - top), jnp.exp(theirs - top)
    den = pltpu.roll(mine, NQ, 1) * f1 + pltpu.roll(theirs, NQ, 1) * f2
    w1, w2 = f1 / den, f2 / den

    def attn_out(h):
        for c in range(2):
            quarters[2 * h + c].wait()
            for p in range((c * NQ + h * HQ) // 2, (c * NQ + h * HQ + HQ) // 2):
                s = pl.ds(8 * p, 8)
                att[s, :] = att[s, :] * w1[:, p:p + 1] + orcv[s, :] * w2[:, p:p + 1]
        lhs = heads_to_lanes(att, (core * NQ + h * HQ, (1 - core) * NQ + h * HQ), HQ)
        sum1[h].start(lambda j: dot(lhs, wo[:, cols(j)]))

    def close1(h):
        def done(j, total):
            hres[owned[h], cols(j)] = (hown[owned[h], cols(j)].astype(F32) + total).astype(BF)

        sum1[h].close(done)
        share1[h].start(norm32(hres[owned[h], :].astype(F32), gain(g2_ref)))

    def mlp(h, total):
        mlp_act(xbuf.at[h], wg, wu, act.at[h], act.shape[2])
        total.start(lambda j: dot(act[h], wd[:, cols(j)]))

    def close2(h):
        def done(j, total):
            h2[owned[h], cols(j)] = (hres[owned[h], cols(j)].astype(F32) + total).astype(BF)

        sum2[h].close(done)
        share2[h].start(norm32(h2[owned[h], :].astype(F32), gain(g3_ref)))

    def cross_q(h):
        share2[h].finish()
        q = dot(xbuf[h], wq[...])
        qgain = qn_ref[...].astype(F32).reshape(1, D)
        heads = [norm32(q[:, n * D:(n + 1) * D].astype(BF).astype(F32), qgain).astype(F32) for n in range(HL)]
        spread_heads(qx, [x[:HQ] for x in heads], core * NQ + h * HQ, HQ)
        spread_heads(qx, [x[HQ:] for x in heads], (1 - core) * NQ + h * HQ, HQ)

    loads[0].wait()
    attn_out(0)
    attn_out(1)
    close1(0)
    share1[0].finish()
    for cp in loads[1:4]:
        cp.wait()
    mlp(0, sum2[0])
    close1(1)
    share1[1].finish()
    mlp(1, sum2[1])
    loads2 = [pltpu.make_async_copy(a, b, wsem.at[1 + n])
              for n, (a, b) in enumerate(((wg2_hbm, wg), (wu2_hbm, wu), (wd2_hbm, wd)))]
    for cp in loads2:
        cp.start()
    close2(0)
    loads[4].wait()
    cross_q(0)
    loads[5].wait()

    col = lax.broadcasted_iota(jnp.int32, (8, T2), 1)
    row = lax.broadcasted_iota(jnp.int32, (8, T2), 0)
    tok = col // KL
    head_ok = (col % KL) == ((row % HL) // (HL // KL))
    first = lax.broadcasted_iota(jnp.int32, (8, D), 0) < HL

    def block(t, _):
        slot = t % NR
        r0 = pl.multiple_of(block_row(t), CR)
        for cp in kv_loads(t):
            cp.wait()
        ps = range(CR // 2)
        lane_pair = lambda buf, p: jnp.concatenate([buf[slot, 2 * p], buf[slot, 2 * p + 1]], axis=1)
        n8 = cnt[pl.ds(r0, CR), :]
        limit = [jnp.concatenate([jnp.where(first, n8[2 * p:2 * p + 1], n8[2 * p + 1:2 * p + 2])] * (T2 // D), axis=1)
                 for p in ps]
        m, l, o = attend([pair_lhs(qx, r0 + 2 * p) for p in ps], [lane_pair(kbuf, p) for p in ps],
                         [lane_pair(vbuf, p) for p in ps], [head_ok & (tok < n) for n in limit])
        for p in ps:
            att[pl.ds(pl.multiple_of(r0 * HL + 8 * p, 8), 8), :] = o[p] / l[p]

        @pl.when(t + NR < blocks)
        def _():
            for cp in kv_loads(t + NR):
                cp.start()
        return 0

    to_core = [rcopy(c0.at[j], c1.at[j], csem.at[0, j], csem.at[1, j], pe["c"]) for j in range(NCH)]
    to_chip = [rcopy(c2.at[j], c3.at[j], csem.at[2, j], csem.at[3, j], pe["x"]) for j in range(NCH)]
    share = [rcopy(s0.at[pl.ds(j * RC, RC)], s1.at[pl.ds(j * RC, RC)], dsem.at[0, j], dsem.at[1, j], pe["c"])
             for j in range(NCH)]

    def pass_chip(j):
        to_core[j].wait_recv()
        c2[j] = c2[j] + c1[j]
        to_chip[j].start()

    def close3(j):
        mine = slice(j * RC, (j + 1) * RC)
        to_chip[j].wait_recv()
        hres[mine, :] = (h2[mine, :].astype(F32) + gate0[mine] * (c2[j] + c3[j])).astype(BF)
        own = norm32(hres[mine, :].astype(F32), gain(g4_ref))
        s0[mine, :] = own.astype(F32)
        share[j].start()
        xbuf[j // 2, pl.ds((j % 2) * RC, RC), :] = own

    def shared3(j):
        share[j].wait_recv()
        xbuf[j // 2, pl.ds(HQ + (j % 2) * RC, RC), :] = s1[pl.ds(j * RC, RC), :].astype(BF)

    def cross_out(j):
        lhs = heads_to_lanes(att, (core * NQ + j * RC, (1 - core) * NQ + j * RC), RC)
        for n in range(NCH):
            part = dot(lhs, wo2[:, cols(n)])
            c0[j, :, cols(n)] = part[RC:]
            c2[j, :, cols(n)] = part[:RC]
        to_core[j].start()

    to_y = [[rcopy(fin.at[h, j], yr.at[h, j], gsem.at[h, 0, j], gsem.at[h, 1, j], pe["y"]) for j in range(NCH)]
            for h in range(2)]
    to_c = [[rcopy(fin.at[h, j], cr.at[0, h, j], gsem.at[h, 2, j], gsem.at[h, 3, j], pe["c"]) for j in range(NCH)]
            for h in range(2)]
    pass_c = [[rcopy(yr.at[h, j], cr.at[1, h, j], gsem.at[h, 4, j], gsem.at[h, 5, j], pe["c"]) for j in range(NCH)]
              for h in range(2)]

    def rows(of_sp, of_core, h):
        return pl.ds(pl.multiple_of(of_sp * NH + of_core * NQ + h * HQ, HQ), HQ)

    def pass_on(h, j):
        to_y[h][j].wait_recv()
        pass_c[h][j].start()

    def close4(h, passing):
        def done(j, total):
            res = (hres[owned[h], cols(j)].astype(F32) + gate1[owned[h]] * total).astype(BF)
            out_ref[rows(sp, core, h), cols(j)] = res
            fin[h, j] = res.astype(F32)
            to_y[h][j].start()
            to_c[h][j].start()
            if passing and j >= 1:
                pass_on(h, j - 1)

        sum4[h].close(done)

    def gathered(h):
        for j in range(NCH):
            out_ref[rows(1 - sp, core, h), cols(j)] = yr[h, j].astype(BF)
            to_c[h][j].wait_recv()
            out_ref[rows(sp, 1 - core, h), cols(j)] = cr[0, h, j].astype(BF)
        for j in range(NCH):
            pass_c[h][j].wait_recv()
            out_ref[rows(1 - sp, 1 - core, h), cols(j)] = cr[1, h, j].astype(BF)
        for j in range(NCH):
            to_y[h][j].wait_send()
            to_c[h][j].wait_send()
            pass_c[h][j].wait_send()

    blocks_to = lambda lo, hi: lax.fori_loop(lo, hi, block, 0)
    blocks_to(0, 4)
    cross_out(0)
    blocks_to(4, 5)
    pass_chip(0)
    blocks_to(5, 7)
    close2(1)
    blocks_to(7, 8)
    cross_out(1)
    cross_q(1)
    blocks_to(8, 9)
    pass_chip(1)
    close3(0)
    blocks_to(9, 12)
    cross_out(2)
    blocks_to(12, 13)
    pass_chip(2)
    close3(1)
    blocks_to(13, 15)
    shared3(0)
    shared3(1)
    for cp in loads2:
        cp.wait()
    mlp(0, sum4[0])
    blocks_to(15, 16)
    cross_out(3)
    close3(2)
    pass_chip(3)
    close4(0, False)
    close3(3)
    for j in range(NCH):
        pass_on(0, j)
    shared3(2)
    shared3(3)
    mlp(1, sum4[1])
    gathered(0)
    close4(1, True)
    pass_on(1, NCH - 1)
    gathered(1)
    for j in range(NCH):
        to_core[j].wait_send()
        to_chip[j].wait_send()
        share[j].wait_send()


def rest_of_step(o, st, hidden, g2, g3, qn, g4, gates, mask, xvalid, ws, k_cross, v_cross):
    wo, wg, wu, wd, wq, wo2 = ws[:6]
    F = wg.shape[1]
    T2 = k_cross.shape[1]
    dma = pltpu.SemaphoreType.DMA
    sum_bufs = [pltpu.VMEM((2, NCH, HQ, W), F32)] * 4 + [dma((2, 4, NCH))]
    share_bufs = [pltpu.VMEM((NQ, HID), F32)] * 2 + [dma((2, 2))]
    return pl.pallas_call(
        rest_kernel,
        in_specs=[ANY, VM, ANY, VM, VM, VM, VM, pl.BlockSpec(memory_space=pltpu.SMEM), VM] + [ANY] * 12,
        out_specs=VM,
        out_shape=jax.ShapeDtypeStruct((NB, HID), BF),
        scratch_shapes=[pltpu.VMEM(w.shape, BF) for w in (wo, wg, wu, wd, wq, wo2)] + [
            dma((10,)), pltpu.VMEM((NR, CR, T2, D), BF), pltpu.VMEM((NR, CR, T2, D), BF), dma((2, NR)),
            pltpu.VMEM((NH * HL, D), F32), pltpu.VMEM((NH * HL, D), F32), pltpu.VMEM((8, D), F32),
            pltpu.VMEM((8, D), F32), dma((2, 5)), pltpu.VMEM((NQ, HID), BF), pltpu.VMEM((NH * HL, D), F32),
            pltpu.VMEM((NH, xvalid.shape[1]), jnp.int32), pltpu.VMEM((NH, D), jnp.int32),
            pltpu.VMEM((NH * 8, D), F32), pltpu.VMEM((2, NQ, HID), BF), pltpu.VMEM((2, NQ, F), BF),
            pltpu.VMEM((NQ, HID), BF), pltpu.VMEM((NQ, HID), BF), pltpu.VMEM((2, NCH, HQ, W), F32),
            pltpu.VMEM((2, NCH, HQ, W), F32), pltpu.VMEM((2, 2, NCH, HQ, W), F32), dma((2, 6, NCH))]
        + sum_bufs + sum_bufs + [pltpu.VMEM((NCH, RC, HID), F32)] * 4 + [dma((4, NCH)), dma((2, NCH))]
        + share_bufs + share_bufs + [dma((2, 4, NCH))],
        compiler_params=pltpu.CompilerParams(collective_id=0, has_side_effects=True, vmem_limit_bytes=VMEM_MAX),
        name="rest_of_step",
    )(o, st, hidden, g2, g3, qn, g4, gates, mask, xvalid, *ws, k_cross, v_cross)


def solution(mesh):
    cache_spec = P('dp', 'sp', 'tp', None)
    cross_spec = P('dp', None, 'tp', None)
    row_spec = P('dp', None)
    vec_spec = P('dp')
    full_spec = P(None)
    col_spec = P(None, 'tp')
    split_rows = P('tp', None)
    in_specs = (row_spec, vec_spec, cache_spec, cache_spec, cross_spec, cross_spec, row_spec, vec_spec,
                full_spec, col_spec, col_spec, col_spec, split_rows, full_spec, col_spec, col_spec, split_rows,
                full_spec, col_spec, full_spec, split_rows, full_spec, full_spec, col_spec, col_spec, split_rows)
    out_specs = (row_spec, cache_spec, cache_spec)

    def local_step(hidden, new_pos, k_self, v_self, k_cross, v_cross, xvalid, rowmask,
                   self_attn_norm, self_wq, self_wk, self_wv, self_wo, self_mlp_norm,
                   self_wgate, self_wup, self_wdown, cross_attn_norm, cross_wq, cross_qnorm,
                   cross_wo, cross_gates, cross_mlp_norm, cross_wgate, cross_wup, cross_wdown):
        flat = lambda a: a.reshape(a.shape[0], a.shape[1] * a.shape[2], a.shape[3])
        k_out, v_out, o, st = self_attention(new_pos, self_attn_norm, hidden, self_wq, self_wk, self_wv,
                                             flat(k_self), flat(v_self))
        weights = (self_wo, self_wgate, self_wup, self_wdown, cross_wq, cross_wo, cross_wgate, cross_wup, cross_wdown)
        h4 = rest_of_step(o, st, hidden, self_mlp_norm, cross_attn_norm, cross_qnorm, cross_mlp_norm, cross_gates,
                          rowmask, xvalid, weights, flat(k_cross), flat(v_cross))
        return h4, k_out.reshape(k_self.shape), v_out.reshape(v_self.shape)

    return jax.shard_map(local_step, mesh=mesh, in_specs=in_specs, out_specs=out_specs, check_vma=False)
```

```python
import functools
import math
import numpy as np
import jax
import jax.numpy as jnp
from jax import lax
from jax.experimental import pallas as pl
from jax.experimental.pallas import tpu as pltpu
from jax.sharding import PartitionSpec as P

NORM_EPS = 1e-5
ROPE_THETA = 500000.0
ROPE_FACTOR = 8.0
LOW_FREQ = 1.0
HIGH_FREQ = 4.0
ORIG_CTX = 8192.0
NEG_BIG = -1e30

BF = jnp.bfloat16
F32 = jnp.float32
D = 128
HL = 4
KL = 2
NB = 256
NH = 128
NQ = 64
HID = 2048
HQ = NQ // 2
NCH = 4
W = HID // NCH
VMEM_MAX = 66 * 1024 * 1024 - 2 * 1024 * 1024
MESH = pl.DeviceIdType.MESH
ANY = pl.BlockSpec(memory_space=pl.ANY)
VM = pl.BlockSpec(memory_space=pltpu.VMEM)


def rope_freqs(head_dim):
    inv_freq = 1.0 / (ROPE_THETA ** (np.arange(0, head_dim, 2) / head_dim))
    wavelen = 2.0 * math.pi / inv_freq
    smooth = (ORIG_CTX / wavelen - LOW_FREQ) / (HIGH_FREQ - LOW_FREQ)
    mid_freq = (1.0 - smooth) * inv_freq / ROPE_FACTOR + smooth * inv_freq
    scaled = np.where(wavelen > ORIG_CTX / LOW_FREQ, inv_freq / ROPE_FACTOR, mid_freq)
    scaled = np.where(wavelen < ORIG_CTX / HIGH_FREQ, inv_freq, scaled)
    return np.concatenate([scaled, scaled]).astype(np.float32)[None, :]


def norm32(vals32, gain32):
    inv = lax.rsqrt(jnp.mean(vals32 * vals32, axis=-1, keepdims=True) + NORM_EPS)
    return (vals32 * inv * gain32).astype(BF)


def dot(a, b):
    return jnp.dot(a, b, preferred_element_type=F32)


def dot_nt(a, b):
    return lax.dot_general(a, b, (((1,), (1,)), ((), ())), preferred_element_type=F32)


def attend(lhs, keys, vals, valid):
    first = lax.broadcasted_iota(jnp.int32, (8, D), 0) < HL
    s = [dot_nt(a, k) * (D ** -0.5) for a, k in zip(lhs, keys)]
    s = [jnp.where(ok, x, NEG_BIG) for ok, x in zip(valid, s)]
    m = [jnp.max(x, axis=-1, keepdims=True) for x in s]
    p = [jnp.where(ok, jnp.exp(x - t), 0.0) for ok, x, t in zip(valid, s, m)]
    l = [jnp.sum(x, axis=-1, keepdims=True) for x in p]
    o = [dot(x.astype(BF), v) for x, v in zip(p, vals)]
    return m, l, [jnp.where(first, x[:, :D], x[:, D:]) for x in o]


def pair_lhs(q_ref, b0):
    q16 = q_ref[pl.ds(pl.multiple_of(b0 * 8, 16), 16), :]
    return jnp.concatenate([q16[:8], q16[8:]], axis=1).astype(BF)


def column(vec, first, rows):
    n = vec.shape[1]
    at = lax.broadcasted_iota(jnp.int32, (rows, n), 1) == lax.broadcasted_iota(jnp.int32, (rows, n), 0) + first
    return jnp.sum(jnp.where(at, vec, 0.0), axis=1, keepdims=True)


def spread_heads(ref, heads, start, rows):
    odd = (lax.broadcasted_iota(jnp.int32, (rows, D), 0) % 2) == 1
    for h in range(HL):
        ref[pl.ds(start * 8 + h, rows, stride=8), :] = jnp.where(odd, 0.0, heads[h])
        ref[pl.ds(start * 8 + HL + h, rows, stride=8), :] = jnp.where(odd, heads[h], 0.0)


SR = 16


def self_kernel(pos_ref, posv_ref, freq_ref, g_ref, hid_hbm, wq_hbm, wk_hbm, wv_hbm, k_hbm, v_hbm,
                ko_hbm, vo_hbm, o_ref, st_ref,
                hid, wq, wk, wv, wsem, kbuf, vbuf, isem, osem, qs, kn, vn):
    T2 = k_hbm.shape[1]
    steps = NB // SR
    first_pos = lax.axis_index("sp") * (T2 // KL)
    loads = [pltpu.make_async_copy(a, b, wsem.at[n])
             for n, (a, b) in enumerate(((hid_hbm, hid), (wq_hbm, wq), (wk_hbm, wk), (wv_hbm, wv)))]
    for cp in loads:
        cp.start()

    def into(i):
        rows = pl.ds(pl.multiple_of(i * SR, SR), SR)
        return (pltpu.make_async_copy(k_hbm.at[rows], kbuf.at[i], isem.at[0, i]),
                pltpu.make_async_copy(v_hbm.at[rows], vbuf.at[i], isem.at[1, i]))

    def out_of(i):
        rows = pl.ds(pl.multiple_of(i * SR, SR), SR)
        return (pltpu.make_async_copy(kbuf.at[i], ko_hbm.at[rows], osem.at[0, i]),
                pltpu.make_async_copy(vbuf.at[i], vo_hbm.at[rows], osem.at[1, i]))

    for i in range(2):
        for cp in into(i):
            cp.start()

    angle = column(posv_ref[...].astype(F32).reshape(1, NB), 0, NB) * freq_ref[...]
    cos, sin = jnp.cos(angle), jnp.sin(angle)
    sin = jnp.where(lax.broadcasted_iota(jnp.int32, (NB, D), 1) < D // 2, -sin, sin)

    def rope(part):
        part = part.astype(BF).astype(F32)
        return (part * cos + pltpu.roll(part, D // 2, 1) * sin).astype(BF).astype(F32)

    loads[0].wait()
    loads[1].wait()
    for i in range(2, steps):
        for cp in into(i):
            cp.start()
    x = norm32(hid[...].astype(F32), g_ref[...].astype(F32).reshape(1, HID))
    q = dot(x, wq[...])
    spread_heads(qs, [rope(q[:, h * D:(h + 1) * D]) for h in range(HL)], 0, NB)
    loads[2].wait()
    k = dot(x, wk[...])
    loads[3].wait()
    v = dot(x, wv[...])
    for h in range(KL):
        kn[pl.ds(h, NB, stride=KL), :] = rope(k[:, h * D:(h + 1) * D])
        vn[pl.ds(h, NB, stride=KL), :] = v[:, h * D:(h + 1) * D].astype(BF).astype(F32)
    st_ref[...] = jnp.zeros_like(st_ref)

    col = lax.broadcasted_iota(jnp.int32, (8, T2), 1)
    row = lax.broadcasted_iota(jnp.int32, (8, T2), 0)
    tok = col // KL
    head_ok = (col % KL) == ((row % HL) // (HL // KL))
    lane = lax.broadcasted_iota(jnp.int32, (8, D), 1)
    i16 = lax.broadcasted_iota(jnp.int32, (16, D), 0)

    def patch(new_ref, dst_ref, slot, r, b, lp):
        base = pl.multiple_of((jnp.clip(lp, 0, T2 // KL - 1) // 8) * 16, 16)
        fresh = jnp.where(i16 % 2 == 0, new_ref[pl.ds(2 * b, 1), :], new_ref[pl.ds(2 * b + 1, 1), :])
        old = dst_ref[slot, r, pl.ds(base, 16), :].astype(F32)
        dst_ref[slot, r, pl.ds(base, 16), :] = jnp.where(base + i16 - i16 % 2 == 2 * lp, fresh, old).astype(BF)

    def body(i, _):
        for cp in into(i):
            cp.wait()
        lps = [pos_ref[i * SR + r] - first_pos for r in range(SR)]
        for r in range(SR):
            patch(kn, kbuf, i, r, i * SR + r, lps[r])
            patch(vn, vbuf, i, r, i * SR + r, lps[r])
        pairs = range(SR // 2)
        both = lambda buf, p: jnp.concatenate([buf[i, 2 * p], buf[i, 2 * p + 1]], axis=1)
        m, l, o = attend([pair_lhs(qs, i * SR + 2 * p) for p in pairs], [both(kbuf, p) for p in pairs],
                         [both(vbuf, p) for p in pairs],
                         [head_ok & (tok <= jnp.where(row < HL, lps[2 * p], lps[2 * p + 1])) for p in pairs])
        half = i // (NH // SR)
        srow = pl.ds(pl.multiple_of(half * 8, 8), 8)
        st = st_ref[srow, :]
        for p in pairs:
            o_ref[pl.ds(pl.multiple_of(i * SR * HL + 8 * p, 8), 8), :] = o[p]
            at = (i - half * (NH // SR)) * (SR // 2) + p
            st = jnp.where(lane == at, m[p], jnp.where(lane == at + NQ, l[p], st))
        st_ref[srow, :] = st
        for cp in out_of(i):
            cp.start()
        return 0

    lax.fori_loop(0, steps, body, 0)
    for i in range(steps):
        for cp in out_of(i):
            cp.wait()


def self_attention(new_pos, g1, hidden, wq, wk, wv, k_self, v_self):
    T2 = k_self.shape[1]
    return pl.pallas_call(
        self_kernel,
        in_specs=[pl.BlockSpec(memory_space=pltpu.SMEM), VM, VM, VM] + [ANY] * 6,
        out_specs=[ANY, ANY, VM, VM],
        scratch_shapes=[pltpu.VMEM(hidden.shape, BF), pltpu.VMEM(wq.shape, BF), pltpu.VMEM(wk.shape, BF),
                        pltpu.VMEM(wv.shape, BF), pltpu.SemaphoreType.DMA((4,)),
                        pltpu.VMEM((NB // SR, SR, T2, D), BF), pltpu.VMEM((NB // SR, SR, T2, D), BF),
                        pltpu.SemaphoreType.DMA((2, NB // SR)), pltpu.SemaphoreType.DMA((2, NB // SR)),
                        pltpu.VMEM((NB * 8, D), F32), pltpu.VMEM((NB * KL, D), F32), pltpu.VMEM((NB * KL, D), F32)],
        out_shape=[jax.ShapeDtypeStruct(k_self.shape, BF), jax.ShapeDtypeStruct(v_self.shape, BF),
                   jax.ShapeDtypeStruct((NB * HL, D), F32), jax.ShapeDtypeStruct((16, D), F32)],
        compiler_params=pltpu.CompilerParams(vmem_limit_bytes=VMEM_MAX),
        name="self_attn",
    )(new_pos, new_pos, jnp.asarray(rope_freqs(D)), g1, hidden, wq, wk, wv, k_self, v_self)


def peers():
    sp, tp = lax.axis_index("sp"), lax.axis_index("tp")
    core = lax.rem(tp, 2)
    return dict(sp=sp, core=core, y={"sp": 1 - sp}, c={"tp": tp + 1 - 2 * core}, x={"tp": lax.rem(tp + 2, 4)})


def entry_barrier(pe):
    barrier = pltpu.get_barrier_semaphore()
    for name in ("y", "c", "x"):
        pl.semaphore_signal(barrier, inc=1, device_id=pe[name], device_id_type=MESH)
    pl.semaphore_wait(barrier, 3)


def rcopy(src, dst, ssem, rsem, dev):
    return pltpu.make_async_remote_copy(src_ref=src, dst_ref=dst, send_sem=ssem, recv_sem=rsem,
                                        device_id=dev, device_id_type=MESH)


class TpSum:
    def __init__(self, pe, half, bufs):
        snd, rcv, chip, xr, sems = bufs
        self.snd, self.rcv, self.chip, self.xr = (b.at[half] for b in (snd, rcv, chip, xr))
        at = lambda n, j: sems.at[half, n, j]
        self.to_core = [rcopy(self.snd.at[j], self.rcv.at[j], at(0, j), at(1, j), pe["c"]) for j in range(NCH)]
        self.to_chip = [rcopy(self.chip.at[j], self.xr.at[j], at(2, j), at(3, j), pe["x"]) for j in range(NCH)]

    def start(self, compute):
        for j in range(NCH):
            part = compute(j)
            self.snd[j] = part[HQ:]
            self.chip[j] = part[:HQ]
            self.to_core[j].start()

    def forward(self):
        for j in range(NCH):
            self.to_core[j].wait_recv()
            self.chip[j] = self.chip[j] + self.rcv[j]
            self.to_chip[j].start()

    def close(self, finish):
        for j in range(NCH):
            self.to_chip[j].wait_recv()
            finish(j, self.chip[j] + self.xr[j])
        for j in range(NCH):
            self.to_core[j].wait_send()
            self.to_chip[j].wait_send()


class Share:
    def __init__(self, pe, half, x_ref, snd, rcv, sems):
        rows = pl.ds(half * HQ, HQ)
        self.snd, self.rcv, self.x = snd.at[rows], rcv.at[rows], x_ref.at[half]
        self.copy = rcopy(self.snd, self.rcv, sems.at[0, half], sems.at[1, half], pe["c"])

    def start(self, own):
        self.snd[...] = own.astype(F32)
        self.copy.start()
        self.x[pl.ds(0, HQ), :] = own

    def finish(self):
        self.copy.wait()
        self.x[pl.ds(HQ, HQ), :] = self.rcv[...].astype(BF)


def mlp_act(x_ref, wg, wu, act, chunks):
    step = act.shape[1] // 3
    for c in chunks:
        s = slice(c * step, (c + 1) * step)
        gate = dot(x_ref[...], wg[:, s]).astype(BF).astype(F32)
        up = dot(x_ref[...], wu[:, s]).astype(BF).astype(F32)
        act[:, s] = (gate * jax.nn.sigmoid(gate) * up).astype(BF)


def cols(j):
    return slice(j * W, (j + 1) * W)


def heads_to_lanes(ref, starts, rows):
    parts = [jnp.concatenate([ref[pl.ds(s * HL + h, rows, stride=HL), :] for h in range(HL)], axis=1) for s in starts]
    return jnp.concatenate(parts, axis=0).astype(BF)


CR = 8
NR = 5
RC = NQ // NCH
XB = 2 * RC // CR


def rest_kernel(o_hbm, st_ref, hid_hbm, g2_ref, g3_ref, qn_ref, g4_ref, gates_ref, mask_ref, valid_hbm,
                wo_hbm, wg_hbm, wu_hbm, wd_hbm, wq_hbm, wo2_hbm, wg2_hbm, wu2_hbm, wd2_hbm, k_hbm, v_hbm,
                out_ref,
                wo, wg, wu, wd, wq, wo2, wsem, kbuf, vbuf, ksem, osnd, orcv, sts, str_, ysem, hown, att, valid, cnt,
                qx, xbuf, act, hres, h2, fin, yr, cr, gsem,
                a0, a1, a2, a3, asem, b0, b1, b2, b3, bsem, c0, c1, c2, c3, csem, dsem,
                s0, s1, ssem, t0, t1, tsem, esem):
    pe = peers()
    sp, core = pe["sp"], pe["core"]
    T2 = k_hbm.shape[1]
    half = NH * HL
    blocks = NH // CR

    local = [pltpu.make_async_copy(o_hbm.at[pl.ds(pl.multiple_of((1 - sp) * half, half), half)], osnd, wsem.at[6]),
             pltpu.make_async_copy(o_hbm.at[pl.ds(pl.multiple_of(sp * half, half), half)], att, wsem.at[7]),
             pltpu.make_async_copy(hid_hbm.at[pl.ds(pl.multiple_of(sp * NH + core * NQ, NQ), NQ)], hown, wsem.at[8]),
             pltpu.make_async_copy(valid_hbm.at[pl.ds(pl.multiple_of(sp * NH, NH), NH)], valid, wsem.at[9])]
    pairs = ((wo_hbm, wo), (wg_hbm, wg), (wu_hbm, wu), (wd_hbm, wd), (wq_hbm, wq), (wo2_hbm, wo2))
    loads = [pltpu.make_async_copy(a, b, wsem.at[n]) for n, (a, b) in enumerate(pairs)]
    for cp in local:
        cp.start()

    def block_row(t):
        chunk, of_core, sub = t // XB, (t % XB) // (XB // 2), t % (XB // 2)
        return of_core * NQ + chunk * RC + sub * CR

    def kv_loads(t):
        rows, slot = pl.ds(pl.multiple_of(sp * NH + block_row(t), CR), CR), t % NR
        return (pltpu.make_async_copy(k_hbm.at[rows], kbuf.at[slot], ksem.at[0, slot]),
                pltpu.make_async_copy(v_hbm.at[rows], vbuf.at[slot], ksem.at[1, slot]))

    with jax.named_scope("enter"):
        entry_barrier(pe)
    both = st_ref[...]
    mine = jnp.where(sp == 0, both[:8], both[8:])
    sts[...] = jnp.where(sp == 0, both[8:], both[:8])
    local[0].wait()
    cp_s = rcopy(sts, str_, ysem.at[0, 4], ysem.at[1, 4], pe["y"])
    cp_s.start()

    def quarter(h, c):
        rows = pl.ds((c * NQ + h * HQ) * HL, HQ * HL)
        return rcopy(osnd.at[rows], orcv.at[rows], ysem.at[0, 2 * h + c], ysem.at[1, 2 * h + c], pe["y"])

    quarters = [quarter(h, c) for h in range(2) for c in range(2)]
    for cp in quarters:
        cp.start()
    for cp in local[1:]:
        cp.wait()
    for cp in loads:
        cp.start()
    for t in range(NR):
        for cp in kv_loads(t):
            cp.start()
    some = jnp.sum((valid[...] > 0).astype(jnp.int32), axis=1, keepdims=True)
    cnt[...] = jnp.broadcast_to(some, cnt.shape)
    row_scale = column(mask_ref[...].astype(F32).reshape(1, NB), sp * NH + core * NQ, NQ)
    gate0 = jnp.tanh(jnp.full((8, D), gates_ref[0], F32))[0:1, 0:1] * row_scale
    gate1 = jnp.tanh(jnp.full((8, D), gates_ref[1], F32))[0:1, 0:1] * row_scale
    gain = lambda ref: ref[...].astype(F32).reshape(1, HID)
    owned = [slice(h * HQ, (h + 1) * HQ) for h in range(2)]
    sum1 = [TpSum(pe, h, (a0, a1, a2, a3, asem)) for h in range(2)]
    sum2 = [TpSum(pe, h, (b0, b1, b2, b3, bsem)) for h in range(2)]
    sum4 = [TpSum(pe, h, (a0, a1, a2, a3, esem)) for h in range(2)]
    share1 = [Share(pe, h, xbuf, s0, s1, ssem) for h in range(2)]
    share2 = [Share(pe, h, xbuf, t0, t1, tsem) for h in range(2)]

    cp_s.wait()
    theirs = str_[...]
    top = jnp.maximum(mine, theirs)
    f1, f2 = jnp.exp(mine - top), jnp.exp(theirs - top)
    den = pltpu.roll(mine, NQ, 1) * f1 + pltpu.roll(theirs, NQ, 1) * f2
    w1, w2 = f1 / den, f2 / den

    def combine(h):
        for c in range(2):
            quarters[2 * h + c].wait()
            for p in range((c * NQ + h * HQ) // 2, (c * NQ + h * HQ + HQ) // 2):
                s = pl.ds(8 * p, 8)
                att[s, :] = att[s, :] * w1[:, p:p + 1] + orcv[s, :] * w2[:, p:p + 1]
        return heads_to_lanes(att, (core * NQ + h * HQ, (1 - core) * NQ + h * HQ), HQ)

    def close1(h):
        def done(j, total):
            hres[owned[h], cols(j)] = (hown[owned[h], cols(j)].astype(F32) + total).astype(BF)

        sum1[h].close(done)
        share1[h].start(norm32(hres[owned[h], :].astype(F32), gain(g2_ref)))

    def mlp_down(h, total):
        total.start(lambda j: dot(act[h], wd[:, cols(j)]))

    def mlp(h, total):
        mlp_act(xbuf.at[h], wg, wu, act.at[h], range(3))
        mlp_down(h, total)

    def close2(h):
        def done(j, total):
            h2[owned[h], cols(j)] = (hres[owned[h], cols(j)].astype(F32) + total).astype(BF)

        sum2[h].close(done)
        share2[h].start(norm32(h2[owned[h], :].astype(F32), gain(g3_ref)))

    def cross_q(h):
        share2[h].finish()
        q = dot(xbuf[h], wq[...])
        qgain = qn_ref[...].astype(F32).reshape(1, D)
        heads = [norm32(q[:, n * D:(n + 1) * D].astype(BF).astype(F32), qgain).astype(F32) for n in range(HL)]
        spread_heads(qx, [x[:HQ] for x in heads], core * NQ + h * HQ, HQ)
        spread_heads(qx, [x[HQ:] for x in heads], (1 - core) * NQ + h * HQ, HQ)

    with jax.named_scope("out_a"):
        lhs0 = combine(0)
        loads[0].wait()
        sum1[0].start(lambda j: dot(lhs0, wo[:, cols(j)]))
    with jax.named_scope("out_b"):
        lhs1 = combine(1)
        sum1[0].forward()
        sum1[1].start(lambda j: dot(lhs1, wo[:, cols(j)]))
        sum1[1].forward()
    with jax.named_scope("close1_a"):
        close1(0)
    with jax.named_scope("share1_a"):
        share1[0].finish()
    for cp in loads[1:4]:
        cp.wait()
    with jax.named_scope("mlp_a"):
        mlp(0, sum2[0])
        sum2[0].forward()
    with jax.named_scope("close1_b"):
        close1(1)
    with jax.named_scope("share1_b"):
        share1[1].finish()
    with jax.named_scope("mlp_b"):
        mlp(1, sum2[1])
        sum2[1].forward()
    loads2 = [pltpu.make_async_copy(a, b, wsem.at[1 + n])
              for n, (a, b) in enumerate(((wg2_hbm, wg), (wu2_hbm, wu), (wd2_hbm, wd)))]
    for cp in loads2:
        cp.start()
    with jax.named_scope("close2_a"):
        close2(0)
    loads[4].wait()
    with jax.named_scope("q_a"):
        cross_q(0)
    loads[5].wait()

    col = lax.broadcasted_iota(jnp.int32, (8, T2), 1)
    row = lax.broadcasted_iota(jnp.int32, (8, T2), 0)
    tok = col // KL
    head_ok = (col % KL) == ((row % HL) // (HL // KL))
    first = lax.broadcasted_iota(jnp.int32, (8, D), 0) < HL

    def block(t, _):
        slot = t % NR
        r0 = pl.multiple_of(block_row(t), CR)
        for cp in kv_loads(t):
            cp.wait()
        ps = range(CR // 2)
        lane_pair = lambda buf, p: jnp.concatenate([buf[slot, 2 * p], buf[slot, 2 * p + 1]], axis=1)
        n8 = cnt[pl.ds(r0, CR), :]
        limit = [jnp.concatenate([jnp.where(first, n8[2 * p:2 * p + 1], n8[2 * p + 1:2 * p + 2])] * (T2 // D), axis=1)
                 for p in ps]
        m, l, o = attend([pair_lhs(qx, r0 + 2 * p) for p in ps], [lane_pair(kbuf, p) for p in ps],
                         [lane_pair(vbuf, p) for p in ps], [head_ok & (tok < n) for n in limit])
        for p in ps:
            att[pl.ds(pl.multiple_of(r0 * HL + 8 * p, 8), 8), :] = o[p] / l[p]

        @pl.when(t + NR < blocks)
        def _():
            for cp in kv_loads(t + NR):
                cp.start()
        return 0

    to_core = [rcopy(c0.at[j], c1.at[j], csem.at[0, j], csem.at[1, j], pe["c"]) for j in range(NCH)]
    to_chip = [rcopy(c2.at[j], c3.at[j], csem.at[2, j], csem.at[3, j], pe["x"]) for j in range(NCH)]
    share = [rcopy(s0.at[pl.ds(j * RC, RC)], s1.at[pl.ds(j * RC, RC)], dsem.at[0, j], dsem.at[1, j], pe["c"])
             for j in range(NCH)]

    def pass_chip(j):
        to_core[j].wait_recv()
        c2[j] = c2[j] + c1[j]
        to_chip[j].start()

    def close3(j):
        mine = slice(j * RC, (j + 1) * RC)
        to_chip[j].wait_recv()
        hres[mine, :] = (h2[mine, :].astype(F32) + gate0[mine] * (c2[j] + c3[j])).astype(BF)
        own = norm32(hres[mine, :].astype(F32), gain(g4_ref))
        s0[mine, :] = own.astype(F32)
        share[j].start()
        xbuf[j // 2, pl.ds((j % 2) * RC, RC), :] = own

    def shared3(j):
        share[j].wait_recv()
        xbuf[j // 2, pl.ds(HQ + (j % 2) * RC, RC), :] = s1[pl.ds(j * RC, RC), :].astype(BF)

    def cross_out(j):
        lhs = heads_to_lanes(att, (core * NQ + j * RC, (1 - core) * NQ + j * RC), RC)
        for n in range(NCH):
            part = dot(lhs, wo2[:, cols(n)])
            c0[j, :, cols(n)] = part[RC:]
            c2[j, :, cols(n)] = part[:RC]
        to_core[j].start()

    to_y = [[rcopy(fin.at[h, j], yr.at[h, j], gsem.at[h, 0, j], gsem.at[h, 1, j], pe["y"]) for j in range(NCH)]
            for h in range(2)]
    to_c = [[rcopy(fin.at[h, j], cr.at[0, h, j], gsem.at[h, 2, j], gsem.at[h, 3, j], pe["c"]) for j in range(NCH)]
            for h in range(2)]
    pass_c = [[rcopy(yr.at[h, j], cr.at[1, h, j], gsem.at[h, 4, j], gsem.at[h, 5, j], pe["c"]) for j in range(NCH)]
              for h in range(2)]

    def rows(of_sp, of_core, h):
        return pl.ds(pl.multiple_of(of_sp * NH + of_core * NQ + h * HQ, HQ), HQ)

    def pass_on(h, j):
        to_y[h][j].wait_recv()
        pass_c[h][j].start()

    def close4(h, passing):
        def done(j, total):
            res = (hres[owned[h], cols(j)].astype(F32) + gate1[owned[h]] * total).astype(BF)
            out_ref[rows(sp, core, h), cols(j)] = res
            fin[h, j] = res.astype(F32)
            to_y[h][j].start()
            to_c[h][j].start()
            if passing and j >= 1:
                pass_on(h, j - 1)

        sum4[h].close(done)

    def gathered(h):
        for j in range(NCH):
            out_ref[rows(1 - sp, core, h), cols(j)] = yr[h, j].astype(BF)
            to_c[h][j].wait_recv()
            out_ref[rows(sp, 1 - core, h), cols(j)] = cr[0, h, j].astype(BF)
        for j in range(NCH):
            pass_c[h][j].wait_recv()
            out_ref[rows(1 - sp, 1 - core, h), cols(j)] = cr[1, h, j].astype(BF)
        for j in range(NCH):
            to_y[h][j].wait_send()
            to_c[h][j].wait_send()
            pass_c[h][j].wait_send()

    blocks_to = lambda lo, hi: lax.fori_loop(lo, hi, block, 0)
    with jax.named_scope("x0"):
        blocks_to(0, 4)
    with jax.named_scope("o0"):
        cross_out(0)
    with jax.named_scope("x4"):
        blocks_to(4, 5)
    with jax.named_scope("pass0"):
        pass_chip(0)
    with jax.named_scope("x5"):
        blocks_to(5, 7)
    with jax.named_scope("close2_b"):
        close2(1)
    with jax.named_scope("x7"):
        blocks_to(7, 8)
    with jax.named_scope("o1"):
        cross_out(1)
    with jax.named_scope("q_b"):
        cross_q(1)
    with jax.named_scope("x8"):
        blocks_to(8, 9)
    with jax.named_scope("pass1"):
        pass_chip(1)
    with jax.named_scope("close3_0"):
        close3(0)
    with jax.named_scope("x9"):
        blocks_to(9, 12)
    with jax.named_scope("o2"):
        cross_out(2)
    with jax.named_scope("x12"):
        blocks_to(12, 13)
    with jax.named_scope("pass2"):
        pass_chip(2)
    with jax.named_scope("close3_1"):
        close3(1)
    with jax.named_scope("x13"):
        blocks_to(13, 16)
    with jax.named_scope("o3"):
        cross_out(3)
    with jax.named_scope("close3_2"):
        close3(2)
    with jax.named_scope("shared01"):
        shared3(0)
        shared3(1)
        for cp in loads2:
            cp.wait()
    with jax.named_scope("mlp2_a"):
        mlp_act(xbuf.at[0], wg, wu, act.at[0], (0,))
        pass_chip(3)
        mlp_act(xbuf.at[0], wg, wu, act.at[0], (1, 2))
        mlp_down(0, sum4[0])
    with jax.named_scope("forward4_a"):
        sum4[0].forward()
    with jax.named_scope("close3_3"):
        close3(3)
    with jax.named_scope("shared23"):
        shared3(2)
        shared3(3)
    with jax.named_scope("mlp2_b"):
        mlp(1, sum4[1])
    with jax.named_scope("forward4_b"):
        sum4[1].forward()
    with jax.named_scope("close4_a"):
        close4(0, False)
    with jax.named_scope("pass_on"):
        for j in range(NCH):
            pass_on(0, j)
    with jax.named_scope("gathered_a"):
        gathered(0)
    with jax.named_scope("close4_b"):
        close4(1, True)
    with jax.named_scope("gathered_b"):
        pass_on(1, NCH - 1)
        gathered(1)
    for j in range(NCH):
        to_core[j].wait_send()
        to_chip[j].wait_send()
        share[j].wait_send()


def rest_of_step(o, st, hidden, g2, g3, qn, g4, gates, mask, xvalid, ws, k_cross, v_cross):
    wo, wg, wu, wd, wq, wo2 = ws[:6]
    F = wg.shape[1]
    T2 = k_cross.shape[1]
    dma = pltpu.SemaphoreType.DMA
    sum_bufs = [pltpu.VMEM((2, NCH, HQ, W), F32)] * 4 + [dma((2, 4, NCH))]
    share_bufs = [pltpu.VMEM((NQ, HID), F32)] * 2 + [dma((2, 2))]
    return pl.pallas_call(
        rest_kernel,
        in_specs=[ANY, VM, ANY, VM, VM, VM, VM, pl.BlockSpec(memory_space=pltpu.SMEM), VM] + [ANY] * 12,
        out_specs=VM,
        out_shape=jax.ShapeDtypeStruct((NB, HID), BF),
        scratch_shapes=[pltpu.VMEM(w.shape, BF) for w in (wo, wg, wu, wd, wq, wo2)] + [
            dma((10,)), pltpu.VMEM((NR, CR, T2, D), BF), pltpu.VMEM((NR, CR, T2, D), BF), dma((2, NR)),
            pltpu.VMEM((NH * HL, D), F32), pltpu.VMEM((NH * HL, D), F32), pltpu.VMEM((8, D), F32),
            pltpu.VMEM((8, D), F32), dma((2, 5)), pltpu.VMEM((NQ, HID), BF), pltpu.VMEM((NH * HL, D), F32),
            pltpu.VMEM((NH, xvalid.shape[1]), jnp.int32), pltpu.VMEM((NH, D), jnp.int32),
            pltpu.VMEM((NH * 8, D), F32), pltpu.VMEM((2, NQ, HID), BF), pltpu.VMEM((2, NQ, F), BF),
            pltpu.VMEM((NQ, HID), BF), pltpu.VMEM((NQ, HID), BF), pltpu.VMEM((2, NCH, HQ, W), F32),
            pltpu.VMEM((2, NCH, HQ, W), F32), pltpu.VMEM((2, 2, NCH, HQ, W), F32), dma((2, 6, NCH))]
        + sum_bufs + sum_bufs + [pltpu.VMEM((NCH, RC, HID), F32)] * 4 + [dma((4, NCH)), dma((2, NCH))]
        + share_bufs + share_bufs + [dma((2, 4, NCH))],
        compiler_params=pltpu.CompilerParams(collective_id=0, has_side_effects=True, vmem_limit_bytes=VMEM_MAX),
        name="rest_of_step",
    )(o, st, hidden, g2, g3, qn, g4, gates, mask, xvalid, *ws, k_cross, v_cross)


def solution(mesh):
    cache_spec = P('dp', 'sp', 'tp', None)
    cross_spec = P('dp', None, 'tp', None)
    row_spec = P('dp', None)
    vec_spec = P('dp')
    full_spec = P(None)
    col_spec = P(None, 'tp')
    split_rows = P('tp', None)
    in_specs = (row_spec, vec_spec, cache_spec, cache_spec, cross_spec, cross_spec, row_spec, vec_spec,
                full_spec, col_spec, col_spec, col_spec, split_rows, full_spec, col_spec, col_spec, split_rows,
                full_spec, col_spec, full_spec, split_rows, full_spec, full_spec, col_spec, col_spec, split_rows)
    out_specs = (row_spec, cache_spec, cache_spec)

    def local_step(hidden, new_pos, k_self, v_self, k_cross, v_cross, xvalid, rowmask,
                   self_attn_norm, self_wq, self_wk, self_wv, self_wo, self_mlp_norm,
                   self_wgate, self_wup, self_wdown, cross_attn_norm, cross_wq, cross_qnorm,
                   cross_wo, cross_gates, cross_mlp_norm, cross_wgate, cross_wup, cross_wdown):
        flat = lambda a: a.reshape(a.shape[0], a.shape[1] * a.shape[2], a.shape[3])
        k_out, v_out, o, st = self_attention(new_pos, self_attn_norm, hidden, self_wq, self_wk, self_wv,
                                             flat(k_self), flat(v_self))
        weights = (self_wo, self_wgate, self_wup, self_wdown, cross_wq, cross_wo, cross_wgate, cross_wup, cross_wdown)
        h4 = rest_of_step(o, st, hidden, self_mlp_norm, cross_attn_norm, cross_qnorm, cross_mlp_norm, cross_gates,
                          rowmask, xvalid, weights, flat(k_cross), flat(v_cross))
        return h4, k_out.reshape(k_self.shape), v_out.reshape(v_self.shape)

    return jax.shard_map(local_step, mesh=mesh, in_specs=in_specs, out_specs=out_specs, check_vma=False)
```

```python
import functools
import math
import numpy as np
import jax
import jax.numpy as jnp
from jax import lax
from jax.experimental import pallas as pl
from jax.experimental.pallas import tpu as pltpu
from jax.sharding import PartitionSpec as P

NORM_EPS = 1e-5
ROPE_THETA = 500000.0
ROPE_FACTOR = 8.0
LOW_FREQ = 1.0
HIGH_FREQ = 4.0
ORIG_CTX = 8192.0
NEG_BIG = -1e30

BF = jnp.bfloat16
F32 = jnp.float32
D = 128
HL = 4
KL = 2
NB = 256
NH = 128
NQ = 64
HID = 2048
HQ = NQ // 2
NCH = 4
W = HID // NCH
VMEM_MAX = 66 * 1024 * 1024 - 2 * 1024 * 1024
MESH = pl.DeviceIdType.MESH
ANY = pl.BlockSpec(memory_space=pl.ANY)
VM = pl.BlockSpec(memory_space=pltpu.VMEM)


def rope_freqs(head_dim):
    inv_freq = 1.0 / (ROPE_THETA ** (np.arange(0, head_dim, 2) / head_dim))
    wavelen = 2.0 * math.pi / inv_freq
    smooth = (ORIG_CTX / wavelen - LOW_FREQ) / (HIGH_FREQ - LOW_FREQ)
    mid_freq = (1.0 - smooth) * inv_freq / ROPE_FACTOR + smooth * inv_freq
    scaled = np.where(wavelen > ORIG_CTX / LOW_FREQ, inv_freq / ROPE_FACTOR, mid_freq)
    scaled = np.where(wavelen < ORIG_CTX / HIGH_FREQ, inv_freq, scaled)
    return np.concatenate([scaled, scaled]).astype(np.float32)[None, :]


def norm32(vals32, gain32):
    inv = lax.rsqrt(jnp.mean(vals32 * vals32, axis=-1, keepdims=True) + NORM_EPS)
    return (vals32 * inv * gain32).astype(BF)


def dot(a, b):
    return jnp.dot(a, b, preferred_element_type=F32)


def dot_nt(a, b):
    return lax.dot_general(a, b, (((1,), (1,)), ((), ())), preferred_element_type=F32)


def attend(lhs, keys, vals, valid):
    first = lax.broadcasted_iota(jnp.int32, (8, D), 0) < HL
    s = [dot_nt(a, k) * (D ** -0.5) for a, k in zip(lhs, keys)]
    s = [jnp.where(ok, x, NEG_BIG) for ok, x in zip(valid, s)]
    m = [jnp.max(x, axis=-1, keepdims=True) for x in s]
    p = [jnp.where(ok, jnp.exp(x - t), 0.0) for ok, x, t in zip(valid, s, m)]
    l = [jnp.sum(x, axis=-1, keepdims=True) for x in p]
    o = [dot(x.astype(BF), v) for x, v in zip(p, vals)]
    return m, l, [jnp.where(first, x[:, :D], x[:, D:]) for x in o]


def pair_lhs(q_ref, b0):
    q16 = q_ref[pl.ds(pl.multiple_of(b0 * 8, 16), 16), :]
    return jnp.concatenate([q16[:8], q16[8:]], axis=1).astype(BF)


def column(vec, first, rows):
    n = vec.shape[1]
    at = lax.broadcasted_iota(jnp.int32, (rows, n), 1) == lax.broadcasted_iota(jnp.int32, (rows, n), 0) + first
    return jnp.sum(jnp.where(at, vec, 0.0), axis=1, keepdims=True)


def spread_heads(ref, heads, start, rows):
    odd = (lax.broadcasted_iota(jnp.int32, (rows, D), 0) % 2) == 1
    for h in range(HL):
        ref[pl.ds(start * 8 + h, rows, stride=8), :] = jnp.where(odd, 0.0, heads[h])
        ref[pl.ds(start * 8 + HL + h, rows, stride=8), :] = jnp.where(odd, heads[h], 0.0)


SR = 16


def self_kernel(pos_ref, posv_ref, freq_ref, g_ref, hid_hbm, wq_hbm, wk_hbm, wv_hbm, k_hbm, v_hbm,
                ko_hbm, vo_hbm, o_ref, st_ref,
                hid, wq, wk, wv, wsem, kbuf, vbuf, isem, osem, qs, kn, vn):
    T2 = k_hbm.shape[1]
    steps = NB // SR
    first_pos = lax.axis_index("sp") * (T2 // KL)
    loads = [pltpu.make_async_copy(a, b, wsem.at[n])
             for n, (a, b) in enumerate(((hid_hbm, hid), (wq_hbm, wq), (wk_hbm, wk), (wv_hbm, wv)))]
    for cp in loads:
        cp.start()

    def into(i):
        rows = pl.ds(pl.multiple_of(i * SR, SR), SR)
        return (pltpu.make_async_copy(k_hbm.at[rows], kbuf.at[i], isem.at[0, i]),
                pltpu.make_async_copy(v_hbm.at[rows], vbuf.at[i], isem.at[1, i]))

    def out_of(i):
        rows = pl.ds(pl.multiple_of(i * SR, SR), SR)
        return (pltpu.make_async_copy(kbuf.at[i], ko_hbm.at[rows], osem.at[0, i]),
                pltpu.make_async_copy(vbuf.at[i], vo_hbm.at[rows], osem.at[1, i]))

    for i in range(2):
        for cp in into(i):
            cp.start()

    with jax.named_scope("qkv"):
        angle = column(posv_ref[...].astype(F32).reshape(1, NB), 0, NB) * freq_ref[...]
        cos, sin = jnp.cos(angle), jnp.sin(angle)
        sin = jnp.where(lax.broadcasted_iota(jnp.int32, (NB, D), 1) < D // 2, -sin, sin)

        def rope(part):
            part = part.astype(BF).astype(F32)
            return (part * cos + pltpu.roll(part, D // 2, 1) * sin).astype(BF).astype(F32)

        loads[0].wait()
        loads[1].wait()
        for i in range(2, steps):
            for cp in into(i):
                cp.start()
        x = norm32(hid[...].astype(F32), g_ref[...].astype(F32).reshape(1, HID))
        q = dot(x, wq[...])
        spread_heads(qs, [rope(q[:, h * D:(h + 1) * D]) for h in range(HL)], 0, NB)
        loads[2].wait()
        k = dot(x, wk[...])
        loads[3].wait()
        v = dot(x, wv[...])
        for h in range(KL):
            kn[pl.ds(h, NB, stride=KL), :] = rope(k[:, h * D:(h + 1) * D])
            vn[pl.ds(h, NB, stride=KL), :] = v[:, h * D:(h + 1) * D].astype(BF).astype(F32)
    st_ref[...] = jnp.zeros_like(st_ref)

    col = lax.broadcasted_iota(jnp.int32, (8, T2), 1)
    row = lax.broadcasted_iota(jnp.int32, (8, T2), 0)
    tok = col // KL
    head_ok = (col % KL) == ((row % HL) // (HL // KL))
    lane = lax.broadcasted_iota(jnp.int32, (8, D), 1)
    i16 = lax.broadcasted_iota(jnp.int32, (16, D), 0)

    def patch(new_ref, dst_ref, slot, r, b, lp):
        base = pl.multiple_of((jnp.clip(lp, 0, T2 // KL - 1) // 8) * 16, 16)
        fresh = jnp.where(i16 % 2 == 0, new_ref[pl.ds(2 * b, 1), :], new_ref[pl.ds(2 * b + 1, 1), :])
        old = dst_ref[slot, r, pl.ds(base, 16), :].astype(F32)
        dst_ref[slot, r, pl.ds(base, 16), :] = jnp.where(base + i16 - i16 % 2 == 2 * lp, fresh, old).astype(BF)

    def body(i, _):
        for cp in into(i):
            cp.wait()
        lps = [pos_ref[i * SR + r] - first_pos for r in range(SR)]
        for r in range(SR):
            patch(kn, kbuf, i, r, i * SR + r, lps[r])
            patch(vn, vbuf, i, r, i * SR + r, lps[r])
        pairs = range(SR // 2)
        both = lambda buf, p: jnp.concatenate([buf[i, 2 * p], buf[i, 2 * p + 1]], axis=1)
        m, l, o = attend([pair_lhs(qs, i * SR + 2 * p) for p in pairs], [both(kbuf, p) for p in pairs],
                         [both(vbuf, p) for p in pairs],
                         [head_ok & (tok <= jnp.where(row < HL, lps[2 * p], lps[2 * p + 1])) for p in pairs])
        half = i // (NH // SR)
        srow = pl.ds(pl.multiple_of(half * 8, 8), 8)
        st = st_ref[srow, :]
        for p in pairs:
            o_ref[pl.ds(pl.multiple_of(i * SR * HL + 8 * p, 8), 8), :] = o[p]
            at = (i - half * (NH // SR)) * (SR // 2) + p
            st = jnp.where(lane == at, m[p], jnp.where(lane == at + NQ, l[p], st))
        st_ref[srow, :] = st
        for cp in out_of(i):
            cp.start()
        return 0

    for i in range(4):
        with jax.named_scope("steps"):
            lax.fori_loop(i * (steps // 4), (i + 1) * (steps // 4), body, 0)
    with jax.named_scope("drain"):
        for i in range(steps):
            for cp in out_of(i):
                cp.wait()


def self_attention(new_pos, g1, hidden, wq, wk, wv, k_self, v_self):
    T2 = k_self.shape[1]
    return pl.pallas_call(
        self_kernel,
        in_specs=[pl.BlockSpec(memory_space=pltpu.SMEM), VM, VM, VM] + [ANY] * 6,
        out_specs=[ANY, ANY, VM, VM],
        scratch_shapes=[pltpu.VMEM(hidden.shape, BF), pltpu.VMEM(wq.shape, BF), pltpu.VMEM(wk.shape, BF),
                        pltpu.VMEM(wv.shape, BF), pltpu.SemaphoreType.DMA((4,)),
                        pltpu.VMEM((NB // SR, SR, T2, D), BF), pltpu.VMEM((NB // SR, SR, T2, D), BF),
                        pltpu.SemaphoreType.DMA((2, NB // SR)), pltpu.SemaphoreType.DMA((2, NB // SR)),
                        pltpu.VMEM((NB * 8, D), F32), pltpu.VMEM((NB * KL, D), F32), pltpu.VMEM((NB * KL, D), F32)],
        out_shape=[jax.ShapeDtypeStruct(k_self.shape, BF), jax.ShapeDtypeStruct(v_self.shape, BF),
                   jax.ShapeDtypeStruct((NB * HL, D), F32), jax.ShapeDtypeStruct((16, D), F32)],
        compiler_params=pltpu.CompilerParams(vmem_limit_bytes=VMEM_MAX),
        name="self_attn",
    )(new_pos, new_pos, jnp.asarray(rope_freqs(D)), g1, hidden, wq, wk, wv, k_self, v_self)


def peers():
    sp, tp = lax.axis_index("sp"), lax.axis_index("tp")
    core = lax.rem(tp, 2)
    return dict(sp=sp, core=core, y={"sp": 1 - sp}, c={"tp": tp + 1 - 2 * core}, x={"tp": lax.rem(tp + 2, 4)})


def entry_barrier(pe):
    barrier = pltpu.get_barrier_semaphore()
    for name in ("y", "c", "x"):
        pl.semaphore_signal(barrier, inc=1, device_id=pe[name], device_id_type=MESH)
    pl.semaphore_wait(barrier, 3)


def rcopy(src, dst, ssem, rsem, dev):
    return pltpu.make_async_remote_copy(src_ref=src, dst_ref=dst, send_sem=ssem, recv_sem=rsem,
                                        device_id=dev, device_id_type=MESH)


class TpSum:
    def __init__(self, pe, half, bufs):
        snd, rcv, chip, xr, sems = bufs
        self.snd, self.rcv, self.chip, self.xr = (b.at[half] for b in (snd, rcv, chip, xr))
        at = lambda n, j: sems.at[half, n, j]
        self.to_core = [rcopy(self.snd.at[j], self.rcv.at[j], at(0, j), at(1, j), pe["c"]) for j in range(NCH)]
        self.to_chip = [rcopy(self.chip.at[j], self.xr.at[j], at(2, j), at(3, j), pe["x"]) for j in range(NCH)]

    def start(self, compute):
        for j in range(NCH):
            part = compute(j)
            self.snd[j] = part[HQ:]
            self.chip[j] = part[:HQ]
            self.to_core[j].start()

    def forward(self):
        for j in range(NCH):
            self.to_core[j].wait_recv()
            self.chip[j] = self.chip[j] + self.rcv[j]
            self.to_chip[j].start()

    def close(self, finish):
        for j in range(NCH):
            self.to_chip[j].wait_recv()
            finish(j, self.chip[j] + self.xr[j])
        for j in range(NCH):
            self.to_core[j].wait_send()
            self.to_chip[j].wait_send()


class Share:
    def __init__(self, pe, half, x_ref, snd, rcv, sems):
        rows = pl.ds(half * HQ, HQ)
        self.snd, self.rcv, self.x = snd.at[rows], rcv.at[rows], x_ref.at[half]
        self.copy = rcopy(self.snd, self.rcv, sems.at[0, half], sems.at[1, half], pe["c"])

    def start(self, own):
        self.snd[...] = own.astype(F32)
        self.copy.start()
        self.x[pl.ds(0, HQ), :] = own

    def finish(self):
        self.copy.wait()
        self.x[pl.ds(HQ, HQ), :] = self.rcv[...].astype(BF)


def mlp_act(x_ref, wg, wu, act, chunks):
    step = act.shape[1] // 3
    for c in chunks:
        s = slice(c * step, (c + 1) * step)
        gate = dot(x_ref[...], wg[:, s]).astype(BF).astype(F32)
        up = dot(x_ref[...], wu[:, s]).astype(BF).astype(F32)
        act[:, s] = (gate * jax.nn.sigmoid(gate) * up).astype(BF)


def cols(j):
    return slice(j * W, (j + 1) * W)


def heads_to_lanes(ref, starts, rows):
    parts = [jnp.concatenate([ref[pl.ds(s * HL + h, rows, stride=HL), :] for h in range(HL)], axis=1) for s in starts]
    return jnp.concatenate(parts, axis=0).astype(BF)


CR = 8
NR = 5
RC = NQ // NCH
XB = 2 * RC // CR


def rest_kernel(o_hbm, st_ref, hid_hbm, g2_ref, g3_ref, qn_ref, g4_ref, gates_ref, mask_ref, valid_hbm,
                wo_hbm, wg_hbm, wu_hbm, wd_hbm, wq_hbm, wo2_hbm, wg2_hbm, wu2_hbm, wd2_hbm, k_hbm, v_hbm,
                out_ref,
                wo, wg, wu, wd, wq, wo2, wsem, kbuf, vbuf, ksem, osnd, orcv, sts, str_, ysem, hown, att, valid, cnt,
                qx, xbuf, act, hres, h2, fin, yr, cr, gsem,
                a0, a1, a2, a3, asem, b0, b1, b2, b3, bsem, c0, c1, c2, c3, csem, dsem,
                s0, s1, ssem, t0, t1, tsem, esem):
    pe = peers()
    sp, core = pe["sp"], pe["core"]
    T2 = k_hbm.shape[1]
    half = NH * HL
    blocks = NH // CR

    local = [pltpu.make_async_copy(o_hbm.at[pl.ds(pl.multiple_of((1 - sp) * half, half), half)], osnd, wsem.at[6]),
             pltpu.make_async_copy(o_hbm.at[pl.ds(pl.multiple_of(sp * half, half), half)], att, wsem.at[7]),
             pltpu.make_async_copy(hid_hbm.at[pl.ds(pl.multiple_of(sp * NH + core * NQ, NQ), NQ)], hown, wsem.at[8]),
             pltpu.make_async_copy(valid_hbm.at[pl.ds(pl.multiple_of(sp * NH, NH), NH)], valid, wsem.at[9])]
    pairs = ((wo_hbm, wo), (wg_hbm, wg), (wu_hbm, wu), (wd_hbm, wd), (wq_hbm, wq), (wo2_hbm, wo2))
    loads = [pltpu.make_async_copy(a, b, wsem.at[n]) for n, (a, b) in enumerate(pairs)]
    for cp in local:
        cp.start()

    def block_row(t):
        chunk, of_core, sub = t // XB, (t % XB) // (XB // 2), t % (XB // 2)
        return of_core * NQ + chunk * RC + sub * CR

    def kv_loads(t):
        rows, slot = pl.ds(pl.multiple_of(sp * NH + block_row(t), CR), CR), t % NR
        return (pltpu.make_async_copy(k_hbm.at[rows], kbuf.at[slot], ksem.at[0, slot]),
                pltpu.make_async_copy(v_hbm.at[rows], vbuf.at[slot], ksem.at[1, slot]))

    with jax.named_scope("enter"):
        entry_barrier(pe)
    both = st_ref[...]
    mine = jnp.where(sp == 0, both[:8], both[8:])
    sts[...] = jnp.where(sp == 0, both[8:], both[:8])
    local[0].wait()
    cp_s = rcopy(sts, str_, ysem.at[0, 4], ysem.at[1, 4], pe["y"])
    cp_s.start()

    def quarter(h, c):
        rows = pl.ds((c * NQ + h * HQ) * HL, HQ * HL)
        return rcopy(osnd.at[rows], orcv.at[rows], ysem.at[0, 2 * h + c], ysem.at[1, 2 * h + c], pe["y"])

    quarters = [quarter(h, c) for h in range(2) for c in range(2)]
    for cp in quarters:
        cp.start()
    for cp in local[1:]:
        cp.wait()
    for cp in loads:
        cp.start()
    for t in range(NR):
        for cp in kv_loads(t):
            cp.start()
    some = jnp.sum((valid[...] > 0).astype(jnp.int32), axis=1, keepdims=True)
    cnt[...] = jnp.broadcast_to(some, cnt.shape)
    row_scale = column(mask_ref[...].astype(F32).reshape(1, NB), sp * NH + core * NQ, NQ)
    gate0 = jnp.tanh(jnp.full((8, D), gates_ref[0], F32))[0:1, 0:1] * row_scale
    gate1 = jnp.tanh(jnp.full((8, D), gates_ref[1], F32))[0:1, 0:1] * row_scale
    gain = lambda ref: ref[...].astype(F32).reshape(1, HID)
    owned = [slice(h * HQ, (h + 1) * HQ) for h in range(2)]
    sum1 = [TpSum(pe, h, (a0, a1, a2, a3, asem)) for h in range(2)]
    sum2 = [TpSum(pe, h, (b0, b1, b2, b3, bsem)) for h in range(2)]
    sum4 = [TpSum(pe, h, (a0, a1, a2, a3, esem)) for h in range(2)]
    share1 = [Share(pe, h, xbuf, s0, s1, ssem) for h in range(2)]
    share2 = [Share(pe, h, xbuf, t0, t1, tsem) for h in range(2)]

    cp_s.wait()
    theirs = str_[...]
    top = jnp.maximum(mine, theirs)
    f1, f2 = jnp.exp(mine - top), jnp.exp(theirs - top)
    den = pltpu.roll(mine, NQ, 1) * f1 + pltpu.roll(theirs, NQ, 1) * f2
    w1, w2 = f1 / den, f2 / den

    def combine(h):
        for c in range(2):
            quarters[2 * h + c].wait()
            for p in range((c * NQ + h * HQ) // 2, (c * NQ + h * HQ + HQ) // 2):
                s = pl.ds(8 * p, 8)
                att[s, :] = att[s, :] * w1[:, p:p + 1] + orcv[s, :] * w2[:, p:p + 1]
        return heads_to_lanes(att, (core * NQ + h * HQ, (1 - core) * NQ + h * HQ), HQ)

    def close1(h):
        def done(j, total):
            hres[owned[h], cols(j)] = (hown[owned[h], cols(j)].astype(F32) + total).astype(BF)

        sum1[h].close(done)
        share1[h].start(norm32(hres[owned[h], :].astype(F32), gain(g2_ref)))

    def mlp_down(h, total):
        total.start(lambda j: dot(act[h], wd[:, cols(j)]))

    def mlp(h, total):
        mlp_act(xbuf.at[h], wg, wu, act.at[h], range(3))
        mlp_down(h, total)

    def close2(h):
        def done(j, total):
            h2[owned[h], cols(j)] = (hres[owned[h], cols(j)].astype(F32) + total).astype(BF)

        sum2[h].close(done)
        share2[h].start(norm32(h2[owned[h], :].astype(F32), gain(g3_ref)))

    def cross_q(h):
        share2[h].finish()
        q = dot(xbuf[h], wq[...])
        qgain = qn_ref[...].astype(F32).reshape(1, D)
        heads = [norm32(q[:, n * D:(n + 1) * D].astype(BF).astype(F32), qgain).astype(F32) for n in range(HL)]
        spread_heads(qx, [x[:HQ] for x in heads], core * NQ + h * HQ, HQ)
        spread_heads(qx, [x[HQ:] for x in heads], (1 - core) * NQ + h * HQ, HQ)

    with jax.named_scope("out_a"):
        lhs0 = combine(0)
        loads[0].wait()
        sum1[0].start(lambda j: dot(lhs0, wo[:, cols(j)]))
    with jax.named_scope("out_b"):
        sum1[0].forward()
        lhs1 = combine(1)
        sum1[1].start(lambda j: dot(lhs1, wo[:, cols(j)]))
        sum1[1].forward()
    with jax.named_scope("close1_a"):
        close1(0)
    with jax.named_scope("share1_a"):
        share1[0].finish()
    for cp in loads[1:4]:
        cp.wait()
    with jax.named_scope("mlp_a"):
        mlp(0, sum2[0])
        sum2[0].forward()
    with jax.named_scope("close1_b"):
        close1(1)
    with jax.named_scope("share1_b"):
        share1[1].finish()
    with jax.named_scope("mlp_b"):
        mlp(1, sum2[1])
        sum2[1].forward()
    loads2 = [pltpu.make_async_copy(a, b, wsem.at[1 + n])
              for n, (a, b) in enumerate(((wg2_hbm, wg), (wu2_hbm, wu), (wd2_hbm, wd)))]
    for cp in loads2:
        cp.start()
    with jax.named_scope("close2_a"):
        close2(0)
    loads[4].wait()
    with jax.named_scope("q_a"):
        cross_q(0)
    loads[5].wait()

    col = lax.broadcasted_iota(jnp.int32, (8, T2), 1)
    row = lax.broadcasted_iota(jnp.int32, (8, T2), 0)
    tok = col // KL
    head_ok = (col % KL) == ((row % HL) // (HL // KL))
    first = lax.broadcasted_iota(jnp.int32, (8, D), 0) < HL

    def block(t, _):
        slot = t % NR
        r0 = pl.multiple_of(block_row(t), CR)
        for cp in kv_loads(t):
            cp.wait()
        ps = range(CR // 2)
        lane_pair = lambda buf, p: jnp.concatenate([buf[slot, 2 * p], buf[slot, 2 * p + 1]], axis=1)
        n8 = cnt[pl.ds(r0, CR), :]
        limit = [jnp.concatenate([jnp.where(first, n8[2 * p:2 * p + 1], n8[2 * p + 1:2 * p + 2])] * (T2 // D), axis=1)
                 for p in ps]
        m, l, o = attend([pair_lhs(qx, r0 + 2 * p) for p in ps], [lane_pair(kbuf, p) for p in ps],
                         [lane_pair(vbuf, p) for p in ps], [head_ok & (tok < n) for n in limit])
        for p in ps:
            att[pl.ds(pl.multiple_of(r0 * HL + 8 * p, 8), 8), :] = o[p] / l[p]

        @pl.when(t + NR < blocks)
        def _():
            for cp in kv_loads(t + NR):
                cp.start()
        return 0

    to_core = [rcopy(c0.at[j], c1.at[j], csem.at[0, j], csem.at[1, j], pe["c"]) for j in range(NCH)]
    to_chip = [rcopy(c2.at[j], c3.at[j], csem.at[2, j], csem.at[3, j], pe["x"]) for j in range(NCH)]
    share = [rcopy(s0.at[pl.ds(j * RC, RC)], s1.at[pl.ds(j * RC, RC)], dsem.at[0, j], dsem.at[1, j], pe["c"])
             for j in range(NCH)]

    def pass_chip(j):
        to_core[j].wait_recv()
        c2[j] = c2[j] + c1[j]
        to_chip[j].start()

    def close3(j):
        mine = slice(j * RC, (j + 1) * RC)
        to_chip[j].wait_recv()
        hres[mine, :] = (h2[mine, :].astype(F32) + gate0[mine] * (c2[j] + c3[j])).astype(BF)
        own = norm32(hres[mine, :].astype(F32), gain(g4_ref))
        s0[mine, :] = own.astype(F32)
        share[j].start()
        xbuf[j // 2, pl.ds((j % 2) * RC, RC), :] = own

    def shared3(j):
        share[j].wait_recv()
        xbuf[j // 2, pl.ds(HQ + (j % 2) * RC, RC), :] = s1[pl.ds(j * RC, RC), :].astype(BF)

    def cross_out(j):
        lhs = heads_to_lanes(att, (core * NQ + j * RC, (1 - core) * NQ + j * RC), RC)
        for n in range(NCH):
            part = dot(lhs, wo2[:, cols(n)])
            c0[j, :, cols(n)] = part[RC:]
            c2[j, :, cols(n)] = part[:RC]
        to_core[j].start()

    to_y = [[rcopy(fin.at[h, j], yr.at[h, j], gsem.at[h, 0, j], gsem.at[h, 1, j], pe["y"]) for j in range(NCH)]
            for h in range(2)]
    to_c = [[rcopy(fin.at[h, j], cr.at[0, h, j], gsem.at[h, 2, j], gsem.at[h, 3, j], pe["c"]) for j in range(NCH)]
            for h in range(2)]
    pass_c = [[rcopy(yr.at[h, j], cr.at[1, h, j], gsem.at[h, 4, j], gsem.at[h, 5, j], pe["c"]) for j in range(NCH)]
              for h in range(2)]

    def rows(of_sp, of_core, h):
        return pl.ds(pl.multiple_of(of_sp * NH + of_core * NQ + h * HQ, HQ), HQ)

    def pass_on(h, j):
        to_y[h][j].wait_recv()
        pass_c[h][j].start()

    def close4(h, passing):
        def done(j, total):
            res = (hres[owned[h], cols(j)].astype(F32) + gate1[owned[h]] * total).astype(BF)
            out_ref[rows(sp, core, h), cols(j)] = res
            fin[h, j] = res.astype(F32)
            to_y[h][j].start()
            to_c[h][j].start()
            if passing is not None:
                pass_on(passing, j)

        sum4[h].close(done)

    def gathered(h):
        for j in range(NCH):
            out_ref[rows(1 - sp, core, h), cols(j)] = yr[h, j].astype(BF)
            to_c[h][j].wait_recv()
            out_ref[rows(sp, 1 - core, h), cols(j)] = cr[0, h, j].astype(BF)
        for j in range(NCH):
            pass_c[h][j].wait_recv()
            out_ref[rows(1 - sp, 1 - core, h), cols(j)] = cr[1, h, j].astype(BF)
        for j in range(NCH):
            to_y[h][j].wait_send()
            to_c[h][j].wait_send()
            pass_c[h][j].wait_send()

    blocks_to = lambda lo, hi: lax.fori_loop(lo, hi, block, 0)
    with jax.named_scope("x0"):
        blocks_to(0, 4)
    with jax.named_scope("o0"):
        cross_out(0)
    with jax.named_scope("x4"):
        blocks_to(4, 5)
    with jax.named_scope("pass0"):
        pass_chip(0)
    with jax.named_scope("x5"):
        blocks_to(5, 7)
    with jax.named_scope("close2_b"):
        close2(1)
    with jax.named_scope("x7"):
        blocks_to(7, 8)
    with jax.named_scope("o1"):
        cross_out(1)
    with jax.named_scope("q_b"):
        cross_q(1)
    with jax.named_scope("x8"):
        blocks_to(8, 9)
    with jax.named_scope("pass1"):
        pass_chip(1)
    with jax.named_scope("close3_0"):
        close3(0)
    with jax.named_scope("x9"):
        blocks_to(9, 12)
    with jax.named_scope("o2"):
        cross_out(2)
    with jax.named_scope("x12"):
        blocks_to(12, 13)
    with jax.named_scope("pass2"):
        pass_chip(2)
    with jax.named_scope("close3_1"):
        close3(1)
    with jax.named_scope("x13"):
        blocks_to(13, 16)
    with jax.named_scope("o3"):
        cross_out(3)
    with jax.named_scope("close3_2"):
        close3(2)
    with jax.named_scope("shared01"):
        shared3(0)
        shared3(1)
        for cp in loads2:
            cp.wait()
    with jax.named_scope("mlp2_a"):
        mlp_act(xbuf.at[0], wg, wu, act.at[0], (0,))
        pass_chip(3)
        mlp_act(xbuf.at[0], wg, wu, act.at[0], (1, 2))
        mlp_down(0, sum4[0])
    with jax.named_scope("forward4_a"):
        sum4[0].forward()
    with jax.named_scope("close3_3"):
        close3(3)
    with jax.named_scope("shared23"):
        shared3(2)
        shared3(3)
    with jax.named_scope("mlp2_b"):
        mlp(1, sum4[1])
    with jax.named_scope("forward4_b"):
        sum4[1].forward()
    with jax.named_scope("close4_a"):
        close4(0, None)
    with jax.named_scope("close4_b"):
        close4(1, 0)
    with jax.named_scope("gathered_a"):
        gathered(0)
    with jax.named_scope("gathered_b"):
        for j in range(NCH):
            pass_on(1, j)
        gathered(1)
    for j in range(NCH):
        to_core[j].wait_send()
        to_chip[j].wait_send()
        share[j].wait_send()


def rest_of_step(o, st, hidden, g2, g3, qn, g4, gates, mask, xvalid, ws, k_cross, v_cross):
    wo, wg, wu, wd, wq, wo2 = ws[:6]
    F = wg.shape[1]
    T2 = k_cross.shape[1]
    dma = pltpu.SemaphoreType.DMA
    sum_bufs = [pltpu.VMEM((2, NCH, HQ, W), F32)] * 4 + [dma((2, 4, NCH))]
    share_bufs = [pltpu.VMEM((NQ, HID), F32)] * 2 + [dma((2, 2))]
    return pl.pallas_call(
        rest_kernel,
        in_specs=[ANY, VM, ANY, VM, VM, VM, VM, pl.BlockSpec(memory_space=pltpu.SMEM), VM] + [ANY] * 12,
        out_specs=VM,
        out_shape=jax.ShapeDtypeStruct((NB, HID), BF),
        scratch_shapes=[pltpu.VMEM(w.shape, BF) for w in (wo, wg, wu, wd, wq, wo2)] + [
            dma((10,)), pltpu.VMEM((NR, CR, T2, D), BF), pltpu.VMEM((NR, CR, T2, D), BF), dma((2, NR)),
            pltpu.VMEM((NH * HL, D), F32), pltpu.VMEM((NH * HL, D), F32), pltpu.VMEM((8, D), F32),
            pltpu.VMEM((8, D), F32), dma((2, 5)), pltpu.VMEM((NQ, HID), BF), pltpu.VMEM((NH * HL, D), F32),
            pltpu.VMEM((NH, xvalid.shape[1]), jnp.int32), pltpu.VMEM((NH, D), jnp.int32),
            pltpu.VMEM((NH * 8, D), F32), pltpu.VMEM((2, NQ, HID), BF), pltpu.VMEM((2, NQ, F), BF),
            pltpu.VMEM((NQ, HID), BF), pltpu.VMEM((NQ, HID), BF), pltpu.VMEM((2, NCH, HQ, W), F32),
            pltpu.VMEM((2, NCH, HQ, W), F32), pltpu.VMEM((2, 2, NCH, HQ, W), F32), dma((2, 6, NCH))]
        + sum_bufs + sum_bufs + [pltpu.VMEM((NCH, RC, HID), F32)] * 4 + [dma((4, NCH)), dma((2, NCH))]
        + share_bufs + share_bufs + [dma((2, 4, NCH))],
        compiler_params=pltpu.CompilerParams(collective_id=0, has_side_effects=True, vmem_limit_bytes=VMEM_MAX),
        name="rest_of_step",
    )(o, st, hidden, g2, g3, qn, g4, gates, mask, xvalid, *ws, k_cross, v_cross)


def solution(mesh):
    cache_spec = P('dp', 'sp', 'tp', None)
    cross_spec = P('dp', None, 'tp', None)
    row_spec = P('dp', None)
    vec_spec = P('dp')
    full_spec = P(None)
    col_spec = P(None, 'tp')
    split_rows = P('tp', None)
    in_specs = (row_spec, vec_spec, cache_spec, cache_spec, cross_spec, cross_spec, row_spec, vec_spec,
                full_spec, col_spec, col_spec, col_spec, split_rows, full_spec, col_spec, col_spec, split_rows,
                full_spec, col_spec, full_spec, split_rows, full_spec, full_spec, col_spec, col_spec, split_rows)
    out_specs = (row_spec, cache_spec, cache_spec)

    def local_step(hidden, new_pos, k_self, v_self, k_cross, v_cross, xvalid, rowmask,
                   self_attn_norm, self_wq, self_wk, self_wv, self_wo, self_mlp_norm,
                   self_wgate, self_wup, self_wdown, cross_attn_norm, cross_wq, cross_qnorm,
                   cross_wo, cross_gates, cross_mlp_norm, cross_wgate, cross_wup, cross_wdown):
        flat = lambda a: a.reshape(a.shape[0], a.shape[1] * a.shape[2], a.shape[3])
        k_out, v_out, o, st = self_attention(new_pos, self_attn_norm, hidden, self_wq, self_wk, self_wv,
                                             flat(k_self), flat(v_self))
        weights = (self_wo, self_wgate, self_wup, self_wdown, cross_wq, cross_wo, cross_wgate, cross_wup, cross_wdown)
        h4 = rest_of_step(o, st, hidden, self_mlp_norm, cross_attn_norm, cross_qnorm, cross_mlp_norm, cross_gates,
                          rowmask, xvalid, weights, flat(k_cross), flat(v_cross))
        return h4, k_out.reshape(k_self.shape), v_out.reshape(v_self.shape)

    return jax.shard_map(local_step, mesh=mesh, in_specs=in_specs, out_specs=out_specs, check_vma=False)
```

```python
import functools
import math
import numpy as np
import jax
import jax.numpy as jnp
from jax import lax
from jax.experimental import pallas as pl
from jax.experimental.pallas import tpu as pltpu
from jax.sharding import PartitionSpec as P

NORM_EPS = 1e-5
ROPE_THETA = 500000.0
ROPE_FACTOR = 8.0
LOW_FREQ = 1.0
HIGH_FREQ = 4.0
ORIG_CTX = 8192.0
NEG_BIG = -1e30

BF = jnp.bfloat16
F32 = jnp.float32
D = 128
HL = 4
KL = 2
NB = 256
NH = 128
NQ = 64
HID = 2048
HQ = NQ // 2
NCH = 4
W = HID // NCH
VMEM_MAX = 66 * 1024 * 1024 - 2 * 1024 * 1024
MESH = pl.DeviceIdType.MESH
ANY = pl.BlockSpec(memory_space=pl.ANY)
VM = pl.BlockSpec(memory_space=pltpu.VMEM)


def rope_freqs(head_dim):
    inv_freq = 1.0 / (ROPE_THETA ** (np.arange(0, head_dim, 2) / head_dim))
    wavelen = 2.0 * math.pi / inv_freq
    smooth = (ORIG_CTX / wavelen - LOW_FREQ) / (HIGH_FREQ - LOW_FREQ)
    mid_freq = (1.0 - smooth) * inv_freq / ROPE_FACTOR + smooth * inv_freq
    scaled = np.where(wavelen > ORIG_CTX / LOW_FREQ, inv_freq / ROPE_FACTOR, mid_freq)
    scaled = np.where(wavelen < ORIG_CTX / HIGH_FREQ, inv_freq, scaled)
    return np.concatenate([scaled, scaled]).astype(np.float32)[None, :]


def norm32(vals32, gain32):
    inv = lax.rsqrt(jnp.mean(vals32 * vals32, axis=-1, keepdims=True) + NORM_EPS)
    return (vals32 * inv * gain32).astype(BF)


def dot(a, b):
    return jnp.dot(a, b, preferred_element_type=F32)


def dot_nt(a, b):
    return lax.dot_general(a, b, (((1,), (1,)), ((), ())), preferred_element_type=F32)


def attend(lhs, keys, vals, valid):
    first = lax.broadcasted_iota(jnp.int32, (8, D), 0) < HL
    s = [dot_nt(a, k) * (D ** -0.5) for a, k in zip(lhs, keys)]
    s = [jnp.where(ok, x, NEG_BIG) for ok, x in zip(valid, s)]
    m = [jnp.max(x, axis=-1, keepdims=True) for x in s]
    p = [jnp.where(ok, jnp.exp(x - t), 0.0) for ok, x, t in zip(valid, s, m)]
    l = [jnp.sum(x, axis=-1, keepdims=True) for x in p]
    o = [dot(x.astype(BF), v) for x, v in zip(p, vals)]
    return m, l, [jnp.where(first, x[:, :D], x[:, D:]) for x in o]


def pair_lhs(q_ref, b0):
    q16 = q_ref[pl.ds(pl.multiple_of(b0 * 8, 16), 16), :]
    return jnp.concatenate([q16[:8], q16[8:]], axis=1).astype(BF)


def column(vec, first, rows):
    n = vec.shape[1]
    at = lax.broadcasted_iota(jnp.int32, (rows, n), 1) == lax.broadcasted_iota(jnp.int32, (rows, n), 0) + first
    return jnp.sum(jnp.where(at, vec, 0.0), axis=1, keepdims=True)


def spread_heads(ref, heads, start, rows):
    odd = (lax.broadcasted_iota(jnp.int32, (rows, D), 0) % 2) == 1
    for h in range(HL):
        ref[pl.ds(start * 8 + h, rows, stride=8), :] = jnp.where(odd, 0.0, heads[h])
        ref[pl.ds(start * 8 + HL + h, rows, stride=8), :] = jnp.where(odd, heads[h], 0.0)


SR = 16


def self_kernel(pos_ref, posv_ref, freq_ref, g_ref, hid_hbm, wq_hbm, wk_hbm, wv_hbm, k_hbm, v_hbm,
                ko_hbm, vo_hbm, o_hbm, st_hbm,
                hid, wq, wk, wv, wsem, kbuf, vbuf, isem, osem, qs, kn, vn, o_ref, st_ref, rsem):
    T2 = k_hbm.shape[1]
    steps = NB // SR
    first_pos = lax.axis_index("sp") * (T2 // KL)
    loads = [pltpu.make_async_copy(a, b, wsem.at[n])
             for n, (a, b) in enumerate(((hid_hbm, hid), (wq_hbm, wq), (wk_hbm, wk), (wv_hbm, wv)))]
    for cp in loads:
        cp.start()

    def into(i):
        rows = pl.ds(pl.multiple_of(i * SR, SR), SR)
        return (pltpu.make_async_copy(k_hbm.at[rows], kbuf.at[i], isem.at[0, i]),
                pltpu.make_async_copy(v_hbm.at[rows], vbuf.at[i], isem.at[1, i]))

    def out_of(i):
        rows = pl.ds(pl.multiple_of(i * SR, SR), SR)
        return (pltpu.make_async_copy(kbuf.at[i], ko_hbm.at[rows], osem.at[0, i]),
                pltpu.make_async_copy(vbuf.at[i], vo_hbm.at[rows], osem.at[1, i]))

    early = 5
    for i in range(early):
        for cp in into(i):
            cp.start()

    with jax.named_scope("qkv"):
        angle = column(posv_ref[...].astype(F32).reshape(1, NB), 0, NB) * freq_ref[...]
        cos, sin = jnp.cos(angle), jnp.sin(angle)
        sin = jnp.where(lax.broadcasted_iota(jnp.int32, (NB, D), 1) < D // 2, -sin, sin)

        def rope(part):
            part = part.astype(BF).astype(F32)
            return (part * cos + pltpu.roll(part, D // 2, 1) * sin).astype(BF).astype(F32)

        loads[0].wait()
        loads[1].wait()
        for i in range(early, steps):
            for cp in into(i):
                cp.start()
        x = norm32(hid[...].astype(F32), g_ref[...].astype(F32).reshape(1, HID))
        q = dot(x, wq[...])
        spread_heads(qs, [rope(q[:, h * D:(h + 1) * D]) for h in range(HL)], 0, NB)
        loads[2].wait()
        k = dot(x, wk[...])
        loads[3].wait()
        v = dot(x, wv[...])
        for h in range(KL):
            kn[pl.ds(h, NB, stride=KL), :] = rope(k[:, h * D:(h + 1) * D])
            vn[pl.ds(h, NB, stride=KL), :] = v[:, h * D:(h + 1) * D].astype(BF).astype(F32)
    st_ref[...] = jnp.zeros_like(st_ref)

    col = lax.broadcasted_iota(jnp.int32, (8, T2), 1)
    row = lax.broadcasted_iota(jnp.int32, (8, T2), 0)
    tok = col // KL
    head_ok = (col % KL) == ((row % HL) // (HL // KL))
    lane = lax.broadcasted_iota(jnp.int32, (8, D), 1)
    i16 = lax.broadcasted_iota(jnp.int32, (16, D), 0)

    def patch(new_ref, dst_ref, slot, r, b, lp):
        base = pl.multiple_of((jnp.clip(lp, 0, T2 // KL - 1) // 8) * 16, 16)
        fresh = jnp.where(i16 % 2 == 0, new_ref[pl.ds(2 * b, 1), :], new_ref[pl.ds(2 * b + 1, 1), :])
        old = dst_ref[slot, r, pl.ds(base, 16), :].astype(F32)
        dst_ref[slot, r, pl.ds(base, 16), :] = jnp.where(base + i16 - i16 % 2 == 2 * lp, fresh, old).astype(BF)

    def body(i, _):
        for cp in into(i):
            cp.wait()
        lps = [pos_ref[i * SR + r] - first_pos for r in range(SR)]
        for r in range(SR):
            patch(kn, kbuf, i, r, i * SR + r, lps[r])
            patch(vn, vbuf, i, r, i * SR + r, lps[r])
        pairs = range(SR // 2)
        both = lambda buf, p: jnp.concatenate([buf[i, 2 * p], buf[i, 2 * p + 1]], axis=1)
        m, l, o = attend([pair_lhs(qs, i * SR + 2 * p) for p in pairs], [both(kbuf, p) for p in pairs],
                         [both(vbuf, p) for p in pairs],
                         [head_ok & (tok <= jnp.where(row < HL, lps[2 * p], lps[2 * p + 1])) for p in pairs])
        half = i // (NH // SR)
        srow = pl.ds(pl.multiple_of(half * 8, 8), 8)
        st = st_ref[srow, :]
        for p in pairs:
            o_ref[pl.ds(pl.multiple_of(i * SR * HL + 8 * p, 8), 8), :] = o[p]
            at = (i - half * (NH // SR)) * (SR // 2) + p
            st = jnp.where(lane == at, m[p], jnp.where(lane == at + NQ, l[p], st))
        st_ref[srow, :] = st
        for cp in out_of(i):
            cp.start()
        return 0

    results = []
    for i in range(4):
        with jax.named_scope("steps"):
            lax.fori_loop(i * (steps // 4), (i + 1) * (steps // 4), body, 0)
        part = pl.ds(i * (NB * HL // 4), NB * HL // 4)
        results.append(pltpu.make_async_copy(o_ref.at[part], o_hbm.at[part], rsem.at[i]))
        results[-1].start()
    results.append(pltpu.make_async_copy(st_ref, st_hbm, rsem.at[4]))
    results[-1].start()
    with jax.named_scope("drain"):
        for i in range(steps):
            for cp in out_of(i):
                cp.wait()
        for cp in results:
            cp.wait()


def self_attention(new_pos, g1, hidden, wq, wk, wv, k_self, v_self):
    T2 = k_self.shape[1]
    return pl.pallas_call(
        self_kernel,
        in_specs=[pl.BlockSpec(memory_space=pltpu.SMEM), VM, VM, VM] + [ANY] * 6,
        out_specs=[ANY] * 4,
        scratch_shapes=[pltpu.VMEM(hidden.shape, BF), pltpu.VMEM(wq.shape, BF), pltpu.VMEM(wk.shape, BF),
                        pltpu.VMEM(wv.shape, BF), pltpu.SemaphoreType.DMA((4,)),
                        pltpu.VMEM((NB // SR, SR, T2, D), BF), pltpu.VMEM((NB // SR, SR, T2, D), BF),
                        pltpu.SemaphoreType.DMA((2, NB // SR)), pltpu.SemaphoreType.DMA((2, NB // SR)),
                        pltpu.VMEM((NB * 8, D), F32), pltpu.VMEM((NB * KL, D), F32), pltpu.VMEM((NB * KL, D), F32),
                        pltpu.VMEM((NB * HL, D), F32), pltpu.VMEM((16, D), F32), pltpu.SemaphoreType.DMA((5,))],
        out_shape=[jax.ShapeDtypeStruct(k_self.shape, BF), jax.ShapeDtypeStruct(v_self.shape, BF),
                   jax.ShapeDtypeStruct((NB * HL, D), F32), jax.ShapeDtypeStruct((16, D), F32)],
        compiler_params=pltpu.CompilerParams(vmem_limit_bytes=VMEM_MAX),
        name="self_attn",
    )(new_pos, new_pos, jnp.asarray(rope_freqs(D)), g1, hidden, wq, wk, wv, k_self, v_self)


def peers():
    sp, tp = lax.axis_index("sp"), lax.axis_index("tp")
    core = lax.rem(tp, 2)
    return dict(sp=sp, core=core, y={"sp": 1 - sp}, c={"tp": tp + 1 - 2 * core}, x={"tp": lax.rem(tp + 2, 4)})


def entry_barrier(pe):
    barrier = pltpu.get_barrier_semaphore()
    for name in ("y", "c", "x"):
        pl.semaphore_signal(barrier, inc=1, device_id=pe[name], device_id_type=MESH)
    pl.semaphore_wait(barrier, 3)


def rcopy(src, dst, ssem, rsem, dev):
    return pltpu.make_async_remote_copy(src_ref=src, dst_ref=dst, send_sem=ssem, recv_sem=rsem,
                                        device_id=dev, device_id_type=MESH)


class TpSum:
    def __init__(self, pe, half, bufs):
        snd, rcv, chip, xr, sems = bufs
        self.snd, self.rcv, self.chip, self.xr = (b.at[half] for b in (snd, rcv, chip, xr))
        at = lambda n, j: sems.at[half, n, j]
        self.to_core = [rcopy(self.snd.at[j], self.rcv.at[j], at(0, j), at(1, j), pe["c"]) for j in range(NCH)]
        self.to_chip = [rcopy(self.chip.at[j], self.xr.at[j], at(2, j), at(3, j), pe["x"]) for j in range(NCH)]

    def start(self, compute):
        for j in range(NCH):
            part = compute(j)
            self.snd[j] = part[HQ:]
            self.chip[j] = part[:HQ]
            self.to_core[j].start()

    def forward(self):
        for j in range(NCH):
            self.to_core[j].wait_recv()
            self.chip[j] = self.chip[j] + self.rcv[j]
            self.to_chip[j].start()

    def close(self, finish):
        for j in range(NCH):
            self.to_chip[j].wait_recv()
            finish(j, self.chip[j] + self.xr[j])
        for j in range(NCH):
            self.to_core[j].wait_send()
            self.to_chip[j].wait_send()


class Share:
    def __init__(self, pe, half, x_ref, snd, rcv, sems):
        rows = pl.ds(half * HQ, HQ)
        self.snd, self.rcv, self.x = snd.at[rows], rcv.at[rows], x_ref.at[half]
        self.copy = rcopy(self.snd, self.rcv, sems.at[0, half], sems.at[1, half], pe["c"])

    def start(self, own):
        self.snd[...] = own.astype(F32)
        self.copy.start()
        self.x[pl.ds(0, HQ), :] = own

    def finish(self):
        self.copy.wait()
        self.x[pl.ds(HQ, HQ), :] = self.rcv[...].astype(BF)


def mlp_act(x_ref, wg, wu, act, chunks):
    step = act.shape[1] // 3
    for c in chunks:
        s = slice(c * step, (c + 1) * step)
        gate = dot(x_ref[...], wg[:, s]).astype(BF).astype(F32)
        up = dot(x_ref[...], wu[:, s]).astype(BF).astype(F32)
        act[:, s] = (gate * jax.nn.sigmoid(gate) * up).astype(BF)


def cols(j):
    return slice(j * W, (j + 1) * W)


def heads_to_lanes(ref, starts, rows):
    parts = [jnp.concatenate([ref[pl.ds(s * HL + h, rows, stride=HL), :] for h in range(HL)], axis=1) for s in starts]
    return jnp.concatenate(parts, axis=0).astype(BF)


CR = 8
NR = 5
RC = NQ // NCH
XB = 2 * RC // CR


def rest_kernel(o_hbm, st_ref, hid_hbm, g2_ref, g3_ref, qn_ref, g4_ref, gates_ref, mask_ref, valid_hbm,
                wo_hbm, wg_hbm, wu_hbm, wd_hbm, wq_hbm, wo2_hbm, wg2_hbm, wu2_hbm, wd2_hbm, k_hbm, v_hbm,
                out_hbm,
                out_ref, rsem, wo, wg, wu, wd, wq, wo2, wsem, kbuf, vbuf, ksem, osnd, orcv, sts, str_, ysem, hown, att, valid, cnt,
                qx, xbuf, act, hres, h2, fin, yr, cr, gsem,
                a0, a1, a2, a3, asem, b0, b1, b2, b3, bsem, c0, c1, c2, c3, csem, dsem,
                s0, s1, ssem, t0, t1, tsem, esem):
    pe = peers()
    sp, core = pe["sp"], pe["core"]
    T2 = k_hbm.shape[1]
    half = NH * HL
    blocks = NH // CR

    local = [pltpu.make_async_copy(o_hbm.at[pl.ds(pl.multiple_of((1 - sp) * half, half), half)], osnd, wsem.at[6]),
             pltpu.make_async_copy(o_hbm.at[pl.ds(pl.multiple_of(sp * half, half), half)], att, wsem.at[7]),
             pltpu.make_async_copy(hid_hbm.at[pl.ds(pl.multiple_of(sp * NH + core * NQ, NQ), NQ)], hown, wsem.at[8]),
             pltpu.make_async_copy(valid_hbm.at[pl.ds(pl.multiple_of(sp * NH, NH), NH)], valid, wsem.at[9])]
    pairs = ((wo_hbm, wo), (wg_hbm, wg), (wu_hbm, wu), (wd_hbm, wd), (wq_hbm, wq), (wo2_hbm, wo2))
    loads = [pltpu.make_async_copy(a, b, wsem.at[n]) for n, (a, b) in enumerate(pairs)]
    for cp in local:
        cp.start()

    def block_row(t):
        chunk, of_core, sub = t // XB, (t % XB) // (XB // 2), t % (XB // 2)
        return of_core * NQ + chunk * RC + sub * CR

    def kv_loads(t):
        rows, slot = pl.ds(pl.multiple_of(sp * NH + block_row(t), CR), CR), t % NR
        return (pltpu.make_async_copy(k_hbm.at[rows], kbuf.at[slot], ksem.at[0, slot]),
                pltpu.make_async_copy(v_hbm.at[rows], vbuf.at[slot], ksem.at[1, slot]))

    with jax.named_scope("enter"):
        entry_barrier(pe)
    both = st_ref[...]
    mine = jnp.where(sp == 0, both[:8], both[8:])
    sts[...] = jnp.where(sp == 0, both[8:], both[:8])
    local[0].wait()
    cp_s = rcopy(sts, str_, ysem.at[0, 4], ysem.at[1, 4], pe["y"])
    cp_s.start()

    def quarter(h, c):
        rows = pl.ds((c * NQ + h * HQ) * HL, HQ * HL)
        return rcopy(osnd.at[rows], orcv.at[rows], ysem.at[0, 2 * h + c], ysem.at[1, 2 * h + c], pe["y"])

    quarters = [quarter(h, c) for h in range(2) for c in range(2)]
    for cp in quarters:
        cp.start()
    for cp in local[1:]:
        cp.wait()
    for cp in loads:
        cp.start()
    for t in range(NR):
        for cp in kv_loads(t):
            cp.start()
    some = jnp.sum((valid[...] > 0).astype(jnp.int32), axis=1, keepdims=True)
    cnt[...] = jnp.broadcast_to(some, cnt.shape)
    row_scale = column(mask_ref[...].astype(F32).reshape(1, NB), sp * NH + core * NQ, NQ)
    gate0 = jnp.tanh(jnp.full((8, D), gates_ref[0], F32))[0:1, 0:1] * row_scale
    gate1 = jnp.tanh(jnp.full((8, D), gates_ref[1], F32))[0:1, 0:1] * row_scale
    gain = lambda ref: ref[...].astype(F32).reshape(1, HID)
    owned = [slice(h * HQ, (h + 1) * HQ) for h in range(2)]
    sum1 = [TpSum(pe, h, (a0, a1, a2, a3, asem)) for h in range(2)]
    sum2 = [TpSum(pe, h, (b0, b1, b2, b3, bsem)) for h in range(2)]
    sum4 = [TpSum(pe, h, (a0, a1, a2, a3, esem)) for h in range(2)]
    share1 = [Share(pe, h, xbuf, s0, s1, ssem) for h in range(2)]
    share2 = [Share(pe, h, xbuf, t0, t1, tsem) for h in range(2)]

    cp_s.wait()
    theirs = str_[...]
    top = jnp.maximum(mine, theirs)
    f1, f2 = jnp.exp(mine - top), jnp.exp(theirs - top)
    den = pltpu.roll(mine, NQ, 1) * f1 + pltpu.roll(theirs, NQ, 1) * f2
    w1, w2 = f1 / den, f2 / den

    def combine(h):
        for c in range(2):
            quarters[2 * h + c].wait()
            for p in range((c * NQ + h * HQ) // 2, (c * NQ + h * HQ + HQ) // 2):
                s = pl.ds(8 * p, 8)
                att[s, :] = att[s, :] * w1[:, p:p + 1] + orcv[s, :] * w2[:, p:p + 1]
        return heads_to_lanes(att, (core * NQ + h * HQ, (1 - core) * NQ + h * HQ), HQ)

    def close1(h):
        def done(j, total):
            hres[owned[h], cols(j)] = (hown[owned[h], cols(j)].astype(F32) + total).astype(BF)

        sum1[h].close(done)
        share1[h].start(norm32(hres[owned[h], :].astype(F32), gain(g2_ref)))

    def mlp_down(h, total):
        total.start(lambda j: dot(act[h], wd[:, cols(j)]))

    def mlp(h, total):
        mlp_act(xbuf.at[h], wg, wu, act.at[h], range(3))
        mlp_down(h, total)

    def close2(h):
        def done(j, total):
            h2[owned[h], cols(j)] = (hres[owned[h], cols(j)].astype(F32) + total).astype(BF)

        sum2[h].close(done)
        share2[h].start(norm32(h2[owned[h], :].astype(F32), gain(g3_ref)))

    def cross_q(h):
        share2[h].finish()
        q = dot(xbuf[h], wq[...])
        qgain = qn_ref[...].astype(F32).reshape(1, D)
        heads = [norm32(q[:, n * D:(n + 1) * D].astype(BF).astype(F32), qgain).astype(F32) for n in range(HL)]
        spread_heads(qx, [x[:HQ] for x in heads], core * NQ + h * HQ, HQ)
        spread_heads(qx, [x[HQ:] for x in heads], (1 - core) * NQ + h * HQ, HQ)

    with jax.named_scope("out_a"):
        lhs0 = combine(0)
        loads[0].wait()
        sum1[0].start(lambda j: dot(lhs0, wo[:, cols(j)]))
    with jax.named_scope("out_b"):
        sum1[0].forward()
        lhs1 = combine(1)
        sum1[1].start(lambda j: dot(lhs1, wo[:, cols(j)]))
        sum1[1].forward()
    with jax.named_scope("close1_a"):
        close1(0)
    with jax.named_scope("share1_a"):
        share1[0].finish()
    for cp in loads[1:4]:
        cp.wait()
    with jax.named_scope("mlp_a"):
        mlp(0, sum2[0])
        sum2[0].forward()
    with jax.named_scope("close1_b"):
        close1(1)
    with jax.named_scope("share1_b"):
        share1[1].finish()
    with jax.named_scope("mlp_b"):
        mlp(1, sum2[1])
        sum2[1].forward()
    loads2 = [pltpu.make_async_copy(a, b, wsem.at[1 + n])
              for n, (a, b) in enumerate(((wg2_hbm, wg), (wu2_hbm, wu), (wd2_hbm, wd)))]
    for cp in loads2:
        cp.start()
    with jax.named_scope("close2_a"):
        close2(0)
    loads[4].wait()
    with jax.named_scope("q_a"):
        cross_q(0)
    loads[5].wait()

    col = lax.broadcasted_iota(jnp.int32, (8, T2), 1)
    row = lax.broadcasted_iota(jnp.int32, (8, T2), 0)
    tok = col // KL
    head_ok = (col % KL) == ((row % HL) // (HL // KL))
    first = lax.broadcasted_iota(jnp.int32, (8, D), 0) < HL

    def block(t, _):
        slot = t % NR
        r0 = pl.multiple_of(block_row(t), CR)
        for cp in kv_loads(t):
            cp.wait()
        ps = range(CR // 2)
        lane_pair = lambda buf, p: jnp.concatenate([buf[slot, 2 * p], buf[slot, 2 * p + 1]], axis=1)
        n8 = cnt[pl.ds(r0, CR), :]
        limit = [jnp.concatenate([jnp.where(first, n8[2 * p:2 * p + 1], n8[2 * p + 1:2 * p + 2])] * (T2 // D), axis=1)
                 for p in ps]
        m, l, o = attend([pair_lhs(qx, r0 + 2 * p) for p in ps], [lane_pair(kbuf, p) for p in ps],
                         [lane_pair(vbuf, p) for p in ps], [head_ok & (tok < n) for n in limit])
        for p in ps:
            att[pl.ds(pl.multiple_of(r0 * HL + 8 * p, 8), 8), :] = o[p] / l[p]

        @pl.when(t + NR < blocks)
        def _():
            for cp in kv_loads(t + NR):
                cp.start()
        return 0

    to_core = [rcopy(c0.at[j], c1.at[j], csem.at[0, j], csem.at[1, j], pe["c"]) for j in range(NCH)]
    to_chip = [rcopy(c2.at[j], c3.at[j], csem.at[2, j], csem.at[3, j], pe["x"]) for j in range(NCH)]
    share = [rcopy(s0.at[pl.ds(j * RC, RC)], s1.at[pl.ds(j * RC, RC)], dsem.at[0, j], dsem.at[1, j], pe["c"])
             for j in range(NCH)]

    def pass_chip(j):
        to_core[j].wait_recv()
        c2[j] = c2[j] + c1[j]
        to_chip[j].start()

    def close3(j):
        mine = slice(j * RC, (j + 1) * RC)
        to_chip[j].wait_recv()
        hres[mine, :] = (h2[mine, :].astype(F32) + gate0[mine] * (c2[j] + c3[j])).astype(BF)
        own = norm32(hres[mine, :].astype(F32), gain(g4_ref))
        s0[mine, :] = own.astype(F32)
        share[j].start()
        xbuf[j // 2, pl.ds((j % 2) * RC, RC), :] = own

    def shared3(j):
        share[j].wait_recv()
        xbuf[j // 2, pl.ds(HQ + (j % 2) * RC, RC), :] = s1[pl.ds(j * RC, RC), :].astype(BF)

    def cross_out(j):
        lhs = heads_to_lanes(att, (core * NQ + j * RC, (1 - core) * NQ + j * RC), RC)
        for n in range(NCH):
            part = dot(lhs, wo2[:, cols(n)])
            c0[j, :, cols(n)] = part[RC:]
            c2[j, :, cols(n)] = part[:RC]
        to_core[j].start()

    to_y = [[rcopy(fin.at[h, j], yr.at[h, j], gsem.at[h, 0, j], gsem.at[h, 1, j], pe["y"]) for j in range(NCH)]
            for h in range(2)]
    to_c = [[rcopy(fin.at[h, j], cr.at[0, h, j], gsem.at[h, 2, j], gsem.at[h, 3, j], pe["c"]) for j in range(NCH)]
            for h in range(2)]
    pass_c = [[rcopy(yr.at[h, j], cr.at[1, h, j], gsem.at[h, 4, j], gsem.at[h, 5, j], pe["c"]) for j in range(NCH)]
              for h in range(2)]

    def rows(of_sp, of_core, h):
        return pl.ds(pl.multiple_of(of_sp * NH + of_core * NQ + h * HQ, HQ), HQ)

    outs = []

    def put(of_sp, of_core, h):
        r = rows(of_sp, of_core, h)
        outs.append(pltpu.make_async_copy(out_ref.at[r], out_hbm.at[r], rsem.at[len(outs)]))
        outs[-1].start()

    def pass_on(h, j):
        to_y[h][j].wait_recv()
        pass_c[h][j].start()

    def close4(h, passing):
        def done(j, total):
            res = (hres[owned[h], cols(j)].astype(F32) + gate1[owned[h]] * total).astype(BF)
            out_ref[rows(sp, core, h), cols(j)] = res
            fin[h, j] = res.astype(F32)
            to_y[h][j].start()
            to_c[h][j].start()
            if passing is not None:
                pass_on(passing, j)

        sum4[h].close(done)
        put(sp, core, h)

    def gathered(h):
        for j in range(NCH):
            to_c[h][j].wait_recv()
            out_ref[rows(sp, 1 - core, h), cols(j)] = cr[0, h, j].astype(BF)
        put(sp, 1 - core, h)
        for j in range(NCH):
            out_ref[rows(1 - sp, core, h), cols(j)] = yr[h, j].astype(BF)
        put(1 - sp, core, h)
        for j in range(NCH):
            pass_c[h][j].wait_recv()
            out_ref[rows(1 - sp, 1 - core, h), cols(j)] = cr[1, h, j].astype(BF)
        put(1 - sp, 1 - core, h)
        for j in range(NCH):
            to_y[h][j].wait_send()
            to_c[h][j].wait_send()
            pass_c[h][j].wait_send()

    blocks_to = lambda lo, hi: lax.fori_loop(lo, hi, block, 0)
    with jax.named_scope("x0"):
        blocks_to(0, 4)
    with jax.named_scope("o0"):
        cross_out(0)
    with jax.named_scope("x4"):
        blocks_to(4, 5)
    with jax.named_scope("pass0"):
        pass_chip(0)
    with jax.named_scope("x5"):
        blocks_to(5, 7)
    with jax.named_scope("close2_b"):
        close2(1)
    with jax.named_scope("x7"):
        blocks_to(7, 8)
    with jax.named_scope("o1"):
        cross_out(1)
    with jax.named_scope("q_b"):
        cross_q(1)
    with jax.named_scope("x8"):
        blocks_to(8, 9)
    with jax.named_scope("pass1"):
        pass_chip(1)
    with jax.named_scope("close3_0"):
        close3(0)
    with jax.named_scope("x9"):
        blocks_to(9, 12)
    with jax.named_scope("o2"):
        cross_out(2)
    with jax.named_scope("x12"):
        blocks_to(12, 13)
    with jax.named_scope("pass2"):
        pass_chip(2)
    with jax.named_scope("close3_1"):
        close3(1)
    with jax.named_scope("x13"):
        blocks_to(13, 16)
    with jax.named_scope("o3"):
        cross_out(3)
    with jax.named_scope("shared01"):
        shared3(0)
        shared3(1)
        for cp in loads2:
            cp.wait()
    with jax.named_scope("mlp2_a"):
        mlp_act(xbuf.at[0], wg, wu, act.at[0], (0,))
        pass_chip(3)
        mlp_act(xbuf.at[0], wg, wu, act.at[0], (1,))
        close3(2)
        mlp_act(xbuf.at[0], wg, wu, act.at[0], (2,))
        mlp_down(0, sum4[0])
    with jax.named_scope("forward4_a"):
        sum4[0].forward()
    with jax.named_scope("close3_3"):
        close3(3)
    with jax.named_scope("shared23"):
        shared3(2)
        shared3(3)
    with jax.named_scope("mlp2_b"):
        mlp(1, sum4[1])
    with jax.named_scope("forward4_b"):
        sum4[1].forward()
    with jax.named_scope("close4_a"):
        close4(0, None)
    with jax.named_scope("close4_b"):
        close4(1, 0)
    with jax.named_scope("gathered_a"):
        gathered(0)
    with jax.named_scope("gathered_b"):
        for j in range(NCH):
            pass_on(1, j)
        gathered(1)
    for j in range(NCH):
        to_core[j].wait_send()
        to_chip[j].wait_send()
        share[j].wait_send()
    for cp in outs:
        cp.wait()


def rest_of_step(o, st, hidden, g2, g3, qn, g4, gates, mask, xvalid, ws, k_cross, v_cross):
    wo, wg, wu, wd, wq, wo2 = ws[:6]
    F = wg.shape[1]
    T2 = k_cross.shape[1]
    dma = pltpu.SemaphoreType.DMA
    sum_bufs = [pltpu.VMEM((2, NCH, HQ, W), F32)] * 4 + [dma((2, 4, NCH))]
    share_bufs = [pltpu.VMEM((NQ, HID), F32)] * 2 + [dma((2, 2))]
    return pl.pallas_call(
        rest_kernel,
        in_specs=[ANY, VM, ANY, VM, VM, VM, VM, pl.BlockSpec(memory_space=pltpu.SMEM), VM] + [ANY] * 12,
        out_specs=ANY,
        out_shape=jax.ShapeDtypeStruct((NB, HID), BF),
        scratch_shapes=[pltpu.VMEM((NB, HID), BF), dma((8,))] + [pltpu.VMEM(w.shape, BF) for w in (wo, wg, wu, wd, wq, wo2)] + [
            dma((10,)), pltpu.VMEM((NR, CR, T2, D), BF), pltpu.VMEM((NR, CR, T2, D), BF), dma((2, NR)),
            pltpu.VMEM((NH * HL, D), F32), pltpu.VMEM((NH * HL, D), F32), pltpu.VMEM((8, D), F32),
            pltpu.VMEM((8, D), F32), dma((2, 5)), pltpu.VMEM((NQ, HID), BF), pltpu.VMEM((NH * HL, D), F32),
            pltpu.VMEM((NH, xvalid.shape[1]), jnp.int32), pltpu.VMEM((NH, D), jnp.int32),
            pltpu.VMEM((NH * 8, D), F32), pltpu.VMEM((2, NQ, HID), BF), pltpu.VMEM((2, NQ, F), BF),
            pltpu.VMEM((NQ, HID), BF), pltpu.VMEM((NQ, HID), BF), pltpu.VMEM((2, NCH, HQ, W), F32),
            pltpu.VMEM((2, NCH, HQ, W), F32), pltpu.VMEM((2, 2, NCH, HQ, W), F32), dma((2, 6, NCH))]
        + sum_bufs + sum_bufs + [pltpu.VMEM((NCH, RC, HID), F32)] * 4 + [dma((4, NCH)), dma((2, NCH))]
        + share_bufs + share_bufs + [dma((2, 4, NCH))],
        compiler_params=pltpu.CompilerParams(collective_id=0, has_side_effects=True, vmem_limit_bytes=VMEM_MAX),
        name="rest_of_step",
    )(o, st, hidden, g2, g3, qn, g4, gates, mask, xvalid, *ws, k_cross, v_cross)


def solution(mesh):
    cache_spec = P('dp', 'sp', 'tp', None)
    cross_spec = P('dp', None, 'tp', None)
    row_spec = P('dp', None)
    vec_spec = P('dp')
    full_spec = P(None)
    col_spec = P(None, 'tp')
    split_rows = P('tp', None)
    in_specs = (row_spec, vec_spec, cache_spec, cache_spec, cross_spec, cross_spec, row_spec, vec_spec,
                full_spec, col_spec, col_spec, col_spec, split_rows, full_spec, col_spec, col_spec, split_rows,
                full_spec, col_spec, full_spec, split_rows, full_spec, full_spec, col_spec, col_spec, split_rows)
    out_specs = (row_spec, cache_spec, cache_spec)

    def local_step(hidden, new_pos, k_self, v_self, k_cross, v_cross, xvalid, rowmask,
                   self_attn_norm, self_wq, self_wk, self_wv, self_wo, self_mlp_norm,
                   self_wgate, self_wup, self_wdown, cross_attn_norm, cross_wq, cross_qnorm,
                   cross_wo, cross_gates, cross_mlp_norm, cross_wgate, cross_wup, cross_wdown):
        flat = lambda a: a.reshape(a.shape[0], a.shape[1] * a.shape[2], a.shape[3])
        k_out, v_out, o, st = self_attention(new_pos, self_attn_norm, hidden, self_wq, self_wk, self_wv,
                                             flat(k_self), flat(v_self))
        weights = (self_wo, self_wgate, self_wup, self_wdown, cross_wq, cross_wo, cross_wgate, cross_wup, cross_wdown)
        h4 = rest_of_step(o, st, hidden, self_mlp_norm, cross_attn_norm, cross_qnorm, cross_mlp_norm, cross_gates,
                          rowmask, xvalid, weights, flat(k_cross), flat(v_cross))
        return h4, k_out.reshape(k_self.shape), v_out.reshape(v_self.shape)

    return jax.shard_map(local_step, mesh=mesh, in_specs=in_specs, out_specs=out_specs, check_vma=False)
```

```python
import functools
import math
import numpy as np
import jax
import jax.numpy as jnp
from jax import lax
from jax.experimental import pallas as pl
from jax.experimental.pallas import tpu as pltpu
from jax.sharding import PartitionSpec as P

NORM_EPS = 1e-5
ROPE_THETA = 500000.0
ROPE_FACTOR = 8.0
LOW_FREQ = 1.0
HIGH_FREQ = 4.0
ORIG_CTX = 8192.0
NEG_BIG = -1e30

BF = jnp.bfloat16
F32 = jnp.float32
D = 128
HL = 4
KL = 2
NB = 256
NH = 128
NQ = 64
HID = 2048
HQ = NQ // 2
NCH = 4
W = HID // NCH
VMEM_MAX = 66 * 1024 * 1024 - 2 * 1024 * 1024
MESH = pl.DeviceIdType.MESH
ANY = pl.BlockSpec(memory_space=pl.ANY)
VM = pl.BlockSpec(memory_space=pltpu.VMEM)


def rope_freqs(head_dim):
    inv_freq = 1.0 / (ROPE_THETA ** (np.arange(0, head_dim, 2) / head_dim))
    wavelen = 2.0 * math.pi / inv_freq
    smooth = (ORIG_CTX / wavelen - LOW_FREQ) / (HIGH_FREQ - LOW_FREQ)
    mid_freq = (1.0 - smooth) * inv_freq / ROPE_FACTOR + smooth * inv_freq
    scaled = np.where(wavelen > ORIG_CTX / LOW_FREQ, inv_freq / ROPE_FACTOR, mid_freq)
    scaled = np.where(wavelen < ORIG_CTX / HIGH_FREQ, inv_freq, scaled)
    return np.concatenate([scaled, scaled]).astype(np.float32)[None, :]


def norm32(vals32, gain32):
    inv = lax.rsqrt(jnp.mean(vals32 * vals32, axis=-1, keepdims=True) + NORM_EPS)
    return (vals32 * inv * gain32).astype(BF)


def dot(a, b):
    return jnp.dot(a, b, preferred_element_type=F32)


def dot_nt(a, b):
    return lax.dot_general(a, b, (((1,), (1,)), ((), ())), preferred_element_type=F32)


def attend(lhs, keys, vals, valid):
    first = lax.broadcasted_iota(jnp.int32, (8, D), 0) < HL
    s = [dot_nt(a, k) * (D ** -0.5) for a, k in zip(lhs, keys)]
    s = [jnp.where(ok, x, NEG_BIG) for ok, x in zip(valid, s)]
    m = [jnp.max(x, axis=-1, keepdims=True) for x in s]
    p = [jnp.where(ok, jnp.exp(x - t), 0.0) for ok, x, t in zip(valid, s, m)]
    l = [jnp.sum(x, axis=-1, keepdims=True) for x in p]
    o = [dot(x.astype(BF), v) for x, v in zip(p, vals)]
    return m, l, [jnp.where(first, x[:, :D], x[:, D:]) for x in o]


def pair_lhs(q_ref, b0):
    q16 = q_ref[pl.ds(pl.multiple_of(b0 * 8, 16), 16), :]
    return jnp.concatenate([q16[:8], q16[8:]], axis=1).astype(BF)


def column(vec, first, rows):
    n = vec.shape[1]
    at = lax.broadcasted_iota(jnp.int32, (rows, n), 1) == lax.broadcasted_iota(jnp.int32, (rows, n), 0) + first
    return jnp.sum(jnp.where(at, vec, 0.0), axis=1, keepdims=True)


def spread_heads(ref, heads, start, rows):
    odd = (lax.broadcasted_iota(jnp.int32, (rows, D), 0) % 2) == 1
    for h in range(HL):
        ref[pl.ds(start * 8 + h, rows, stride=8), :] = jnp.where(odd, 0.0, heads[h])
        ref[pl.ds(start * 8 + HL + h, rows, stride=8), :] = jnp.where(odd, heads[h], 0.0)


SR = 16


def self_kernel(pos_ref, posv_ref, freq_ref, g_ref, hid_hbm, wq_hbm, wk_hbm, wv_hbm, k_hbm, v_hbm,
                ko_hbm, vo_hbm, o_hbm, st_hbm,
                hid, wq, wk, wv, wsem, kbuf, vbuf, isem, osem, qs, kn, vn, o_ref, st_ref, rsem):
    T2 = k_hbm.shape[1]
    steps = NB // SR
    first_pos = lax.axis_index("sp") * (T2 // KL)
    loads = [pltpu.make_async_copy(a, b, wsem.at[n])
             for n, (a, b) in enumerate(((hid_hbm, hid), (wq_hbm, wq), (wk_hbm, wk), (wv_hbm, wv)))]
    for cp in loads:
        cp.start()

    def into(i):
        rows = pl.ds(pl.multiple_of(i * SR, SR), SR)
        return (pltpu.make_async_copy(k_hbm.at[rows], kbuf.at[i], isem.at[0, i]),
                pltpu.make_async_copy(v_hbm.at[rows], vbuf.at[i], isem.at[1, i]))

    def out_of(i):
        rows = pl.ds(pl.multiple_of(i * SR, SR), SR)
        return (pltpu.make_async_copy(kbuf.at[i], ko_hbm.at[rows], osem.at[0, i]),
                pltpu.make_async_copy(vbuf.at[i], vo_hbm.at[rows], osem.at[1, i]))

    early = 5
    for i in range(early):
        for cp in into(i):
            cp.start()

    with jax.named_scope("qkv"):
        angle = column(posv_ref[...].astype(F32).reshape(1, NB), 0, NB) * freq_ref[...]
        cos, sin = jnp.cos(angle), jnp.sin(angle)
        sin = jnp.where(lax.broadcasted_iota(jnp.int32, (NB, D), 1) < D // 2, -sin, sin)

        def rope(part):
            part = part.astype(BF).astype(F32)
            return (part * cos + pltpu.roll(part, D // 2, 1) * sin).astype(BF).astype(F32)

        loads[0].wait()
        loads[1].wait()
        for i in range(early, steps):
            for cp in into(i):
                cp.start()
        x = norm32(hid[...].astype(F32), g_ref[...].astype(F32).reshape(1, HID))
        q = dot(x, wq[...])
        spread_heads(qs, [rope(q[:, h * D:(h + 1) * D]) for h in range(HL)], 0, NB)
        loads[2].wait()
        k = dot(x, wk[...])
        loads[3].wait()
        v = dot(x, wv[...])
        for h in range(KL):
            kn[pl.ds(h, NB, stride=KL), :] = rope(k[:, h * D:(h + 1) * D])
            vn[pl.ds(h, NB, stride=KL), :] = v[:, h * D:(h + 1) * D].astype(BF).astype(F32)
    st_ref[...] = jnp.zeros_like(st_ref)

    col = lax.broadcasted_iota(jnp.int32, (8, T2), 1)
    row = lax.broadcasted_iota(jnp.int32, (8, T2), 0)
    tok = col // KL
    head_ok = (col % KL) == ((row % HL) // (HL // KL))
    lane = lax.broadcasted_iota(jnp.int32, (8, D), 1)
    i16 = lax.broadcasted_iota(jnp.int32, (16, D), 0)

    def patch(new_ref, dst_ref, slot, r, b, lp):
        base = pl.multiple_of((jnp.clip(lp, 0, T2 // KL - 1) // 8) * 16, 16)
        fresh = jnp.where(i16 % 2 == 0, new_ref[pl.ds(2 * b, 1), :], new_ref[pl.ds(2 * b + 1, 1), :])
        old = dst_ref[slot, r, pl.ds(base, 16), :].astype(F32)
        dst_ref[slot, r, pl.ds(base, 16), :] = jnp.where(base + i16 - i16 % 2 == 2 * lp, fresh, old).astype(BF)

    def body(i, _):
        for cp in into(i):
            cp.wait()
        lps = [pos_ref[i * SR + r] - first_pos for r in range(SR)]
        for r in range(SR):
            patch(kn, kbuf, i, r, i * SR + r, lps[r])
            patch(vn, vbuf, i, r, i * SR + r, lps[r])
        pairs = range(SR // 2)
        both = lambda buf, p: jnp.concatenate([buf[i, 2 * p], buf[i, 2 * p + 1]], axis=1)
        m, l, o = attend([pair_lhs(qs, i * SR + 2 * p) for p in pairs], [both(kbuf, p) for p in pairs],
                         [both(vbuf, p) for p in pairs],
                         [head_ok & (tok <= jnp.where(row < HL, lps[2 * p], lps[2 * p + 1])) for p in pairs])
        half = i // (NH // SR)
        srow = pl.ds(pl.multiple_of(half * 8, 8), 8)
        st = st_ref[srow, :]
        for p in pairs:
            o_ref[pl.ds(pl.multiple_of(i * SR * HL + 8 * p, 8), 8), :] = o[p]
            at = (i - half * (NH // SR)) * (SR // 2) + p
            st = jnp.where(lane == at, m[p], jnp.where(lane == at + NQ, l[p], st))
        st_ref[srow, :] = st
        for cp in out_of(i):
            cp.start()
        return 0

    results = []
    for i in range(4):
        with jax.named_scope("steps"):
            lax.fori_loop(i * (steps // 4), (i + 1) * (steps // 4), body, 0)
        part = pl.ds(i * (NB * HL // 4), NB * HL // 4)
        results.append(pltpu.make_async_copy(o_ref.at[part], o_hbm.at[part], rsem.at[i]))
        results[-1].start()
    results.append(pltpu.make_async_copy(st_ref, st_hbm, rsem.at[4]))
    results[-1].start()
    with jax.named_scope("drain"):
        for i in range(steps):
            for cp in out_of(i):
                cp.wait()
        for cp in results:
            cp.wait()


def self_attention(new_pos, g1, hidden, wq, wk, wv, k_self, v_self):
    T2 = k_self.shape[1]
    return pl.pallas_call(
        self_kernel,
        in_specs=[pl.BlockSpec(memory_space=pltpu.SMEM), VM, VM, VM] + [ANY] * 6,
        out_specs=[ANY] * 4,
        scratch_shapes=[pltpu.VMEM(hidden.shape, BF), pltpu.VMEM(wq.shape, BF), pltpu.VMEM(wk.shape, BF),
                        pltpu.VMEM(wv.shape, BF), pltpu.SemaphoreType.DMA((4,)),
                        pltpu.VMEM((NB // SR, SR, T2, D), BF), pltpu.VMEM((NB // SR, SR, T2, D), BF),
                        pltpu.SemaphoreType.DMA((2, NB // SR)), pltpu.SemaphoreType.DMA((2, NB // SR)),
                        pltpu.VMEM((NB * 8, D), F32), pltpu.VMEM((NB * KL, D), F32), pltpu.VMEM((NB * KL, D), F32),
                        pltpu.VMEM((NB * HL, D), F32), pltpu.VMEM((16, D), F32), pltpu.SemaphoreType.DMA((5,))],
        out_shape=[jax.ShapeDtypeStruct(k_self.shape, BF), jax.ShapeDtypeStruct(v_self.shape, BF),
                   jax.ShapeDtypeStruct((NB * HL, D), F32), jax.ShapeDtypeStruct((16, D), F32)],
        compiler_params=pltpu.CompilerParams(vmem_limit_bytes=VMEM_MAX),
        name="self_attn",
    )(new_pos, new_pos, jnp.asarray(rope_freqs(D)), g1, hidden, wq, wk, wv, k_self, v_self)


def peers():
    sp, tp = lax.axis_index("sp"), lax.axis_index("tp")
    core = lax.rem(tp, 2)
    return dict(sp=sp, core=core, y={"sp": 1 - sp}, c={"tp": tp + 1 - 2 * core}, x={"tp": lax.rem(tp + 2, 4)})


def entry_barrier(pe):
    barrier = pltpu.get_barrier_semaphore()
    for name in ("y", "c", "x"):
        pl.semaphore_signal(barrier, inc=1, device_id=pe[name], device_id_type=MESH)
    pl.semaphore_wait(barrier, 3)


def rcopy(src, dst, ssem, rsem, dev):
    return pltpu.make_async_remote_copy(src_ref=src, dst_ref=dst, send_sem=ssem, recv_sem=rsem,
                                        device_id=dev, device_id_type=MESH)


class TpSum:
    def __init__(self, pe, half, bufs):
        snd, rcv, chip, xr, sems = bufs
        self.snd, self.rcv, self.chip, self.xr = (b.at[half] for b in (snd, rcv, chip, xr))
        at = lambda n, j: sems.at[half, n, j]
        self.to_core = [rcopy(self.snd.at[j], self.rcv.at[j], at(0, j), at(1, j), pe["c"]) for j in range(NCH)]
        self.to_chip = [rcopy(self.chip.at[j], self.xr.at[j], at(2, j), at(3, j), pe["x"]) for j in range(NCH)]

    def start(self, compute):
        for j in range(NCH):
            part = compute(j)
            self.snd[j] = part[HQ:]
            self.chip[j] = part[:HQ]
            self.to_core[j].start()

    def forward(self):
        for j in range(NCH):
            self.to_core[j].wait_recv()
            self.chip[j] = self.chip[j] + self.rcv[j]
            self.to_chip[j].start()

    def close(self, finish):
        for j in range(NCH):
            self.to_chip[j].wait_recv()
            finish(j, self.chip[j] + self.xr[j])
        for j in range(NCH):
            self.to_core[j].wait_send()
            self.to_chip[j].wait_send()


class Share:
    def __init__(self, pe, half, x_ref, snd, rcv, sems):
        rows = pl.ds(half * HQ, HQ)
        self.snd, self.rcv, self.x = snd.at[rows], rcv.at[rows], x_ref.at[half]
        self.copy = rcopy(self.snd, self.rcv, sems.at[0, half], sems.at[1, half], pe["c"])

    def start(self, own):
        self.snd[...] = own.astype(F32)
        self.copy.start()
        self.x[pl.ds(0, HQ), :] = own

    def finish(self):
        self.copy.wait()
        self.x[pl.ds(HQ, HQ), :] = self.rcv[...].astype(BF)


def mlp_act(x_ref, wg, wu, act, chunks):
    step = act.shape[1] // 3
    for c in chunks:
        s = slice(c * step, (c + 1) * step)
        gate = dot(x_ref[...], wg[:, s]).astype(BF).astype(F32)
        up = dot(x_ref[...], wu[:, s]).astype(BF).astype(F32)
        act[:, s] = (gate * jax.nn.sigmoid(gate) * up).astype(BF)


def cols(j):
    return slice(j * W, (j + 1) * W)


def heads_to_lanes(ref, starts, rows):
    parts = [jnp.concatenate([ref[pl.ds(s * HL + h, rows, stride=HL), :] for h in range(HL)], axis=1) for s in starts]
    return jnp.concatenate(parts, axis=0).astype(BF)


CR = 8
NR = 5
RC = NQ // NCH
XB = 2 * RC // CR


def rest_kernel(o_hbm, st_ref, hid_hbm, g2_ref, g3_ref, qn_ref, g4_ref, gates_ref, mask_ref, valid_hbm,
                wo_hbm, wg_hbm, wu_hbm, wd_hbm, wq_hbm, wo2_hbm, wg2_hbm, wu2_hbm, wd2_hbm, k_hbm, v_hbm,
                out_hbm,
                out_ref, rsem, wo, wg, wu, wd, wq, wo2, wsem, kbuf, vbuf, ksem, osnd, orcv, sts, str_, ysem, hown, att, valid, cnt,
                qx, xbuf, act, hres, h2, fin, yr, cr, gsem,
                a0, a1, a2, a3, asem, b0, b1, b2, b3, bsem, c0, c1, c2, c3, csem, dsem,
                s0, s1, ssem, t0, t1, tsem, esem):
    pe = peers()
    sp, core = pe["sp"], pe["core"]
    T2 = k_hbm.shape[1]
    half = NH * HL
    blocks = NH // CR

    local = [pltpu.make_async_copy(o_hbm.at[pl.ds(pl.multiple_of((1 - sp) * half, half), half)], osnd, wsem.at[6]),
             pltpu.make_async_copy(o_hbm.at[pl.ds(pl.multiple_of(sp * half, half), half)], att, wsem.at[7]),
             pltpu.make_async_copy(hid_hbm.at[pl.ds(pl.multiple_of(sp * NH + core * NQ, NQ), NQ)], hown, wsem.at[8]),
             pltpu.make_async_copy(valid_hbm.at[pl.ds(pl.multiple_of(sp * NH, NH), NH)], valid, wsem.at[9])]
    pairs = ((wo_hbm, wo), (wg_hbm, wg), (wu_hbm, wu), (wd_hbm, wd), (wq_hbm, wq), (wo2_hbm, wo2))
    loads = [pltpu.make_async_copy(a, b, wsem.at[n]) for n, (a, b) in enumerate(pairs)]
    for cp in local:
        cp.start()

    def block_row(t):
        chunk, of_core, sub = t // XB, (t % XB) // (XB // 2), t % (XB // 2)
        return of_core * NQ + chunk * RC + sub * CR

    def kv_loads(t):
        rows, slot = pl.ds(pl.multiple_of(sp * NH + block_row(t), CR), CR), t % NR
        return (pltpu.make_async_copy(k_hbm.at[rows], kbuf.at[slot], ksem.at[0, slot]),
                pltpu.make_async_copy(v_hbm.at[rows], vbuf.at[slot], ksem.at[1, slot]))

    with jax.named_scope("enter"):
        entry_barrier(pe)
    both = st_ref[...]
    mine = jnp.where(sp == 0, both[:8], both[8:])
    sts[...] = jnp.where(sp == 0, both[8:], both[:8])
    local[0].wait()
    cp_s = rcopy(sts, str_, ysem.at[0, 4], ysem.at[1, 4], pe["y"])
    cp_s.start()

    def quarter(h, c):
        rows = pl.ds((c * NQ + h * HQ) * HL, HQ * HL)
        return rcopy(osnd.at[rows], orcv.at[rows], ysem.at[0, 2 * h + c], ysem.at[1, 2 * h + c], pe["y"])

    quarters = [quarter(h, c) for h in range(2) for c in range(2)]
    for cp in quarters:
        cp.start()
    for cp in local[1:]:
        cp.wait()
    for cp in loads:
        cp.start()
    for t in range(NR):
        for cp in kv_loads(t):
            cp.start()
    some = jnp.sum((valid[...] > 0).astype(jnp.int32), axis=1, keepdims=True)
    cnt[...] = jnp.broadcast_to(some, cnt.shape)
    row_scale = column(mask_ref[...].astype(F32).reshape(1, NB), sp * NH + core * NQ, NQ)
    gate0 = jnp.tanh(jnp.full((8, D), gates_ref[0], F32))[0:1, 0:1] * row_scale
    gate1 = jnp.tanh(jnp.full((8, D), gates_ref[1], F32))[0:1, 0:1] * row_scale
    gain = lambda ref: ref[...].astype(F32).reshape(1, HID)
    owned = [slice(h * HQ, (h + 1) * HQ) for h in range(2)]
    sum1 = [TpSum(pe, h, (a0, a1, a2, a3, asem)) for h in range(2)]
    sum2 = [TpSum(pe, h, (b0, b1, b2, b3, bsem)) for h in range(2)]
    sum4 = [TpSum(pe, h, (a0, a1, a2, a3, esem)) for h in range(2)]
    share1 = [Share(pe, h, xbuf, s0, s1, ssem) for h in range(2)]
    share2 = [Share(pe, h, xbuf, t0, t1, tsem) for h in range(2)]

    cp_s.wait()
    theirs = str_[...]
    top = jnp.maximum(mine, theirs)
    f1, f2 = jnp.exp(mine - top), jnp.exp(theirs - top)
    den = pltpu.roll(mine, NQ, 1) * f1 + pltpu.roll(theirs, NQ, 1) * f2
    w1, w2 = f1 / den, f2 / den

    def combine(h):
        for c in range(2):
            quarters[2 * h + c].wait()
            for p in range((c * NQ + h * HQ) // 2, (c * NQ + h * HQ + HQ) // 2):
                s = pl.ds(8 * p, 8)
                att[s, :] = att[s, :] * w1[:, p:p + 1] + orcv[s, :] * w2[:, p:p + 1]
        return heads_to_lanes(att, (core * NQ + h * HQ, (1 - core) * NQ + h * HQ), HQ)

    def close1(h):
        def done(j, total):
            hres[owned[h], cols(j)] = (hown[owned[h], cols(j)].astype(F32) + total).astype(BF)

        sum1[h].close(done)
        share1[h].start(norm32(hres[owned[h], :].astype(F32), gain(g2_ref)))

    def mlp_down(h, total):
        total.start(lambda j: dot(act[h], wd[:, cols(j)]))

    def mlp(h, total):
        mlp_act(xbuf.at[h], wg, wu, act.at[h], range(3))
        mlp_down(h, total)

    def close2(h):
        def done(j, total):
            h2[owned[h], cols(j)] = (hres[owned[h], cols(j)].astype(F32) + total).astype(BF)

        sum2[h].close(done)
        share2[h].start(norm32(h2[owned[h], :].astype(F32), gain(g3_ref)))

    def cross_q(h):
        share2[h].finish()
        q = dot(xbuf[h], wq[...])
        qgain = qn_ref[...].astype(F32).reshape(1, D)
        heads = [norm32(q[:, n * D:(n + 1) * D].astype(BF).astype(F32), qgain).astype(F32) for n in range(HL)]
        spread_heads(qx, [x[:HQ] for x in heads], core * NQ + h * HQ, HQ)
        spread_heads(qx, [x[HQ:] for x in heads], (1 - core) * NQ + h * HQ, HQ)

    with jax.named_scope("out_a"):
        lhs0 = combine(0)
        loads[0].wait()
        sum1[0].start(lambda j: dot(lhs0, wo[:, cols(j)]))
    with jax.named_scope("out_b"):
        sum1[0].forward()
        lhs1 = combine(1)
        sum1[1].start(lambda j: dot(lhs1, wo[:, cols(j)]))
        sum1[1].forward()
    with jax.named_scope("close1_a"):
        close1(0)
    with jax.named_scope("share1_a"):
        share1[0].finish()
    for cp in loads[1:4]:
        cp.wait()
    with jax.named_scope("mlp_a"):
        mlp(0, sum2[0])
    with jax.named_scope("close1_b"):
        close1(1)
    with jax.named_scope("forward2_a"):
        sum2[0].forward()
    with jax.named_scope("share1_b"):
        share1[1].finish()
    with jax.named_scope("mlp_b"):
        mlp(1, sum2[1])
    loads2 = [pltpu.make_async_copy(a, b, wsem.at[1 + n])
              for n, (a, b) in enumerate(((wg2_hbm, wg), (wu2_hbm, wu), (wd2_hbm, wd)))]
    for cp in loads2:
        cp.start()
    with jax.named_scope("close2_a"):
        close2(0)
    with jax.named_scope("forward2_b"):
        sum2[1].forward()
    loads[4].wait()
    with jax.named_scope("q_a"):
        cross_q(0)
    loads[5].wait()

    col = lax.broadcasted_iota(jnp.int32, (8, T2), 1)
    row = lax.broadcasted_iota(jnp.int32, (8, T2), 0)
    tok = col // KL
    head_ok = (col % KL) == ((row % HL) // (HL // KL))
    first = lax.broadcasted_iota(jnp.int32, (8, D), 0) < HL

    def block(t, _):
        slot = t % NR
        r0 = pl.multiple_of(block_row(t), CR)
        for cp in kv_loads(t):
            cp.wait()
        ps = range(CR // 2)
        lane_pair = lambda buf, p: jnp.concatenate([buf[slot, 2 * p], buf[slot, 2 * p + 1]], axis=1)
        n8 = cnt[pl.ds(r0, CR), :]
        limit = [jnp.concatenate([jnp.where(first, n8[2 * p:2 * p + 1], n8[2 * p + 1:2 * p + 2])] * (T2 // D), axis=1)
                 for p in ps]
        m, l, o = attend([pair_lhs(qx, r0 + 2 * p) for p in ps], [lane_pair(kbuf, p) for p in ps],
                         [lane_pair(vbuf, p) for p in ps], [head_ok & (tok < n) for n in limit])
        for p in ps:
            att[pl.ds(pl.multiple_of(r0 * HL + 8 * p, 8), 8), :] = o[p] / l[p]

        @pl.when(t + NR < blocks)
        def _():
            for cp in kv_loads(t + NR):
                cp.start()
        return 0

    to_core = [rcopy(c0.at[j], c1.at[j], csem.at[0, j], csem.at[1, j], pe["c"]) for j in range(NCH)]
    to_chip = [rcopy(c2.at[j], c3.at[j], csem.at[2, j], csem.at[3, j], pe["x"]) for j in range(NCH)]
    share = [rcopy(s0.at[pl.ds(j * RC, RC)], s1.at[pl.ds(j * RC, RC)], dsem.at[0, j], dsem.at[1, j], pe["c"])
             for j in range(NCH)]

    def pass_chip(j):
        to_core[j].wait_recv()
        c2[j] = c2[j] + c1[j]
        to_chip[j].start()

    def close3(j):
        mine = slice(j * RC, (j + 1) * RC)
        to_chip[j].wait_recv()
        hres[mine, :] = (h2[mine, :].astype(F32) + gate0[mine] * (c2[j] + c3[j])).astype(BF)
        own = norm32(hres[mine, :].astype(F32), gain(g4_ref))
        s0[mine, :] = own.astype(F32)
        share[j].start()
        xbuf[j // 2, pl.ds((j % 2) * RC, RC), :] = own

    def shared3(j):
        share[j].wait_recv()
        xbuf[j // 2, pl.ds(HQ + (j % 2) * RC, RC), :] = s1[pl.ds(j * RC, RC), :].astype(BF)

    def cross_out(j):
        lhs = heads_to_lanes(att, (core * NQ + j * RC, (1 - core) * NQ + j * RC), RC)
        for n in range(NCH):
            part = dot(lhs, wo2[:, cols(n)])
            c0[j, :, cols(n)] = part[RC:]
            c2[j, :, cols(n)] = part[:RC]
        to_core[j].start()

    to_y = [[rcopy(fin.at[h, j], yr.at[h, j], gsem.at[h, 0, j], gsem.at[h, 1, j], pe["y"]) for j in range(NCH)]
            for h in range(2)]
    to_c = [[rcopy(fin.at[h, j], cr.at[0, h, j], gsem.at[h, 2, j], gsem.at[h, 3, j], pe["c"]) for j in range(NCH)]
            for h in range(2)]
    pass_c = [[rcopy(yr.at[h, j], cr.at[1, h, j], gsem.at[h, 4, j], gsem.at[h, 5, j], pe["c"]) for j in range(NCH)]
              for h in range(2)]

    def rows(of_sp, of_core, h):
        return pl.ds(pl.multiple_of(of_sp * NH + of_core * NQ + h * HQ, HQ), HQ)

    outs = []

    def put(of_sp, of_core, h):
        r = rows(of_sp, of_core, h)
        outs.append(pltpu.make_async_copy(out_ref.at[r], out_hbm.at[r], rsem.at[len(outs)]))
        outs[-1].start()

    def pass_on(h, j):
        to_y[h][j].wait_recv()
        pass_c[h][j].start()

    def close4(h, passing):
        def done(j, total):
            res = (hres[owned[h], cols(j)].astype(F32) + gate1[owned[h]] * total).astype(BF)
            out_ref[rows(sp, core, h), cols(j)] = res
            fin[h, j] = res.astype(F32)
            to_y[h][j].start()
            to_c[h][j].start()
            if passing is not None:
                pass_on(passing, j)

        sum4[h].close(done)
        put(sp, core, h)

    def gathered(h):
        for j in range(NCH):
            to_c[h][j].wait_recv()
            out_ref[rows(sp, 1 - core, h), cols(j)] = cr[0, h, j].astype(BF)
        put(sp, 1 - core, h)
        for j in range(NCH):
            out_ref[rows(1 - sp, core, h), cols(j)] = yr[h, j].astype(BF)
        put(1 - sp, core, h)
        for j in range(NCH):
            pass_c[h][j].wait_recv()
            out_ref[rows(1 - sp, 1 - core, h), cols(j)] = cr[1, h, j].astype(BF)
        put(1 - sp, 1 - core, h)
        for j in range(NCH):
            to_y[h][j].wait_send()
            to_c[h][j].wait_send()
            pass_c[h][j].wait_send()

    blocks_to = lambda lo, hi: lax.fori_loop(lo, hi, block, 0)
    with jax.named_scope("x0"):
        blocks_to(0, 4)
    with jax.named_scope("o0"):
        cross_out(0)
    with jax.named_scope("x4"):
        blocks_to(4, 5)
    with jax.named_scope("pass0"):
        pass_chip(0)
    with jax.named_scope("x5"):
        blocks_to(5, 7)
    with jax.named_scope("close2_b"):
        close2(1)
    with jax.named_scope("x7"):
        blocks_to(7, 8)
    with jax.named_scope("o1"):
        cross_out(1)
    with jax.named_scope("q_b"):
        cross_q(1)
    with jax.named_scope("x8"):
        blocks_to(8, 9)
    with jax.named_scope("pass1"):
        pass_chip(1)
    with jax.named_scope("close3_0"):
        close3(0)
    with jax.named_scope("x9"):
        blocks_to(9, 12)
    with jax.named_scope("o2"):
        cross_out(2)
    with jax.named_scope("x12"):
        blocks_to(12, 13)
    with jax.named_scope("pass2"):
        pass_chip(2)
    with jax.named_scope("close3_1"):
        close3(1)
    with jax.named_scope("x13"):
        blocks_to(13, 16)
    with jax.named_scope("o3"):
        cross_out(3)
    with jax.named_scope("shared01"):
        shared3(0)
        shared3(1)
        for cp in loads2:
            cp.wait()
    with jax.named_scope("mlp2_a"):
        mlp_act(xbuf.at[0], wg, wu, act.at[0], (0,))
        pass_chip(3)
        mlp_act(xbuf.at[0], wg, wu, act.at[0], (1,))
        close3(2)
        mlp_act(xbuf.at[0], wg, wu, act.at[0], (2,))
        mlp_down(0, sum4[0])
    with jax.named_scope("forward4_a"):
        sum4[0].forward()
    with jax.named_scope("close3_3"):
        close3(3)
    with jax.named_scope("shared23"):
        shared3(2)
        shared3(3)
    with jax.named_scope("mlp2_b"):
        mlp(1, sum4[1])
    with jax.named_scope("forward4_b"):
        sum4[1].forward()
    with jax.named_scope("close4_a"):
        close4(0, None)
    with jax.named_scope("close4_b"):
        close4(1, 0)
    with jax.named_scope("gathered_a"):
        gathered(0)
    with jax.named_scope("gathered_b"):
        for j in range(NCH):
            pass_on(1, j)
        gathered(1)
    for j in range(NCH):
        to_core[j].wait_send()
        to_chip[j].wait_send()
        share[j].wait_send()
    for cp in outs:
        cp.wait()


def rest_of_step(o, st, hidden, g2, g3, qn, g4, gates, mask, xvalid, ws, k_cross, v_cross):
    wo, wg, wu, wd, wq, wo2 = ws[:6]
    F = wg.shape[1]
    T2 = k_cross.shape[1]
    dma = pltpu.SemaphoreType.DMA
    sum_bufs = [pltpu.VMEM((2, NCH, HQ, W), F32)] * 4 + [dma((2, 4, NCH))]
    share_bufs = [pltpu.VMEM((NQ, HID), F32)] * 2 + [dma((2, 2))]
    return pl.pallas_call(
        rest_kernel,
        in_specs=[ANY, VM, ANY, VM, VM, VM, VM, pl.BlockSpec(memory_space=pltpu.SMEM), VM] + [ANY] * 12,
        out_specs=ANY,
        out_shape=jax.ShapeDtypeStruct((NB, HID), BF),
        scratch_shapes=[pltpu.VMEM((NB, HID), BF), dma((8,))] + [pltpu.VMEM(w.shape, BF) for w in (wo, wg, wu, wd, wq, wo2)] + [
            dma((10,)), pltpu.VMEM((NR, CR, T2, D), BF), pltpu.VMEM((NR, CR, T2, D), BF), dma((2, NR)),
            pltpu.VMEM((NH * HL, D), F32), pltpu.VMEM((NH * HL, D), F32), pltpu.VMEM((8, D), F32),
            pltpu.VMEM((8, D), F32), dma((2, 5)), pltpu.VMEM((NQ, HID), BF), pltpu.VMEM((NH * HL, D), F32),
            pltpu.VMEM((NH, xvalid.shape[1]), jnp.int32), pltpu.VMEM((NH, D), jnp.int32),
            pltpu.VMEM((NH * 8, D), F32), pltpu.VMEM((2, NQ, HID), BF), pltpu.VMEM((2, NQ, F), BF),
            pltpu.VMEM((NQ, HID), BF), pltpu.VMEM((NQ, HID), BF), pltpu.VMEM((2, NCH, HQ, W), F32),
            pltpu.VMEM((2, NCH, HQ, W), F32), pltpu.VMEM((2, 2, NCH, HQ, W), F32), dma((2, 6, NCH))]
        + sum_bufs + sum_bufs + [pltpu.VMEM((NCH, RC, HID), F32)] * 4 + [dma((4, NCH)), dma((2, NCH))]
        + share_bufs + share_bufs + [dma((2, 4, NCH))],
        compiler_params=pltpu.CompilerParams(collective_id=0, has_side_effects=True, vmem_limit_bytes=VMEM_MAX),
        name="rest_of_step",
    )(o, st, hidden, g2, g3, qn, g4, gates, mask, xvalid, *ws, k_cross, v_cross)


def solution(mesh):
    cache_spec = P('dp', 'sp', 'tp', None)
    cross_spec = P('dp', None, 'tp', None)
    row_spec = P('dp', None)
    vec_spec = P('dp')
    full_spec = P(None)
    col_spec = P(None, 'tp')
    split_rows = P('tp', None)
    in_specs = (row_spec, vec_spec, cache_spec, cache_spec, cross_spec, cross_spec, row_spec, vec_spec,
                full_spec, col_spec, col_spec, col_spec, split_rows, full_spec, col_spec, col_spec, split_rows,
                full_spec, col_spec, full_spec, split_rows, full_spec, full_spec, col_spec, col_spec, split_rows)
    out_specs = (row_spec, cache_spec, cache_spec)

    def local_step(hidden, new_pos, k_self, v_self, k_cross, v_cross, xvalid, rowmask,
                   self_attn_norm, self_wq, self_wk, self_wv, self_wo, self_mlp_norm,
                   self_wgate, self_wup, self_wdown, cross_attn_norm, cross_wq, cross_qnorm,
                   cross_wo, cross_gates, cross_mlp_norm, cross_wgate, cross_wup, cross_wdown):
        flat = lambda a: a.reshape(a.shape[0], a.shape[1] * a.shape[2], a.shape[3])
        k_out, v_out, o, st = self_attention(new_pos, self_attn_norm, hidden, self_wq, self_wk, self_wv,
                                             flat(k_self), flat(v_self))
        weights = (self_wo, self_wgate, self_wup, self_wdown, cross_wq, cross_wo, cross_wgate, cross_wup, cross_wdown)
        h4 = rest_of_step(o, st, hidden, self_mlp_norm, cross_attn_norm, cross_qnorm, cross_mlp_norm, cross_gates,
                          rowmask, xvalid, weights, flat(k_cross), flat(v_cross))
        return h4, k_out.reshape(k_self.shape), v_out.reshape(v_self.shape)

    return jax.shard_map(local_step, mesh=mesh, in_specs=in_specs, out_specs=out_specs, check_vma=False)
```
